32 devices in a mesh: seq: 8 (over y, x, core), zero: 4 (over z).
Axes of the slice: x: 2, y: 2, z: 4, core: 2. Of those that a mesh axis runs over, the one named last changes fastest.
Arguments:
- hidden: bfloat16 [4, 1024, 1280], P('zero', 'seq'), may hold values from -6 to 6
- output_grad: bfloat16 [4, 1024, 2560], P('zero', 'seq'), may hold values from -6 to 6
- input_weight: bfloat16 [1280, 2856], P('zero'), may hold values from -0.15625 to 0.15625
- step_bias: float32 [40], replicated, may hold values from -7 to -2
- decay_log: float32 [40], replicated, may hold values from -4 to 1
- skip_gain: float32 [40], replicated, may hold values from 0.5 to 1.5
Outputs:
- hidden_grad: bfloat16 [4, 1024, 1280], P('zero', 'seq')
- weight_grad: float32 [1280, 2856], P(('seq', 'zero'))
- head_grads: float32 [3, 40], replicated
The draws below stay inside these ranges and needn't reach their ends.
All inputs are finite; a program needn't handle non-finite values.
Results may differ from the reference program's by a relative error of at most 0.0049.
Values may be sent and summed in bfloat16 or wider, within the bound.
A program may use at most 192 MiB of HBM per device.

```python
import jax
import jax.numpy as jnp
from jax import lax

D = 1280
HEADS = 40
HEAD_DIM = 64
STATE = 128
GROUP = 128
INNER = 2560
PROJ = 2856
LENGTH = 1024
SEQS = 4


def levels(key, shape, split, smallest, top_value):
    loudness = 1.0
    for position, blocks in split:
        steps = jax.random.uniform(jax.random.fold_in(jax.random.fold_in(key, 6), position), (blocks,), jnp.float32, smallest / len(split), top_value / len(split))
        loudness = loudness * jnp.repeat(jnp.exp(steps), shape[position] // blocks).reshape((-1,) + (1,) * (len(shape) - 1 - position))
    return loudness


def normal_values(stream_key, shape, deviation, bound, split=(), dtype=jnp.bfloat16):
    drawn = jax.random.normal(stream_key, shape, jnp.float32) * deviation
    if len(split) > 0:
        drawn = levels(stream_key, shape, split, -0.22, 0.18) * drawn
    return jnp.clip(drawn, min=-bound, max=bound).astype(dtype)


def setup_inputs(seed: int = 0) -> dict:
    seeds = jax.random.split(jax.random.key(seed), 7)
    return {
        "hidden": normal_values(seeds[0], (SEQS, LENGTH, D), 1.0, 6.0, ((0, 4), (1, 8))),
        "output_grad": normal_values(seeds[1], (SEQS, LENGTH, INNER), 1.0, 6.0, ((0, 4), (1, 8))),
        "input_weight": normal_values(seeds[2], (D, PROJ), D ** -0.5, 0.15625, ((0, 4),)),
        "step_bias": jnp.clip(jax.random.uniform(seeds[3], (HEADS,), jnp.float32, -7.0, -2.0), -7.0, -2.0),
        "decay_log": jnp.clip(jax.random.uniform(seeds[4], (HEADS,), jnp.float32, -4.0, 1.0), -4.0, 1.0),
        "skip_gain": jnp.clip(jax.random.uniform(seeds[5], (HEADS,), jnp.float32, 0.5, 1.5), 0.5, 1.5),
    }


highest = lax.Precision.HIGHEST

def state_mixer(columns, step_bias, decay_log, skip_gain, initial):
    length = columns.shape[0]
    blocks = length // GROUP
    values = jax.nn.silu(columns[:, :INNER])
    input_map = jax.nn.silu(columns[:, INNER:INNER + STATE]).reshape(blocks, GROUP, STATE)
    output_map = jax.nn.silu(columns[:, INNER + STATE:INNER + 2 * STATE]).reshape(blocks, GROUP, STATE)
    step_size = jax.nn.softplus(columns[:, INNER + 2 * STATE:] + step_bias)
    log_decay = -jnp.exp(decay_log) * step_size
    head_values = values.reshape(blocks, GROUP, HEADS, HEAD_DIM)
    scaled = head_values * step_size.reshape(blocks, GROUP, HEADS)[:, :, :, None]
    cumulative = jnp.cumsum(log_decay.reshape(blocks, GROUP, HEADS), axis=1)
    causal = (lax.broadcasted_iota(jnp.int32, (GROUP, GROUP), 0) >= lax.broadcasted_iota(jnp.int32, (GROUP, GROUP), 1))[None, :, :, None]
    differences = cumulative[:, :, None, :] - cumulative[:, None, :, :]
    within = jnp.where(causal, jnp.exp(jnp.where(causal, differences, 0.0)), 0.0)
    scores = jnp.einsum('kqn,ksn->kqs', output_map, input_map, precision=highest)
    inside = jnp.einsum('kqsh,kshp->kqhp', scores[:, :, :, None] * within, scaled, precision=highest)
    tail_decay = jnp.exp(cumulative[:, -1:, :] - cumulative)
    group_states = jnp.einsum('kshp,ksn->khpn', scaled * tail_decay[:, :, :, None], input_map, precision=highest)
    totals = cumulative[:, -1, :]

    def advance(running, inputs):
        block_total, block_state = inputs
        return (jnp.exp(block_total)[:, None, None] * running + block_state, running)
    final_state, entering = lax.scan(advance, initial, (totals, group_states))
    from_state = jnp.einsum('kqn,khpn->kqhp', output_map, entering, precision=highest) * jnp.exp(cumulative)[:, :, :, None]
    mixed_out = inside + from_state + skip_gain[None, None, :, None] * head_values
    return (mixed_out.reshape(length, INNER), final_state, lax.optimization_barrier(jnp.sum(totals, axis=0)))

def reference(hidden, output_grad, input_weight, step_bias, decay_log, skip_gain):
    initial = jnp.zeros((HEADS, HEAD_DIM, STATE), jnp.float32)

    def one_sequence(running, inputs):
        weight_sum, head_sum = running
        tokens, cotangent = inputs
        projected = jnp.dot(tokens, input_weight, preferred_element_type=jnp.float32)

        def forward(columns, bias_part, log_part, gain_part):
            return state_mixer(columns, bias_part, log_part, gain_part, initial)[0]
        unused, pullback = jax.vjp(forward, projected, step_bias, decay_log, skip_gain)
        column_grad, bias_grad, log_grad, gain_grad = pullback(cotangent.astype(jnp.float32))
        rounded = column_grad.astype(jnp.bfloat16)
        token_grad = lax.dot_general(rounded, input_weight, (((1,), (1,)), ((), ())), preferred_element_type=jnp.float32).astype(jnp.bfloat16)
        weight_sum = weight_sum + lax.dot_general(tokens, rounded, (((0,), (0,)), ((), ())), preferred_element_type=jnp.float32)
        head_sum = head_sum + jnp.stack([bias_grad, log_grad, gain_grad])
        return ((weight_sum, head_sum), token_grad)
    starting = (jnp.zeros((D, PROJ), jnp.float32), jnp.zeros((3, HEADS), jnp.float32))
    (weight_grad, head_grads), hidden_grad = lax.scan(one_sequence, starting, (hidden, output_grad))
    return (hidden_grad, weight_grad, head_grads)
```

```python
import functools

import jax
import jax.numpy as jnp
from jax import lax
from jax.experimental import pallas as pl
from jax.experimental.pallas import tpu as pltpu
from jax.sharding import PartitionSpec as P

HEAD_DIM = 64
STATE = 128
MESH = pl.DeviceIdType.MESH
F32 = jnp.float32
BF16 = jnp.bfloat16


def up(size, unit):
    return -(-size // unit) * unit


def nn(a, b):
    return lax.dot_general(a, b, (((1,), (0,)), ((), ())), preferred_element_type=F32)


def nt(a, b):
    return lax.dot_general(a, b, (((1,), (1,)), ((), ())), preferred_element_type=F32)


def tn(a, b):
    return lax.dot_general(a, b, (((0,), (0,)), ((), ())), preferred_element_type=F32)


def halves(a):
    high = a.astype(BF16)
    return high, (a - high.astype(F32)).astype(BF16)


def greet(peers):
    barrier = pltpu.get_barrier_semaphore()
    for peer in peers:
        pl.semaphore_signal(barrier, inc=1, device_id=peer, device_id_type=MESH)
    pl.semaphore_wait(barrier, len(peers))


def remote(src, dst, send, recv, peer):
    return pltpu.make_async_remote_copy(src, dst, send, recv, peer, MESH)


def mixer_backward_kernel(
    seqs, zeros, hp,
    hidden, cotangent, weight, bias_in, log_in, gain_in,
    hid, rows_out, head_out,
    window, tiny, cotv, cott,
    toks, tokt, wall, wallt, pre, dys, xs, tails, states, grads, grad, acc, steps, cums, cumt, sigr,
    maps, got_map, part, got_part, sent, tok_in, wbuf, rflow, lflow, zsend, rows_in, hin, hsum, hmine, hall,
    asem, tsem, psem, csem, ssem, msem, dsem, ksem, rsem, gsem, hsem, wsem, loc,
):
    me_s, me_z = lax.axis_index("seq"), lax.axis_index("zero")
    chips = seqs // 2
    chip, core = me_s // 2, lax.rem(me_s, 2)
    sib = me_s // 2 * 2 + 1 - core
    sibling = (sib, me_z)
    length, model = hidden.shape
    rows = weight.shape[0]
    width = wall.shape[1] - STATE
    inner = dys.shape[1]
    slots = acc.shape[1]
    full = cotangent.shape[1]
    chunks, group = seqs, length
    vals, top = STATE, STATE + inner
    up_peer, down_peer = (me_s, me_z + 1), (me_s, me_z - 1)
    half = rows // 2
    last_z = zeros - 1
    pairs = 2 * group

    start = pl.multiple_of(me_s * inner // 128 * 128, 128)
    mine = pl.ds(pl.multiple_of(me_z * rows, rows), rows)
    fetch = [
        pltpu.make_async_copy(weight.at[:, pl.ds(start, window.shape[1])], window, loc.at[0]),
        pltpu.make_async_copy(
            weight.at[:, pl.ds(pl.multiple_of(full + core * STATE, 128), STATE)],
            wall.at[mine, pl.ds(0, STATE)], loc.at[1],
        ),
        pltpu.make_async_copy(weight.at[:, pl.ds(full + 2 * STATE, tiny.shape[1])], tiny, loc.at[2]),
        pltpu.make_async_copy(hidden, toks.at[me_s], loc.at[3]),
        pltpu.make_async_copy(cotangent, cotv, loc.at[4]),
    ]
    for copy in fetch:
        copy.start()
    heads = tiny.shape[1]
    head_row = lax.broadcasted_iota(jnp.int32, (heads, width - top), 0)
    head_col = lax.broadcasted_iota(jnp.int32, (heads, width - top), 1)
    chosen = jnp.logical_and(head_row == me_s * hp + head_col, head_col < hp)
    chosen = jnp.where(chosen, 1.0, 0.0).astype(BF16)
    fetch[2].wait()
    wall[mine, top:width] = nn(tiny[...], chosen).astype(BF16)
    fetch[0].wait()
    if hp % 2:
        shifted = lax.rem(me_s, 2)
        for shift in (0, 1):
            @pl.when(shifted == shift)
            def _():
                wall[mine, vals:top] = window[:, shift * HEAD_DIM : shift * HEAD_DIM + inner]
    else:
        wall[mine, vals:top] = window[...]
    fetch[1].wait()
    fetch[3].wait()

    greet(
        [(lax.rem(me_s + d, seqs), me_z) for d in range(1, seqs)]
        + [(me_s, lax.rem(me_z + d, zeros)) for d in range(1, zeros)]
    )

    def piece(at, p):
        first = pl.multiple_of(at * rows + p * half, half)
        return wall.at[pl.ds(first, half), pl.ds(0, width)]

    def flow(way, h, p, recv):
        at = me_z - h if way == 0 else me_z + h
        return remote(
            piece(at, p), piece(at, p), asem.at[way, 0, h, p], asem.at[way, 1, h + (1 - recv), p],
            up_peer if way == 0 else down_peer,
        )

    def sends(way, h):
        if way == 0:
            return jnp.logical_and(me_z < last_z, me_z >= h)
        return jnp.logical_and(me_z > 0, me_z + h <= last_z)

    def comes(way, h):
        return me_z >= h if way == 0 else me_z + h <= last_z

    def shared(at):
        first = pl.multiple_of(at * rows, rows)
        return remote(
            wall.at[pl.ds(first, rows), pl.ds(0, STATE)],
            wall.at[pl.ds(first, rows), pl.ds(width, STATE)],
            ssem.at[0, at], ssem.at[1, at], sibling,
        )

    for p in (0, 1):
        for way in (0, 1):
            @pl.when(sends(way, 0))
            def _():
                flow(way, 0, p, 0).start()

    def token(src_s, dst, lo, size, slot):
        block = toks.at[src_s, pl.ds(lo, size)]
        return remote(block, block, tsem.at[0, slot], tsem.at[1, slot], (dst, me_z))

    def passed(src_s, slot):
        return remote(toks.at[src_s], toks.at[src_s], psem.at[0, slot], psem.at[1, slot], sibling)

    square = chips == 4
    cut = length // 2
    to_sibling = [passed(me_s, 0)]
    if square:
        flat = chip + 1 - 2 * lax.rem(chip, 2)
        tall = lax.rem(chip + 2, 4)
        far = lax.rem(flat + 2, 4)
        around = [flat, tall]
    else:
        around = [lax.rem(chip + d, chips) for d in range(1, chips)]
    direct = [token(me_s, c * 2 + core, 0, length, i) for i, c in enumerate(around)]
    for copy in direct + to_sibling:
        copy.start()
    shared(me_z).start()

    pre[...] = jnp.zeros_like(pre)
    fetch[4].wait()
    strip = 512

    def turn_cot(j, carry):
        at = pl.ds(pl.multiple_of(j * strip, strip), strip)
        cott[at, :] = cotv[:, at].T
        return carry

    lax.fori_loop(0, full // strip, turn_cot, 0)

    def cot_of(s):
        return cott.at[pl.ds(pl.multiple_of(s * inner, inner), inner)]

    dys[me_s] = cot_of(me_s)[...]

    def step_hop(h):
        for p in (0, 1):
            for way in (0, 1):
                @pl.when(comes(way, h))
                def _():
                    flow(way, h, p, 1).wait_recv()
                if h < last_z:
                    @pl.when(sends(way, h))
                    def _():
                        flow(way, h, p, 0).start()
        for way in (0, 1):
            @pl.when(comes(way, h))
            def _():
                shared(me_z - h if way == 0 else me_z + h).start()

    if zeros > 2:
        step_hop(1)

    if square:
        onward = [
            token(flat * 2 + core, tall * 2 + core, 0, cut, 2),
            token(tall * 2 + core, flat * 2 + core, cut, length - cut, 3),
        ]
        for i in (0, 1):
            direct[i].wait_recv()
            onward[i].start()
        direct += onward
        more = [passed(flat * 2 + core, 1), passed(tall * 2 + core, 2)]
    else:
        more = []
        for d in range(1, chips):
            direct[d - 1].wait_recv()
            more.append(passed(lax.rem(chip - d + chips, chips) * 2 + core, d))
    for copy in more:
        copy.start()
    to_sibling += more

    cots = []
    for d in range(1, seqs):
        peer = lax.rem(me_s + d, seqs)
        cots.append(remote(cot_of(peer), dys.at[me_s], csem.at[0, d], csem.at[1, d], (peer, me_z)))
    for copy in cots:
        copy.start()

    for h in range(2, last_z):
        step_hop(h)

    if square:
        token(far * 2 + core, tall * 2 + core, 0, cut, 2).wait_recv()
        token(far * 2 + core, flat * 2 + core, cut, length - cut, 3).wait_recv()
        to_sibling.append(passed(far * 2 + core, 3))
        to_sibling[-1].start()
    for copy in to_sibling:
        copy.wait_recv()

    def turn(k, carry):
        at = pl.ds(pl.multiple_of(k * group, group), group)
        tokt[:, at] = toks[k].T
        return carry

    lax.fori_loop(0, chunks, turn, 0)

    def project(j):
        shared(j).wait_recv()
        at = pl.ds(pl.multiple_of(j * rows, rows), rows)
        wallt[j] = wall[at, :].T

        def part_of(i, carry):
            cols = pl.ds(pl.multiple_of(i * pairs, pairs), pairs)
            pre[:, cols] += nn(wallt[j], tokt[at, cols])
            return carry

        lax.fori_loop(0, chunks // 2, part_of, 0)

    def near(j, carry):
        distance = jnp.abs(j - me_z)
        ready = distance < last_z if zeros > 1 else distance < 1

        @pl.when(ready)
        def _():
            project(j)
        return carry

    lax.fori_loop(0, zeros, near, 0)
    if zeros > 1:
        step_hop(last_z)
        far_end = jnp.logical_or(me_z == 0, me_z == last_z)

        @pl.when(far_end)
        def _():
            project(last_z - me_z)

    in_at = pl.multiple_of(core * width, 128)
    out_at = pl.multiple_of((1 - core) * width, 128)
    slot = lax.broadcasted_iota(jnp.int32, (slots, heads), 0)
    own_head = jnp.logical_and(
        lax.broadcasted_iota(jnp.int32, (slots, heads), 1) == me_s * hp + slot, slot < hp
    )

    def own(ref):
        return jnp.sum(jnp.where(own_head, ref[...], 0.0), axis=1, keepdims=True)

    bias, rate, gain = own(bias_in), -jnp.exp(own(log_in)), own(gain_in)
    row = lax.broadcasted_iota(jnp.int32, (group, group), 0)
    col = lax.broadcasted_iota(jnp.int32, (group, group), 1)
    causal = col >= row

    def spread(values):
        return jnp.concatenate(
            [jnp.broadcast_to(values[h : h + 1], (HEAD_DIM, values.shape[1])) for h in range(hp)], axis=0
        )

    def gather_rows(whole):
        parts = [
            jnp.sum(whole[h * HEAD_DIM : (h + 1) * HEAD_DIM], axis=0, keepdims=True) for h in range(hp)
        ]
        if slots > hp:
            parts.append(jnp.zeros((slots - hp, whole.shape[1]), F32))
        return jnp.concatenate(parts, axis=0)

    raw = pre[top : top + slots, :] + bias
    soft = jax.nn.softplus(raw)
    curve = jax.nn.sigmoid(raw)
    stacked = jnp.concatenate([soft[:, k * group : (k + 1) * group] for k in range(chunks)], axis=0)
    steps[...] = stacked
    sigr[...] = jnp.concatenate([curve[:, k * group : (k + 1) * group] for k in range(chunks)], axis=0)
    logs = jnp.concatenate([rate] * chunks, axis=0) * stacked
    before = jnp.where(causal, 1.0, 0.0).astype(BF16)
    after = jnp.where(col <= row, 1.0, 0.0).astype(BF16)

    def summed(values, mask):
        a = values.astype(BF16)
        rest = values - a.astype(F32)
        b = rest.astype(BF16)
        c = (rest - b.astype(F32)).astype(BF16)
        return nn(a, mask) + (nn(b, mask) + nn(c, mask))

    cums[...] = summed(logs, before)

    grad[...] = jnp.zeros_like(grad)

    def small(ref, k):
        return ref[pl.ds(pl.multiple_of(k * slots, slots), slots), :]

    def forward(k, carry):
        at = pl.ds(pl.multiple_of(k * group, group), group)
        p = pre[vals:top, at]
        sig = jax.nn.sigmoid(p)
        x = p * sig
        xs[k] = x
        pre[vals:top, at] = sig * (1.0 + p * (1.0 - sig))
        step, cum = small(steps, k), small(cums, k)
        last = cum[:, group - 1 :]
        m_in = pre[pl.ds(in_at, STATE), at]
        in16 = (m_in * jax.nn.sigmoid(m_in)).astype(BF16)
        tail16 = (x * spread(step * jnp.exp(last - cum))).astype(BF16)
        tails[k] = tail16
        cumt[k] = jnp.concatenate([cum, jnp.zeros((group - slots, group), F32)], axis=0).T
        held = grad[...]
        states[k] = held.astype(BF16)
        grad[...] = spread(jnp.exp(jnp.broadcast_to(last, (slots, STATE)))) * held + nt(tail16, in16)
        return carry

    lax.fori_loop(0, chunks, forward, 0)
    states[chunks] = grad[...].astype(BF16)
    grad[...] = jnp.zeros_like(grad)
    acc[...] = jnp.zeros_like(acc)
    gain_full = spread(jnp.broadcast_to(gain, (slots, group)))
    grads[pl.ds(top, width - top), :] = jnp.zeros((width - top, chunks * group), BF16)
    for copy in cots:
        copy.wait_recv()

    def map_copy(k):
        return remote(maps.at[1 - core, k], got_map.at[k], msem.at[0, k], msem.at[1, k], sibling)

    def backward(n, carry):
        k = chunks - 1 - n
        at = pl.ds(pl.multiple_of(k * group, group), group)
        step, cum = small(steps, k), small(cums, k)
        last = cum[:, group - 1 :]
        x = xs[k]
        step_full = spread(step)
        u16 = (x * step_full).astype(BF16)
        tail16 = tails[k]
        m_in, m_out = pre[pl.ds(in_at, STATE), at], pre[pl.ds(out_at, STATE), at]
        s_in, s_out = jax.nn.sigmoid(m_in), jax.nn.sigmoid(m_out)
        in16, out16 = (m_in * s_in).astype(BF16), (m_out * s_out).astype(BF16)
        dy16 = dys[k]
        dy = dy16.astype(F32)
        tail = spread(jnp.exp(last - cum))
        lead = spread(jnp.exp(cum))
        leave = spread(jnp.exp(jnp.broadcast_to(last, (slots, STATE))))
        held16 = states[k]
        g_out = grad[...]
        g16 = g_out.astype(BF16)
        dy_lead = dy * lead
        lead16 = dy_lead.astype(BF16)

        score = tn(in16, out16)
        cum_col = cumt[k]
        d_score = jnp.zeros((group, group), F32)
        du_parts, r_parts = [], []
        for h in range(hp):
            at_h = slice(h * HEAD_DIM, (h + 1) * HEAD_DIM)
            diff = cum[h : h + 1] - cum_col[:, h : h + 1]
            within = jnp.exp(jnp.where(causal, diff, -1e30))
            mixing = (score * within).astype(BF16)
            d_mix = tn(u16[at_h], dy16[at_h])
            du_parts.append(nt(dy16[at_h], mixing))
            d_score = d_score + d_mix * within
            r_parts.append(jnp.sum(d_mix * mixing.astype(F32), axis=0, keepdims=True))
        if slots > hp:
            r_parts.append(jnp.zeros((slots - hp, group), F32))
        du = jnp.concatenate(du_parts, axis=0) + nn(g16, in16) * tail
        from_x = gather_rows(du * x)
        from_u = gather_rows(du * u16.astype(F32))
        lead_rows = gather_rows(dy_lead * nn(held16, out16))
        cross = jnp.sum(gather_rows(g_out * states[k + 1].astype(F32)), axis=1, keepdims=True)
        d_cum = jnp.concatenate(r_parts, axis=0) + lead_rows - from_u
        d_log = summed(d_cum, after) + cross
        d_raw = (from_x + rate * d_log) * small(sigr, k)

        d_score16 = d_score.astype(BF16)
        d_out = nn(in16, d_score16) + tn(held16, lead16)
        d_in = nt(out16, d_score16) + tn(g16, tail16)
        grad[...] = leave * g_out + nt(lead16, out16)

        d_in = d_in * (s_in * (1.0 + m_in * (1.0 - s_in)))
        d_out = d_out * (s_out * (1.0 + m_out * (1.0 - s_out)))
        grads[vals:top, at] = ((du * step_full + dy * gain_full) * pre[vals:top, at]).astype(BF16)
        grads[pl.ds(in_at, STATE), at] = d_in.astype(BF16)
        grads[pl.ds(out_at, STATE), at] = d_out.astype(BF16)
        fill = jnp.zeros((16 - slots, group), F32)
        grads[top : top + 16, at] = jnp.concatenate([d_raw, fill], axis=0).astype(BF16)
        maps[0, k] = d_in
        maps[1, k] = d_out
        acc[0] += d_raw
        acc[1] += d_log * (rate * step)
        acc[2] += gather_rows(dy * x)
        map_copy(k).start()
        return carry

    lax.fori_loop(0, chunks, backward, 0)

    block = wbuf.shape[3]
    many = 4 if seqs % 4 == 0 else 2
    span = many * zeros * block

    def merge(k, carry):
        map_copy(k).wait_recv()
        at = pl.ds(pl.multiple_of(k * group, group), group)
        got_map[k] = maps[core, k] + got_map[k]
        return carry

    lax.fori_loop(0, chunks, merge, 0)
    own_map = jnp.concatenate([got_map[k].astype(BF16) for k in range(chunks)], axis=1)

    def weigh(q, carry):
        at = pl.ds(pl.multiple_of(q * span, span), span)
        product = jnp.concatenate(
            [nt(tokt[at, :], own_map), nt(tokt[at, :], grads[vals:width, :])], axis=1
        )
        for a in range(many):
            for t in range(zeros):
                first = (a * zeros + t) * block
                wbuf[t, a % 2, q * (many // 2) + a // 2] = product[first : first + block].astype(BF16)
        return carry

    lax.fori_loop(0, seqs // many, weigh, 0)

    def back_flow(way, t, p):
        landed = rflow if way == 0 else lflow
        peer = up_peer if way == 0 else down_peer
        return remote(wbuf.at[t, p], landed.at[t, p], rsem.at[way, 0, t, p], rsem.at[way, 1, t, p], peer)

    for z, way in ((0, 0), (last_z, 1)):
        if zeros > 1:
            @pl.when(me_z == z)
            def _():
                for i in range(last_z):
                    for p in (0, 1):
                        back_flow(way, last_z - i if way == 0 else i, p).start()

    wide_head = hmine.shape[1]
    place_row = lax.broadcasted_iota(jnp.int32, (slots, wide_head), 0)
    place = jnp.logical_and(
        lax.broadcasted_iota(jnp.int32, (slots, wide_head), 1) == me_s * hp + place_row, place_row < hp
    )
    lines = [
        jnp.sum(
            jnp.where(place, jnp.sum(acc[i], axis=1, keepdims=True), 0.0), axis=0, keepdims=True
        )
        for i in range(3)
    ]
    hmine[...] = jnp.concatenate(lines + [jnp.zeros((5, wide_head), F32)], axis=0)
    hin[me_z] = hmine[...]

    def head_copy(d):
        return remote(
            hmine, hin.at[me_z], hsem.at[0, d], hsem.at[1, d], (me_s, lax.rem(me_z + d, zeros))
        )

    for d in range(1, zeros):
        head_copy(d).start()

    def turn_of(n):
        return lax.rem(chip + 1 + n, chips)

    def give(i):
        return remote(part.at[i, 1 - core], got_part.at[i], dsem.at[0, i], dsem.at[1, i], sibling)

    def token_send(i):
        return remote(
            sent.at[i], tok_in.at[chip], ksem.at[0, i], ksem.at[1, chip], (i * 2 + core, me_z)
        )

    def settle(n):
        i = turn_of(n)
        give(i).wait_recv()

        def add(j, carry):
            at = pl.ds(pl.multiple_of(j * 128, 128), 128)
            sent[i, at, :] = (part[i, core, at, :] + got_part[i, at, :]).astype(BF16)
            return carry

        lax.fori_loop(0, model // 128, add, 0)

        @pl.when(i != chip)
        def _():
            token_send(i).start()

    def back_project(n, carry):
        i = turn_of(n)
        cols = pl.ds(pl.multiple_of(i * pairs, pairs), pairs)

        def strip_of(j, inner_carry):
            at = pl.ds(pl.multiple_of(j * (model // 2), model // 2), model // 2)
            product = nn(wall[at, :], grads[:, cols])
            part[i, 0, at, :] = product[:, :group]
            part[i, 1, at, :] = product[:, group:]
            return inner_carry

        lax.fori_loop(0, 2, strip_of, 0)
        give(i).start()

        @pl.when(n > 0)
        def _():
            settle(n - 1)
        return carry

    lax.fori_loop(0, chips, back_project, 0)
    settle(chips - 1)

    def along(s):
        return remote(
            zsend.at[s], rows_in.at[me_s], wsem.at[0, s], wsem.at[1, me_s], (s, me_z)
        )

    def events(z):
        found = []
        for i in range(last_z):
            for p in (0, 1):
                for way in (0, 1):
                    t = last_z - i if way == 0 else i
                    if (way == 0 and 0 < z < t) or (way == 1 and t < z < last_z):
                        hops = z if way == 0 else last_z - z
                        found.append((2 * i + p + 3 * hops, p, way, t))
        return sorted(found)

    for z in range(zeros):
        @pl.when(me_z == z)
        def _():
            for _, p, way, t in events(z):
                landed = rflow if way == 0 else lflow
                back_flow(way, t, p).wait_recv()

                def add(j, carry):
                    wbuf[t, p, j] = (wbuf[t, p, j].astype(F32) + landed[t, p, j].astype(F32)).astype(BF16)
                    return carry

                lax.fori_loop(0, seqs // 2, add, 0)
                back_flow(way, t, p).start()
            for p in (0, 1):
                if z > 0:
                    back_flow(0, z, p).wait_recv()
                if z < last_z:
                    back_flow(1, z, p).wait_recv()

                def close(j, carry):
                    value = wbuf[z, p, j].astype(F32)
                    if z > 0:
                        value = value + rflow[z, p, j].astype(F32)
                    if z < last_z:
                        value = value + lflow[z, p, j].astype(F32)
                    zsend[2 * j + p] = value.astype(BF16)
                    return carry

                lax.fori_loop(0, seqs // 2, close, 0)
                for j in range(seqs // 2):
                    @pl.when(me_s != 2 * j + p)
                    def _():
                        along(2 * j + p).start()

    rows_in[me_s] = zsend[me_s]
    for d in range(1, zeros):
        head_copy(d).wait_recv()
    sums = hin[0]
    for d in range(1, zeros):
        sums = sums + hin[d]
    hsum[...] = sums
    hall[me_s] = sums

    def head_along(d):
        return remote(
            hsum, hall.at[me_s], gsem.at[0, d], gsem.at[1, d], (lax.rem(me_s + d, seqs), me_z)
        )

    for d in range(1, seqs):
        head_along(d).start()

    for d in range(1, chips):
        at = lax.rem(chip + d, chips)
        remote(
            sent.at[at], tok_in.at[at], ksem.at[0, at], ksem.at[1, at], (at * 2 + core, me_z)
        ).wait_recv()
    tok_in[chip] = sent[chip]

    def finish(j, carry):
        at = pl.ds(pl.multiple_of(j * 128, 128), 128)
        value = tok_in[0, at, :].astype(F32)
        for c in range(1, chips):
            value = value + tok_in[c, at, :].astype(F32)
        hid[:, at] = value.T.astype(BF16)
        return carry

    lax.fori_loop(0, model // 128, finish, 0)

    for d in range(1, seqs):
        at = lax.rem(me_s + d, seqs)
        remote(
            zsend.at[at], rows_in.at[at], wsem.at[0, at], wsem.at[1, at], (at, me_z)
        ).wait_recv()
        head_along(d).wait_recv()
    map_sums = [jnp.zeros((block, STATE), F32), jnp.zeros((block, STATE), F32)]
    for s in range(seqs):
        piece_in = rows_in[s].astype(F32)
        rows_out[:, s * inner : (s + 1) * inner] = piece_in[:, vals:top]
        rows_out[:, full + 2 * STATE + s * hp : full + 2 * STATE + (s + 1) * hp] = piece_in[:, top : top + hp]
        map_sums[s % 2] = map_sums[s % 2] + piece_in[:, :STATE]
    rows_out[:, full : full + 2 * STATE] = jnp.concatenate(map_sums, axis=1)
    sums = hall[0]
    for s in range(1, seqs):
        sums = sums + hall[s]
    head_out[...] = sums[:3, :heads]

    for p in (0, 1):
        for way in (0, 1):
            for h in range(last_z):
                @pl.when(sends(way, h))
                def _():
                    flow(way, h, p, 0).wait_send()
            for t in range(zeros):
                ahead = me_z < t if way == 0 else me_z > t

                @pl.when(ahead)
                def _():
                    back_flow(way, t, p).wait_send()
    for j in range(zeros):
        shared(j).wait_send()
    for copy in direct + to_sibling + cots:
        copy.wait_send()
    for k in range(chunks):
        map_copy(k).wait_send()
    for i in range(chips):
        give(i).wait_send()

        @pl.when(i != chip)
        def _():
            token_send(i).wait_send()
    for d in range(1, zeros):
        head_copy(d).wait_send()
    for d in range(1, seqs):
        head_along(d).wait_send()
    for s in range(seqs):
        @pl.when(me_s != s)
        def _():
            along(s).wait_send()


def mixer_backward(hidden, cotangent, weight, bias, log, gain, seqs, zeros, hp):
    length, model = hidden.shape
    rows = weight.shape[0]
    heads = bias.shape[1]
    inner = hp * HEAD_DIM
    slots = up(hp, 8)
    width = up(STATE + inner + 16, 128)
    block = rows // seqs
    chips = seqs // 2
    wide = width + STATE
    total = seqs * length
    full = seqs * inner
    span = up(inner + (HEAD_DIM if hp % 2 else 0), 128)
    lanes = up(heads, 128)
    dma = pltpu.SemaphoreType.DMA
    vmem = pl.BlockSpec(memory_space=pltpu.VMEM)
    anywhere = pl.BlockSpec(memory_space=pl.ANY)
    return pl.pallas_call(
        functools.partial(mixer_backward_kernel, seqs, zeros, hp),
        out_shape=(
            jax.ShapeDtypeStruct((length, model), BF16),
            jax.ShapeDtypeStruct((block, full + 2 * STATE + heads), F32),
            jax.ShapeDtypeStruct((3, heads), F32),
        ),
        in_specs=[anywhere] * 3 + [vmem] * 3,
        out_specs=(vmem,) * 3,
        scratch_shapes=[
            pltpu.VMEM((rows, span), BF16),
            pltpu.VMEM((rows, heads), BF16),
            pltpu.VMEM((length, full), BF16),
            pltpu.VMEM((full, length), BF16),
            pltpu.VMEM((seqs, length, model), BF16),
            pltpu.VMEM((model, total), BF16),
            pltpu.VMEM((model, wide), BF16),
            pltpu.VMEM((zeros, wide, rows), BF16),
            pltpu.VMEM((wide, total), F32),
            pltpu.VMEM((seqs, inner, length), BF16),
            pltpu.VMEM((seqs, inner, length), F32),
            pltpu.VMEM((seqs, inner, length), BF16),
            pltpu.VMEM((seqs + 1, inner, STATE), BF16),
            pltpu.VMEM((wide, total), BF16),
            pltpu.VMEM((inner, STATE), F32),
            pltpu.VMEM((3, slots, length), F32),
            pltpu.VMEM((seqs * slots, length), F32),
            pltpu.VMEM((seqs * slots, length), F32),
            pltpu.VMEM((seqs, length, length), F32),
            pltpu.VMEM((seqs * slots, length), F32),
            pltpu.VMEM((2, seqs, STATE, length), F32),
            pltpu.VMEM((seqs, STATE, length), F32),
            pltpu.VMEM((chips, 2, model, length), F32),
            pltpu.VMEM((chips, model, length), F32),
            pltpu.VMEM((chips, model, length), BF16),
            pltpu.VMEM((chips, model, length), BF16),
            pltpu.VMEM((zeros, 2, seqs // 2, block, width), BF16),
            pltpu.VMEM((zeros, 2, seqs // 2, block, width), BF16),
            pltpu.VMEM((zeros, 2, seqs // 2, block, width), BF16),
            pltpu.VMEM((seqs, block, width), BF16),
            pltpu.VMEM((seqs, block, width), BF16),
            pltpu.VMEM((zeros, 8, lanes), F32),
            pltpu.VMEM((8, lanes), F32),
            pltpu.VMEM((8, lanes), F32),
            pltpu.VMEM((seqs, 8, lanes), F32),
            dma((2, 2, zeros + 1, 2)),
            dma((2, seqs)),
            dma((2, seqs)),
            dma((2, seqs)),
            dma((2, zeros)),
            dma((2, seqs)),
            dma((2, chips)),
            dma((2, chips)),
            dma((2, 2, zeros, 2)),
            dma((2, seqs)),
            dma((2, zeros)),
            dma((2, seqs)),
            dma((5,)),
        ],
        compiler_params=pltpu.CompilerParams(
            collective_id=0, has_side_effects=True, vmem_limit_bytes=60 * 1024 * 1024
        ),
        name="mixer_backward",
    )(hidden, cotangent, weight, bias, log, gain)


def body(seqs, zeros, hidden, output_grad, input_weight, step_bias, decay_log, skip_gain):
    heads = step_bias.shape[0]
    hp = up(heads, seqs) // seqs
    spare = seqs * hp - heads
    full, total = heads * HEAD_DIM, seqs * hp * HEAD_DIM
    tokens, cot, weight = hidden[0], output_grad[0], input_weight
    params = [step_bias, decay_log, skip_gain]
    if spare:
        cot = jnp.pad(cot, ((0, 0), (0, total - full)))
        gap = jnp.zeros((weight.shape[0], total - full), BF16)
        few = jnp.zeros((weight.shape[0], spare), BF16)
        weight = jnp.concatenate([weight[:, :full], gap, weight[:, full:], few], axis=1)
        params = [jnp.pad(v, (0, spare)) for v in params]
    token_grad, weight_grad, head_grads = mixer_backward(
        tokens, cot, weight, *[v[None] for v in params], seqs, zeros, hp
    )
    if spare:
        weight_grad = jnp.concatenate(
            [weight_grad[:, :full], weight_grad[:, total : total + 2 * STATE + heads]], axis=1
        )
        head_grads = head_grads[:, :heads]
    return (token_grad[None], weight_grad, head_grads)


def solution(mesh):
    placed = (P("zero", "seq", None), P("zero", "seq", None), P("zero", None), P(), P(), P())
    return jax.shard_map(
        functools.partial(body, mesh.shape["seq"], mesh.shape["zero"]),
        mesh=mesh,
        in_specs=placed,
        out_specs=(P("zero", "seq", None), P(("seq", "zero"), None), P()),
        check_vma=False,
    )
```

```python
import functools

import jax
import jax.numpy as jnp
from jax import lax
from jax.experimental import pallas as pl
from jax.experimental.pallas import tpu as pltpu
from jax.sharding import PartitionSpec as P

HEAD_DIM = 64
STATE = 128
MESH = pl.DeviceIdType.MESH
F32 = jnp.float32
BF16 = jnp.bfloat16


def up(size, unit):
    return -(-size // unit) * unit


def nn(a, b):
    return lax.dot_general(a, b, (((1,), (0,)), ((), ())), preferred_element_type=F32)


def nt(a, b):
    return lax.dot_general(a, b, (((1,), (1,)), ((), ())), preferred_element_type=F32)


def tn(a, b):
    return lax.dot_general(a, b, (((0,), (0,)), ((), ())), preferred_element_type=F32)


def halves(a):
    high = a.astype(BF16)
    return high, (a - high.astype(F32)).astype(BF16)


def remote(src, dst, send, recv, peer):
    return pltpu.make_async_remote_copy(src, dst, send, recv, peer, MESH)


def groups_of(hp):
    first = hp - hp // 2
    second = hp - first
    return (first, up(first * HEAD_DIM + 16, 128)), (second, up(second * HEAD_DIM, 128))


def mixer_backward_kernel(
    seqs, zeros, hp,
    hidden, cotangent, weight, bias_in, log_in, gain_in,
    hid, rows_out, head_out,
    window, tiny, cotv, cott,
    toks, tokt, wall, wallt, pre, dys, xs, tails, states, grads, grad, acc, steps, cums, cumt, sigr,
    maps, got_map, part, got_part, sent, tok_in, wbuf, rflow, lflow, zsend, rows_in, hin, hsum, hmine, hall,
    ins, outs, scores, swbuf, swin, stsend, stin,
    asem, tsem, psem, csem, ssem, msem, dsem, ksem, rsem, gsem, hsem, wsem, loc, ysem, xsem,
):
    me_s, me_z = lax.axis_index("seq"), lax.axis_index("zero")
    chips = seqs // 2
    chip, core = me_s // 2, lax.rem(me_s, 2)
    sib = me_s // 2 * 2 + 1 - core
    sibling = (sib, me_z)
    length, model = hidden.shape
    rows = weight.shape[0]
    wide = wall.shape[1]
    inner = dys.shape[1]
    (n1, w1), (n2, w2) = groups_of(hp)
    in1, in2 = n1 * HEAD_DIM, n2 * HEAD_DIM
    slots = acc.shape[1]
    full = cotangent.shape[1]
    chunks, group = seqs, length
    v1 = 2 * STATE
    top, v2 = v1 + in1, v1 + w1
    extra = wide
    up_peer, down_peer = (me_s, me_z + 1), (me_s, me_z - 1)
    half = rows // 2
    last_z = zeros - 1
    pairs = 2 * group

    peers = [(lax.rem(me_s + d, seqs), me_z) for d in range(1, seqs)]
    peers += [(me_s, lax.rem(me_z + d, zeros)) for d in range(1, zeros)]
    barrier = pltpu.get_barrier_semaphore()
    for peer in peers:
        pl.semaphore_signal(barrier, inc=1, device_id=peer, device_id_type=MESH)

    start = pl.multiple_of(me_s * inner // 128 * 128, 128)
    mine = pl.ds(pl.multiple_of(me_z * rows, rows), rows)
    fetch = [
        pltpu.make_async_copy(weight.at[:, pl.ds(start, window.shape[1])], window, loc.at[0]),
        pltpu.make_async_copy(
            weight.at[:, pl.ds(pl.multiple_of(full + core * STATE, 128), STATE)],
            wall.at[mine, pl.ds(STATE, STATE)], loc.at[1],
        ),
        pltpu.make_async_copy(weight.at[:, pl.ds(full + 2 * STATE, tiny.shape[1])], tiny, loc.at[2]),
        pltpu.make_async_copy(hidden, toks.at[me_s], loc.at[3]),
        pltpu.make_async_copy(cotangent, cotv, loc.at[4]),
    ]
    for copy in fetch:
        copy.start()
    heads = tiny.shape[1]
    head_row = lax.broadcasted_iota(jnp.int32, (heads, v2 - top), 0)
    head_col = lax.broadcasted_iota(jnp.int32, (heads, v2 - top), 1)
    chosen = jnp.logical_and(head_row == me_s * hp + head_col, head_col < hp)
    chosen = jnp.where(chosen, 1.0, 0.0).astype(BF16)
    fetch[2].wait()
    wall[mine, top:v2] = nn(tiny[...], chosen).astype(BF16)
    fetch[0].wait()
    def place_values(shift):
        wall[mine, v1:top] = window[:, shift : shift + in1]
        wall[mine, v2 : v2 + in2] = window[:, shift + in1 : shift + inner]
        if w2 > in2:
            wall[mine, v2 + in2 : v2 + w2] = jnp.zeros((rows, w2 - in2), BF16)

    if hp % 2:
        shifted = lax.rem(me_s, 2)
        for shift in (0, 1):
            @pl.when(shifted == shift)
            def _():
                place_values(shift * HEAD_DIM)
    else:
        place_values(0)
    fetch[1].wait()
    fetch[3].wait()

    pl.semaphore_wait(barrier, len(peers))

    spans = ((STATE, STATE + w1), (v2, w2))

    def piece(g, at, p):
        first = pl.multiple_of(at * rows + p * half, half)
        return wall.at[pl.ds(first, half), pl.ds(*spans[g])]

    def flow(g, way, h, p, recv):
        at = me_z - h if way == 0 else me_z + h
        return remote(
            piece(g, at, p), piece(g, at, p),
            asem.at[g, way, 0, h, p], asem.at[g, way, 1, h + (1 - recv), p],
            up_peer if way == 0 else down_peer,
        )

    def sends(way, h):
        if way == 0:
            return jnp.logical_and(me_z < last_z, me_z >= h)
        return jnp.logical_and(me_z > 0, me_z + h <= last_z)

    def comes(way, h):
        return me_z >= h if way == 0 else me_z + h <= last_z

    def shared(at):
        first = pl.multiple_of(at * rows, rows)
        return remote(
            wall.at[pl.ds(first, rows), pl.ds(STATE, STATE)],
            wall.at[pl.ds(first, rows), pl.ds(0, STATE)],
            ssem.at[0, at], ssem.at[1, at], sibling,
        )

    for p in (0, 1):
        for way in (0, 1):
            @pl.when(sends(way, 0))
            def _():
                flow(0, way, 0, p, 0).start()

    def own_late(h):
        for way in (0, 1):
            distance = me_z if way == 0 else last_z - me_z

            @pl.when(jnp.logical_and(distance == h, sends(way, 0)))
            def _():
                for p in (0, 1):
                    flow(1, way, 0, p, 0).start()

    own_late(0)

    def token(src_s, dst, lo, size, slot):
        block = toks.at[src_s, pl.ds(lo, size)]
        return remote(block, block, tsem.at[0, slot], tsem.at[1, slot], (dst, me_z))

    def passed(src_s, slot):
        return remote(toks.at[src_s], toks.at[src_s], psem.at[0, slot], psem.at[1, slot], sibling)

    square = chips == 4
    cut = length // 2
    to_sibling = [passed(me_s, 0)]
    if square:
        flat = chip + 1 - 2 * lax.rem(chip, 2)
        tall = lax.rem(chip + 2, 4)
        far = lax.rem(flat + 2, 4)
        around = [flat, tall]
    else:
        around = [lax.rem(chip + d, chips) for d in range(1, chips)]
    direct = [token(me_s, c * 2 + core, 0, length, i) for i, c in enumerate(around)]
    for copy in direct + to_sibling:
        copy.start()
    shared(me_z).start()

    pre[...] = jnp.zeros_like(pre)
    fetch[4].wait()
    strip = 512

    def turn_cot(j, carry):
        at = pl.ds(pl.multiple_of(j * strip, strip), strip)
        cott[at, :] = cotv[:, at].T
        return carry

    lax.fori_loop(0, full // strip, turn_cot, 0)

    def cot_of(s):
        return cott.at[pl.ds(pl.multiple_of(s * inner, inner), inner)]

    dys[me_s] = cot_of(me_s)[...]

    def step_hop(h):
        for p in (0, 1):
            for way in (0, 1):
                @pl.when(comes(way, h))
                def _():
                    flow(0, way, h, p, 1).wait_recv()
                if h < last_z:
                    @pl.when(sends(way, h))
                    def _():
                        flow(0, way, h, p, 0).start()
        if h < last_z:
            own_late(h)
        for way in (0, 1):
            @pl.when(comes(way, h))
            def _():
                shared(me_z - h if way == 0 else me_z + h).start()

    def late_hop(h, onward):
        for p in (0, 1):
            for way in (0, 1):
                goes = sends(way, h) if h < last_z else jnp.bool_(False)
                if onward:
                    if h < last_z:
                        @pl.when(goes)
                        def _():
                            flow(1, way, h, p, 1).wait_recv()
                            flow(1, way, h, p, 0).start()
                else:
                    @pl.when(jnp.logical_and(comes(way, h), jnp.logical_not(goes)))
                    def _():
                        flow(1, way, h, p, 1).wait_recv()

    if zeros > 2:
        step_hop(1)

    def chip_of(n):
        if square:
            return lax.rem(chip // 2 + n // 2, 2) * 2 + lax.rem(lax.rem(chip, 2) + n % 2, 2)
        return lax.rem(chip + n, chips)

    def turn(n, carry):
        for half_chip in (0, 1):
            k = chip_of(n) * 2 + half_chip
            tokt[:, pl.ds(pl.multiple_of(k * group, group), group)] = toks[k].T
        return carry

    early = 3 if square else 0
    if square:
        onward = [
            token(flat * 2 + core, tall * 2 + core, 0, cut, 2),
            token(tall * 2 + core, flat * 2 + core, cut, length - cut, 3),
        ]
        for i in (0, 1):
            direct[i].wait_recv()
            onward[i].start()
        direct += onward
        more = [passed(flat * 2 + core, 1), passed(tall * 2 + core, 2)]
        for copy in more:
            copy.start()
        to_sibling += more
        for copy in to_sibling:
            copy.wait_recv()
        lax.fori_loop(0, early, turn, 0)

    for h in range(2, last_z):
        step_hop(h)

    def flip(j):
        shared(j).wait_recv()
        wallt[j] = wall[pl.ds(pl.multiple_of(j * rows, rows), rows), :v2].T

    def project(j, first, final):
        def part_of(n, carry):
            at = pl.ds(pl.multiple_of(j * rows, rows), rows)
            cols = pl.ds(pl.multiple_of(chip_of(n) * pairs, pairs), pairs)
            pre[:v2, cols] += nn(wallt[j], tokt[at, cols])
            return carry

        lax.fori_loop(first, final, part_of, 0)

    def near(first, final, fresh):
        def one(j, carry):
            distance = jnp.abs(j - me_z)
            ready = distance < last_z if zeros > 1 else distance < 1

            @pl.when(ready)
            def _():
                if fresh:
                    flip(j)
                project(j, first, final)
            return carry

        lax.fori_loop(0, zeros, one, 0)

    if early:
        near(0, early, True)

    if square:
        token(far * 2 + core, tall * 2 + core, 0, cut, 2).wait_recv()
        token(far * 2 + core, flat * 2 + core, cut, length - cut, 3).wait_recv()
        rest = [passed(far * 2 + core, 3)]
    else:
        rest = []
        for d in range(1, chips):
            direct[d - 1].wait_recv()
            rest.append(passed(lax.rem(chip - d + chips, chips) * 2 + core, d))
    for copy in rest:
        copy.start()
    cots = []
    for d in range(1, seqs):
        peer = lax.rem(me_s + d, seqs)
        cots.append(remote(cot_of(peer), dys.at[me_s], csem.at[0, d], csem.at[1, d], (peer, me_z)))
    for copy in cots:
        copy.start()
    if not square:
        rest = to_sibling + rest
    for copy in rest:
        copy.wait_recv()
    to_sibling = to_sibling + rest if square else rest
    lax.fori_loop(early, chips, turn, 0)
    near(early, chips, not early)

    batch = 4 * group if chunks % 4 == 0 else pairs

    if zeros > 2:
        late_hop(1, True)
    if zeros > 1:
        step_hop(last_z)
        far_end = jnp.logical_or(me_z == 0, me_z == last_z)

        @pl.when(far_end)
        def _():
            flip(last_z - me_z)
            project(last_z - me_z, 0, chips)

    in_at = pl.multiple_of((1 - core) * STATE, 128)
    out_at = pl.multiple_of(core * STATE, 128)
    slot = lax.broadcasted_iota(jnp.int32, (slots, heads), 0)
    own_head = jnp.logical_and(
        lax.broadcasted_iota(jnp.int32, (slots, heads), 1) == me_s * hp + slot, slot < hp
    )

    def own(ref):
        return jnp.sum(jnp.where(own_head, ref[...], 0.0), axis=1, keepdims=True)

    bias, rate, gain = own(bias_in), -jnp.exp(own(log_in)), own(gain_in)
    row = lax.broadcasted_iota(jnp.int32, (group, group), 0)
    col = lax.broadcasted_iota(jnp.int32, (group, group), 1)
    causal = col >= row

    def spread(values, span):
        return jnp.concatenate(
            [jnp.broadcast_to(values[h : h + 1], (HEAD_DIM, values.shape[1])) for h in span], axis=0
        )

    def gather_rows(whole, span):
        parts = [
            jnp.sum(whole[i * HEAD_DIM : (i + 1) * HEAD_DIM], axis=0, keepdims=True)
            for i in range(len(span))
        ]
        return padded(parts, span)

    def padded(parts, span):
        lanes = parts[0].shape[1]
        if span[0] > 0:
            parts = [jnp.zeros((span[0], lanes), F32)] + parts
        if slots > span[-1] + 1:
            parts = parts + [jnp.zeros((slots - span[-1] - 1, lanes), F32)]
        return jnp.concatenate(parts, axis=0)

    raw = pre[top : top + slots, :] + bias
    soft = jax.nn.softplus(raw)
    curve = jax.nn.sigmoid(raw)
    stacked = jnp.concatenate([soft[:, k * group : (k + 1) * group] for k in range(chunks)], axis=0)
    steps[...] = stacked
    sigr[...] = jnp.concatenate([curve[:, k * group : (k + 1) * group] for k in range(chunks)], axis=0)
    logs = jnp.concatenate([rate] * chunks, axis=0) * stacked
    before = jnp.where(causal, 1.0, 0.0).astype(BF16)
    after = jnp.where(col <= row, 1.0, 0.0).astype(BF16)

    def summed(values, mask):
        a = values.astype(BF16)
        rest = values - a.astype(F32)
        b = rest.astype(BF16)
        c = (rest - b.astype(F32)).astype(BF16)
        return nn(a, mask) + (nn(b, mask) + nn(c, mask))

    cums[...] = summed(logs, before)

    def small(ref, k):
        return ref[pl.ds(pl.multiple_of(k * slots, slots), slots), :]

    def forward(g, k):
        span, mine_v, size = (range(n1), v1, in1) if g == 0 else (range(n1, hp), v2, in2)
        here = slice(span[0] * HEAD_DIM, span[0] * HEAD_DIM + size)
        at = pl.ds(pl.multiple_of(k * group, group), group)
        p = pre[mine_v : mine_v + size, at]
        sig = jax.nn.sigmoid(p)
        x = p * sig
        xs[k, here] = x
        pre[mine_v : mine_v + size, at] = sig * (1.0 + p * (1.0 - sig))
        step, cum = small(steps, k), small(cums, k)
        last = cum[:, group - 1 :]
        if g == 0:
            m_in, m_out = pre[pl.ds(in_at, STATE), at], pre[pl.ds(out_at, STATE), at]
            in16 = (m_in * jax.nn.sigmoid(m_in)).astype(BF16)
            out16 = (m_out * jax.nn.sigmoid(m_out)).astype(BF16)
            ins[k] = in16
            outs[k] = out16
            scores[k] = tn(in16, out16)
            cumt[k] = jnp.concatenate([cum, jnp.zeros((group - slots, group), F32)], axis=0).T
        else:
            in16 = ins[k]
        tail16 = (x * spread(step * jnp.exp(last - cum), span)).astype(BF16)
        tails[k, here] = tail16
        held = grad[here]
        states[k, here] = held.astype(BF16)
        leave = spread(jnp.exp(jnp.broadcast_to(last, (slots, STATE))), span)
        grad[here] = leave * held + nt(tail16, in16)

    def map_copy(k):
        return remote(maps.at[1 - core, k], got_map.at[k], msem.at[0, k], msem.at[1, k], sibling)

    def backward(g, k):
        span, mine_v, size = (range(n1), v1, in1) if g == 0 else (range(n1, hp), v2, in2)
        here = slice(span[0] * HEAD_DIM, span[0] * HEAD_DIM + size)
        at = pl.ds(pl.multiple_of(k * group, group), group)
        step, cum = small(steps, k), small(cums, k)
        last = cum[:, group - 1 :]
        x = xs[k, here]
        step_full = spread(step, span)
        u16 = (x * step_full).astype(BF16)
        tail16 = tails[k, here]
        in16, out16 = ins[k], outs[k]
        dy16 = dys[k, here]
        dy = dy16.astype(F32)
        tail = spread(jnp.exp(last - cum), span)
        lead = spread(jnp.exp(cum), span)
        leave = spread(jnp.exp(jnp.broadcast_to(last, (slots, STATE))), span)
        held16 = states[k, here]
        g_out = grad[here]
        g16 = g_out.astype(BF16)
        dy_lead = dy * lead
        lead16 = dy_lead.astype(BF16)

        score = scores[k]
        cum_col = cumt[k]
        d_score = jnp.zeros((group, group), F32)
        du_parts, r_parts = [], []
        for i, h in enumerate(span):
            at_h = slice(i * HEAD_DIM, (i + 1) * HEAD_DIM)
            diff = cum[h : h + 1] - cum_col[:, h : h + 1]
            within = jnp.exp(jnp.where(causal, diff, -1e30))
            mixing = (score * within).astype(BF16)
            d_mix = tn(u16[at_h], dy16[at_h])
            du_parts.append(nt(dy16[at_h], mixing))
            d_score = d_score + d_mix * within
            r_parts.append(jnp.sum(d_mix * mixing.astype(F32), axis=0, keepdims=True))
        du = jnp.concatenate(du_parts, axis=0) + nn(g16, in16) * tail
        from_x = gather_rows(du * x, span)
        from_u = gather_rows(du * u16.astype(F32), span)
        lead_rows = gather_rows(dy_lead * nn(held16, out16), span)
        cross = jnp.sum(gather_rows(g_out * states[k + 1, here].astype(F32), span), axis=1, keepdims=True)
        d_cum = padded(r_parts, span) + lead_rows - from_u
        d_log = summed(d_cum, after) + cross
        d_raw = (from_x + rate * d_log) * small(sigr, k)

        d_score16 = d_score.astype(BF16)
        d_out = nn(in16, d_score16) + tn(held16, lead16)
        d_in = nt(out16, d_score16) + tn(g16, tail16)
        grad[here] = leave * g_out + nt(lead16, out16)
        slope = pre[mine_v : mine_v + size, at]
        gain_full = spread(jnp.broadcast_to(gain, (slots, group)), span)
        grads[mine_v : mine_v + size, at] = ((du * step_full + dy * gain_full) * slope).astype(BF16)
        fill = jnp.zeros((16 - slots, group), F32)
        raw16 = jnp.concatenate([d_raw, fill], axis=0).astype(BF16)
        acc[0] += d_raw
        acc[1] += d_log * (rate * step)
        acc[2] += gather_rows(dy * x, span)
        if g == 0:
            grads[top : top + 16, at] = raw16
            maps[0, k] = d_in
            maps[1, k] = d_out
        else:
            grads[top : top + 16, at] += raw16
            m_in, m_out = pre[pl.ds(in_at, STATE), at], pre[pl.ds(out_at, STATE), at]
            s_in, s_out = jax.nn.sigmoid(m_in), jax.nn.sigmoid(m_out)
            d_in = (maps[0, k] + d_in) * (s_in * (1.0 + m_in * (1.0 - s_in)))
            d_out = (maps[1, k] + d_out) * (s_out * (1.0 + m_out * (1.0 - s_out)))
            maps[0, k] = d_in
            maps[1, k] = d_out
            grads[pl.ds(in_at, STATE), at] = d_in.astype(BF16)
            grads[pl.ds(out_at, STATE), at] = d_out.astype(BF16)
            map_copy(k).start()

    def both_ways(g):
        def ahead(k, carry):
            forward(g, k)
            return carry

        def back(n, carry):
            backward(g, chunks - 1 - n)
            return carry

        here = slice(0, in1) if g == 0 else slice(in1, inner)
        lax.fori_loop(0, chunks, ahead, 0)
        states[chunks, here] = grad[here].astype(BF16)
        grad[here] = jnp.zeros_like(grad[here])
        if g == 0:
            for h in range(2, last_z):
                late_hop(h, True)
            for copy in cots:
                copy.wait_recv()
        if g == 0:
            lax.fori_loop(0, chunks, back, 0)
        else:
            lax.fori_loop(0, chunks // 2, back, 0)
            serve(0, 1)
            lax.fori_loop(chunks // 2, chunks, back, 0)

    block = wbuf.shape[4]
    many = 4 if seqs % 4 == 0 else 2
    span_rows = many * zeros * block

    def weigh(g, first, size):
        def part_of(q, carry):
            at = pl.ds(pl.multiple_of(q * span_rows, span_rows), span_rows)
            product = nt(tokt[at, :], grads[first : first + size, :])
            for a in range(many):
                for t in range(zeros):
                    lo = (a * zeros + t) * block
                    wbuf[g, t, a % 2, q * (many // 2) + a // 2, :, 0:size] = product[
                        lo : lo + block
                    ].astype(BF16)
            return carry

        lax.fori_loop(0, seqs // many, part_of, 0)

    sizes = (w1, w2 + STATE)

    def back_flow(g, way, t, p):
        landed = rflow if way == 0 else lflow
        peer = up_peer if way == 0 else down_peer
        return remote(
            wbuf.at[g, t, p, :, :, pl.ds(0, sizes[g])], landed.at[g, t, p, :, :, pl.ds(0, sizes[g])],
            rsem.at[g, way, 0, t, p], rsem.at[g, way, 1, t, p], peer,
        )

    def from_ends(g):
        for z, way in ((0, 0), (last_z, 1)):
            if zeros > 1:
                @pl.when(me_z == z)
                def _():
                    for i in range(last_z):
                        for p in (0, 1):
                            back_flow(g, way, last_z - i if way == 0 else i, p).start()

    low = model // 2

    def turn_of(n):
        return lax.rem(chip + 1 + n, chips)

    def give(i, j):
        at = pl.ds(j * low, low)
        return remote(
            part.at[i, 1 - core, at], got_part.at[i, at], dsem.at[0, i, j], dsem.at[1, i, j], sibling
        )

    def token_send(i):
        return remote(
            sent.at[i], tok_in.at[chip], ksem.at[0, i], ksem.at[1, chip], (i * 2 + core, me_z)
        )

    def settle(n):
        i = turn_of(n)
        for j in (0, 1):
            at = slice(j * low, (j + 1) * low)
            give(i, j).wait_recv()
            sent[i, at, :] = (part[i, core, at, :] + got_part[i, at, :]).astype(BF16)

        @pl.when(i != chip)
        def _():
            token_send(i).start()

    def events(z):
        found = []
        for g in (0, 1):
            for p in (0, 1):
                ends = 0.0
                for i in range(last_z):
                    for way in (0, 1):
                        t = last_z - i if way == 0 else i
                        hops = z if way == 0 else last_z - z
                        if hops == 0:
                            continue
                        when = (g * last_z + i) * 2 + p + 1 + 2.2 * hops
                        if t == z:
                            ends = max(ends, when)
                        elif (way == 0) == (z < t):
                            found.append((when, 1 + g, "pass", (way, t, p)))
                found.append((ends + 0.01, 1 + g, "end", p))
            if g == 0:
                found.append((ends + 0.02, 1, "heads", 0))
        return sorted(found, key=lambda e: e[:2])

    served = 4

    def serve(first, final):
        for z in range(zeros):
            listed = events(z)
            soon = [e for e in listed if e[1:3] == (1, "pass")][:served]
            todo = [e for e in listed if e not in soon] if final is None else soon[first:final]
            if todo:
                @pl.when(me_z == z)
                def _():
                    serve_at(z, todo)

    def serve_at(z, todo):
        for _, g, what, p in todo:
            g = g - 1
            if what == "pass":
                way, t, p = p
                landed = rflow if way == 0 else lflow
                back_flow(g, way, t, p).wait_recv()
                wbuf[g, t, p] = (
                    wbuf[g, t, p].astype(F32) + landed[g, t, p].astype(F32)
                ).astype(BF16)
                back_flow(g, way, t, p).start()
            elif what == "heads":
                close_heads()
                drain()
            else:
                finish_piece(z, g, p)

    def head_copy(d):
        return remote(
            hmine, hin.at[me_z], hsem.at[0, d], hsem.at[1, d], (me_s, lax.rem(me_z + d, zeros))
        )

    def head_along(d):
        return remote(
            hsum, hall.at[me_s], gsem.at[0, d], gsem.at[1, d], (lax.rem(me_s + d, seqs), me_z)
        )

    def close_heads():
        for d in range(1, zeros):
            head_copy(d).wait_recv()
        sums = hin[0]
        for d in range(1, zeros):
            sums = sums + hin[d]
        hsum[...] = sums
        hall[me_s] = sums
        for d in range(1, seqs):
            head_along(d).start()

    def drain():
        for g in (0, 1):
            for p in (0, 1):
                for way in (0, 1):
                    for h in range(last_z):
                        @pl.when(sends(way, h))
                        def _():
                            flow(g, way, h, p, 0).wait_send()
        for j in range(zeros):
            shared(j).wait_send()
        for copy in direct + to_sibling + cots:
            copy.wait_send()

        def gone(k, carry):
            map_copy(k).wait_send()
            return carry

        lax.fori_loop(0, chunks, gone, 0)
        for i in range(chips):
            for j in (0, 1):
                give(i, j).wait_send()

    def finish_piece(z, g, p):
        if z > 0:
            back_flow(g, 0, z, p).wait_recv()
        if z < last_z:
            back_flow(g, 1, z, p).wait_recv()
        if g == 1 and p == 0:
            for d in range(1, zeros):
                steps_copy(d).wait_recv()
            total = swin[0].astype(F32)
            for d in range(1, zeros):
                total = total + swin[d].astype(F32)
            total = total.astype(BF16)
            for s in range(seqs):
                stsend[s] = total[:, s * 16 : (s + 1) * 16]
            for s in range(seqs):
                @pl.when(me_s != s)
                def _():
                    steps_along(s).start()
        for j in range(seqs // 2):
            s = 2 * j + p
            value = wbuf[g, z, p, j, :, 0 : sizes[g]].astype(F32)
            if z > 0:
                value = value + rflow[g, z, p, j, :, 0 : sizes[g]].astype(F32)
            if z < last_z:
                value = value + lflow[g, z, p, j, :, 0 : sizes[g]].astype(F32)
            zsend[g, s, :, 0 : sizes[g]] = value.astype(BF16)
        for j in range(seqs // 2):
            @pl.when(me_s != 2 * j + p)
            def _():
                along(g, 2 * j + p).start()

    def along(g, s):
        lanes = pl.ds(0, sizes[g])
        return remote(
            zsend.at[g, s, :, lanes], rows_in.at[g, me_s, :, lanes],
            wsem.at[g, 0, s], wsem.at[g, 1, me_s], (s, me_z),
        )

    def steps_along(s):
        return remote(stsend.at[s], stin.at[me_s], xsem.at[0, s], xsem.at[1, me_s], (s, me_z))

    def steps_copy(d):
        target = lax.rem(me_z + d, zeros)
        return remote(
            swbuf.at[target], swin.at[me_z], ysem.at[0, d], ysem.at[1, d], (me_s, target)
        )

    grad[...] = jnp.zeros_like(grad)
    acc[...] = jnp.zeros_like(acc)
    grads[pl.ds(top, v2 - top), :] = jnp.zeros((v2 - top, chunks * group), BF16)
    if w2 > in2:
        grads[pl.ds(v2 + in2, w2 - in2), :] = jnp.zeros((w2 - in2, chunks * group), BF16)
    both_ways(0)
    weigh(0, v1, w1)
    from_ends(0)

    for h in range(1, zeros):
        late_hop(h, False)

    def project_late(i, carry):
        cols = pl.ds(pl.multiple_of(i * batch, batch), batch)
        pre[v2:wide, cols] = tn(wall[:, v2:wide], tokt[:, cols])
        return carry

    lax.fori_loop(0, chunks * group // batch, project_late, 0)
    both_ways(1)
    serve(1, 2)

    for j in (0, 1):
        at = slice(j * low, (j + 1) * low)
        product = nn(wall[at, :], grads[0:wide, :])
        for k in range(chunks):
            part[k // 2, k % 2, at, :] = product[:, k * group : (k + 1) * group]
        for n in range(chips):
            give(turn_of(n), j).start()
        serve(2 + j, 3 + j)

    def merge(k, carry):
        map_copy(k).wait_recv()
        at = pl.ds(pl.multiple_of(k * group, group), group)
        grads[extra : extra + STATE, at] = (maps[core, k] + got_map[k]).astype(BF16)
        return carry

    lax.fori_loop(0, chunks, merge, 0)
    wide_head = hmine.shape[1]
    place_row = lax.broadcasted_iota(jnp.int32, (slots, wide_head), 0)
    place = jnp.logical_and(
        lax.broadcasted_iota(jnp.int32, (slots, wide_head), 1) == me_s * hp + place_row, place_row < hp
    )
    lines = [
        jnp.sum(
            jnp.where(place, jnp.sum(acc[i], axis=1, keepdims=True), 0.0), axis=0, keepdims=True
        )
        for i in range(3)
    ]
    hmine[...] = jnp.concatenate(lines + [jnp.zeros((5, wide_head), F32)], axis=0)
    hin[me_z] = hmine[...]

    for d in range(1, zeros):
        head_copy(d).start()

    weigh(1, v2, w2 + STATE)
    from_ends(1)

    steps_grad = nt(tokt[...], grads[top : top + 16, :])
    for t in range(zeros):
        lines = [
            steps_grad[(s * zeros + t) * block : (s * zeros + t + 1) * block] for s in range(seqs)
        ]
        swbuf[t] = jnp.concatenate(lines, axis=1).astype(BF16)
    swin[me_z] = swbuf[me_z]

    for d in range(1, zeros):
        steps_copy(d).start()

    for n in range(chips):
        settle(n)
    serve(None, None)

    for g in (0, 1):
        rows_in[g, me_s] = zsend[g, me_s]
    for d in range(1, chips):
        at = lax.rem(chip + d, chips)
        remote(
            sent.at[at], tok_in.at[at], ksem.at[0, at], ksem.at[1, at], (at * 2 + core, me_z)
        ).wait_recv()
    tok_in[chip] = sent[chip]

    for j in (0, 1):
        at = slice(j * low, (j + 1) * low)
        value = tok_in[0, at, :].astype(F32)
        for source in range(1, chips):
            value = value + tok_in[source, at, :].astype(F32)
        hid[:, at] = value.T.astype(BF16)

    def landed_from(g, s):
        @pl.when(me_s != s)
        def _():
            lanes = pl.ds(0, sizes[g])
            remote(
                zsend.at[g, s, :, lanes], rows_in.at[g, s, :, lanes],
                wsem.at[g, 0, s], wsem.at[g, 1, s], (s, me_z),
            ).wait_recv()

    stin[me_s] = stsend[me_s]
    for s in range(seqs):
        @pl.when(me_s != s)
        def _():
            remote(stsend.at[s], stin.at[s], xsem.at[0, s], xsem.at[1, s], (s, me_z)).wait_recv()
    for s in range(seqs):
        landed_from(0, s)
        piece_in = rows_in[0, s].astype(F32)
        rows_out[:, s * inner : s * inner + in1] = piece_in[:, :in1]
    for d in range(1, seqs):
        head_along(d).wait_recv()
    map_sums = [jnp.zeros((block, STATE), F32), jnp.zeros((block, STATE), F32)]
    for s in range(seqs):
        landed_from(1, s)
        piece_in = rows_in[1, s].astype(F32)
        rows_out[:, s * inner + in1 : (s + 1) * inner] = piece_in[:, :in2]
        base = full + 2 * STATE + s * hp
        rows_out[:, base : base + hp] = stin[s, :, :hp].astype(F32)
        map_sums[s % 2] = map_sums[s % 2] + piece_in[:, w2 : w2 + STATE]
    rows_out[:, full : full + 2 * STATE] = jnp.concatenate(map_sums, axis=1)
    sums = hall[0]
    for s in range(1, seqs):
        sums = sums + hall[s]
    head_out[...] = sums[:3, :heads]

    for g in (0, 1):
        for p in (0, 1):
            for way in (0, 1):
                for t in range(zeros):
                    ahead = me_z < t if way == 0 else me_z > t

                    @pl.when(ahead)
                    def _():
                        back_flow(g, way, t, p).wait_send()
    for d in range(1, zeros):
        steps_copy(d).wait_send()
        head_copy(d).wait_send()
    for d in range(1, seqs):
        head_along(d).wait_send()
    for s in range(seqs):
        @pl.when(me_s != s)
        def _():
            along(0, s).wait_send()
            along(1, s).wait_send()
            steps_along(s).wait_send()
    for i in range(chips):
        @pl.when(i != chip)
        def _():
            token_send(i).wait_send()


def mixer_backward(hidden, cotangent, weight, bias, log, gain, seqs, zeros, hp):
    length, model = hidden.shape
    rows = weight.shape[0]
    heads = bias.shape[1]
    inner = hp * HEAD_DIM
    slots = up(hp, 8)
    (n1, w1), (n2, w2) = groups_of(hp)
    wide = 2 * STATE + w1 + w2
    ends = max(w1, w2 + STATE)
    block = rows // seqs
    chips = seqs // 2
    total = seqs * length
    full = seqs * inner
    span = up(inner + (HEAD_DIM if hp % 2 else 0), 128)
    lanes = up(heads, 128)
    dma = pltpu.SemaphoreType.DMA
    vmem = pl.BlockSpec(memory_space=pltpu.VMEM)
    anywhere = pl.BlockSpec(memory_space=pl.ANY)
    return pl.pallas_call(
        functools.partial(mixer_backward_kernel, seqs, zeros, hp),
        out_shape=(
            jax.ShapeDtypeStruct((length, model), BF16),
            jax.ShapeDtypeStruct((block, full + 2 * STATE + heads), F32),
            jax.ShapeDtypeStruct((3, heads), F32),
        ),
        in_specs=[anywhere] * 3 + [vmem] * 3,
        out_specs=(vmem,) * 3,
        scratch_shapes=[
            pltpu.VMEM((rows, span), BF16),
            pltpu.VMEM((rows, heads), BF16),
            pltpu.VMEM((length, full), BF16),
            pltpu.VMEM((full, length), BF16),
            pltpu.VMEM((seqs, length, model), BF16),
            pltpu.VMEM((model, total), BF16),
            pltpu.VMEM((model, wide), BF16),
            pltpu.VMEM((zeros, 2 * STATE + w1, rows), BF16),
            pltpu.VMEM((wide, total), F32),
            pltpu.VMEM((seqs, inner, length), BF16),
            pltpu.VMEM((seqs, inner, length), F32),
            pltpu.VMEM((seqs, inner, length), BF16),
            pltpu.VMEM((seqs + 1, inner, STATE), BF16),
            pltpu.VMEM((wide + STATE, total), BF16),
            pltpu.VMEM((inner, STATE), F32),
            pltpu.VMEM((3, slots, length), F32),
            pltpu.VMEM((seqs * slots, length), F32),
            pltpu.VMEM((seqs * slots, length), F32),
            pltpu.VMEM((seqs, length, length), F32),
            pltpu.VMEM((seqs * slots, length), F32),
            pltpu.VMEM((2, seqs, STATE, length), F32),
            pltpu.VMEM((seqs, STATE, length), F32),
            pltpu.VMEM((chips, 2, model, length), F32),
            pltpu.VMEM((chips, model, length), F32),
            pltpu.VMEM((chips, model, length), BF16),
            pltpu.VMEM((chips, model, length), BF16),
            pltpu.VMEM((2, zeros, 2, seqs // 2, block, ends), BF16),
            pltpu.VMEM((2, zeros, 2, seqs // 2, block, ends), BF16),
            pltpu.VMEM((2, zeros, 2, seqs // 2, block, ends), BF16),
            pltpu.VMEM((2, seqs, block, ends), BF16),
            pltpu.VMEM((2, seqs, block, ends), BF16),
            pltpu.VMEM((zeros, 8, lanes), F32),
            pltpu.VMEM((8, lanes), F32),
            pltpu.VMEM((8, lanes), F32),
            pltpu.VMEM((seqs, 8, lanes), F32),
            pltpu.VMEM((seqs, STATE, length), BF16),
            pltpu.VMEM((seqs, STATE, length), BF16),
            pltpu.VMEM((seqs, length, length), F32),
            pltpu.VMEM((zeros, block, seqs * 16), BF16),
            pltpu.VMEM((zeros, block, seqs * 16), BF16),
            pltpu.VMEM((seqs, block, 16), BF16),
            pltpu.VMEM((seqs, block, 16), BF16),
            dma((2, 2, 2, zeros + 1, 2)),
            dma((2, seqs)),
            dma((2, seqs)),
            dma((2, seqs)),
            dma((2, zeros)),
            dma((2, seqs)),
            dma((2, chips, 2)),
            dma((2, chips)),
            dma((2, 2, 2, zeros, 2)),
            dma((2, seqs)),
            dma((2, zeros)),
            dma((2, 2, seqs)),
            dma((5,)),
            dma((2, zeros)),
            dma((2, seqs)),
        ],
        compiler_params=pltpu.CompilerParams(
            collective_id=0, has_side_effects=True, vmem_limit_bytes=63 * 1024 * 1024
        ),
        name="mixer_backward",
    )(hidden, cotangent, weight, bias, log, gain)


def store_kernel(*refs):
    count = len(refs) // 2
    sem = refs[-1]
    copies = [pltpu.make_async_copy(refs[i], refs[count + i], sem.at[i]) for i in range(count)]
    for copy in copies:
        copy.start()
    for copy in copies:
        copy.wait()


def store(*arrays):
    return pl.pallas_call(
        store_kernel,
        out_shape=tuple(jax.ShapeDtypeStruct(a.shape, a.dtype) for a in arrays),
        in_specs=[pl.BlockSpec(memory_space=pltpu.VMEM)] * len(arrays),
        out_specs=(pl.BlockSpec(memory_space=pl.ANY),) * len(arrays),
        scratch_shapes=[pltpu.SemaphoreType.DMA((len(arrays),))],
        name="store",
    )(*arrays)


def body(seqs, zeros, hidden, output_grad, input_weight, step_bias, decay_log, skip_gain):
    heads = step_bias.shape[0]
    hp = up(heads, seqs) // seqs
    spare = seqs * hp - heads
    full, total = heads * HEAD_DIM, seqs * hp * HEAD_DIM
    tokens, cot, weight = hidden[0], output_grad[0], input_weight
    params = [step_bias, decay_log, skip_gain]
    if spare:
        cot = jnp.pad(cot, ((0, 0), (0, total - full)))
        gap = jnp.zeros((weight.shape[0], total - full), BF16)
        few = jnp.zeros((weight.shape[0], spare), BF16)
        weight = jnp.concatenate([weight[:, :full], gap, weight[:, full:], few], axis=1)
        params = [jnp.pad(v, (0, spare)) for v in params]
    token_grad, weight_grad, head_grads = mixer_backward(
        tokens, cot, weight, *[v[None] for v in params], seqs, zeros, hp
    )
    token_grad, weight_grad, head_grads = store(token_grad, weight_grad, head_grads)
    if spare:
        weight_grad = jnp.concatenate(
            [weight_grad[:, :full], weight_grad[:, total : total + 2 * STATE + heads]], axis=1
        )
        head_grads = head_grads[:, :heads]
    return (token_grad[None], weight_grad, head_grads)


def solution(mesh):
    placed = (P("zero", "seq", None), P("zero", "seq", None), P("zero", None), P(), P(), P())
    return jax.shard_map(
        functools.partial(body, mesh.shape["seq"], mesh.shape["zero"]),
        mesh=mesh,
        in_specs=placed,
        out_specs=(P("zero", "seq", None), P(("seq", "zero"), None), P()),
        check_vma=False,
    )
```

```python
import functools

import jax
import jax.numpy as jnp
from jax import lax
from jax.experimental import pallas as pl
from jax.experimental.pallas import tpu as pltpu
from jax.sharding import PartitionSpec as P

HEAD_DIM = 64
STATE = 128
MESH = pl.DeviceIdType.MESH
F32 = jnp.float32
BF16 = jnp.bfloat16


def up(size, unit):
    return -(-size // unit) * unit


def nn(a, b):
    return lax.dot_general(a, b, (((1,), (0,)), ((), ())), preferred_element_type=F32)


def nt(a, b):
    return lax.dot_general(a, b, (((1,), (1,)), ((), ())), preferred_element_type=F32)


def tn(a, b):
    return lax.dot_general(a, b, (((0,), (0,)), ((), ())), preferred_element_type=F32)


def halves(a):
    high = a.astype(BF16)
    return high, (a - high.astype(F32)).astype(BF16)


def remote(src, dst, send, recv, peer):
    return pltpu.make_async_remote_copy(src, dst, send, recv, peer, MESH)


def groups_of(hp):
    first = hp - hp // 2
    second = hp - first
    return (first, up(first * HEAD_DIM + 16, 128)), (second, up(second * HEAD_DIM, 128))


def mixer_backward_kernel(
    seqs, zeros, hp,
    hidden, cotangent, weight, bias_in, log_in, gain_in,
    hid_hbm, rows_hbm, head_hbm,
    hid, rows_out, head_out, window, tiny, cotv, cott,
    toks, tokt, wall, wallt, pre, dys, xs, tails, states, grads, grad, acc, steps, cums, cumt, sigr,
    maps, got_map, wall2, mgrads, sgrads, sent, tok_in, wbuf, rflow, lflow, zsend, rows_in, hin, hsum, hmine, hall,
    ins, outs, scores, swbuf, swin, stsend, stin,
    asem, tsem, psem, csem, ssem, msem, dsem, ksem, rsem, gsem, hsem, wsem, loc, ysem, xsem, qsem,
):
    me_s, me_z = lax.axis_index("seq"), lax.axis_index("zero")
    chips = seqs // 2
    chip, core = me_s // 2, lax.rem(me_s, 2)
    sib = me_s // 2 * 2 + 1 - core
    sibling = (sib, me_z)
    length, model = hidden.shape
    rows = weight.shape[0]
    wide = wall.shape[1]
    inner = dys.shape[1]
    (n1, w1), (n2, w2) = groups_of(hp)
    in1, in2 = n1 * HEAD_DIM, n2 * HEAD_DIM
    slots = acc.shape[1]
    full = cotangent.shape[1]
    chunks, group = seqs, length
    v1 = 2 * STATE
    top, v2 = v1 + in1, v1 + w1
    extra = wide
    up_peer, down_peer = (me_s, me_z + 1), (me_s, me_z - 1)
    half = rows // 2
    last_z = zeros - 1
    pairs = 2 * group

    peers = [(lax.rem(me_s + d, seqs), me_z) for d in range(1, seqs)]
    peers += [(me_s, lax.rem(me_z + d, zeros)) for d in range(1, zeros)]
    barrier = pltpu.get_barrier_semaphore()
    for peer in peers:
        pl.semaphore_signal(barrier, inc=1, device_id=peer, device_id_type=MESH)

    start = pl.multiple_of(me_s * inner // 128 * 128, 128)
    mine = pl.ds(pl.multiple_of(me_z * rows, rows), rows)
    fetch = [
        pltpu.make_async_copy(weight.at[:, pl.ds(start, window.shape[1])], window, loc.at[0]),
        pltpu.make_async_copy(
            weight.at[:, pl.ds(pl.multiple_of(full + core * STATE, 128), STATE)],
            wall.at[mine, pl.ds(STATE, STATE)], loc.at[1],
        ),
        pltpu.make_async_copy(weight.at[:, pl.ds(full + 2 * STATE, tiny.shape[1])], tiny, loc.at[2]),
        pltpu.make_async_copy(hidden, toks.at[me_s], loc.at[3]),
        pltpu.make_async_copy(cotangent, cotv, loc.at[4]),
    ]
    for copy in fetch:
        copy.start()
    heads = tiny.shape[1]
    head_row = lax.broadcasted_iota(jnp.int32, (heads, v2 - top), 0)
    head_col = lax.broadcasted_iota(jnp.int32, (heads, v2 - top), 1)
    chosen = jnp.logical_and(head_row == me_s * hp + head_col, head_col < hp)
    chosen = jnp.where(chosen, 1.0, 0.0).astype(BF16)
    fetch[2].wait()
    wall[mine, top:v2] = nn(tiny[...], chosen).astype(BF16)
    fetch[0].wait()
    def place_values(shift):
        wall[mine, v1:top] = window[:, shift : shift + in1]
        wall[mine, v2 : v2 + in2] = window[:, shift + in1 : shift + inner]
        if w2 > in2:
            wall[mine, v2 + in2 : v2 + w2] = jnp.zeros((rows, w2 - in2), BF16)

    if hp % 2:
        shifted = lax.rem(me_s, 2)
        for shift in (0, 1):
            @pl.when(shifted == shift)
            def _():
                place_values(shift * HEAD_DIM)
    else:
        place_values(0)
    fetch[1].wait()
    fetch[3].wait()

    pl.semaphore_wait(barrier, len(peers))

    spans = ((STATE, STATE + w1), (v2, w2))

    def piece(g, at, p):
        first = pl.multiple_of(at * rows + p * half, half)
        return wall.at[pl.ds(first, half), pl.ds(*spans[g])]

    def flow(g, way, h, p, recv):
        at = me_z - h if way == 0 else me_z + h
        return remote(
            piece(g, at, p), piece(g, at, p),
            asem.at[g, way, 0, min(h, last_z - 1), p], asem.at[g, way, 1, h - recv, p],
            up_peer if way == 0 else down_peer,
        )

    def sends(way, h):
        if way == 0:
            return jnp.logical_and(me_z < last_z, me_z >= h)
        return jnp.logical_and(me_z > 0, me_z + h <= last_z)

    def comes(way, h):
        return me_z >= h if way == 0 else me_z + h <= last_z

    def shared(at):
        first = pl.multiple_of(at * rows, rows)
        return remote(
            wall.at[pl.ds(first, rows), pl.ds(STATE, STATE)],
            wall.at[pl.ds(first, rows), pl.ds(0, STATE)],
            ssem.at[0, at], ssem.at[1, at], sibling,
        )

    for p in (0, 1):
        for way in (0, 1):
            @pl.when(sends(way, 0))
            def _():
                flow(0, way, 0, p, 0).start()

    def own_late(h):
        for way in (0, 1):
            distance = me_z if way == 0 else last_z - me_z

            @pl.when(jnp.logical_and(distance == h, sends(way, 0)))
            def _():
                for p in (0, 1):
                    flow(1, way, 0, p, 0).start()

    own_late(0)

    def token(src_s, dst, lo, size, slot):
        block = toks.at[src_s, pl.ds(lo, size)]
        return remote(block, block, tsem.at[0, slot], tsem.at[1, slot], (dst, me_z))

    def passed(src_s, slot):
        return remote(toks.at[src_s], toks.at[src_s], psem.at[0, slot], psem.at[1, slot], sibling)

    square = chips == 4
    cut = length // 2
    to_sibling = [passed(me_s, 0)]
    if square:
        flat = chip + 1 - 2 * lax.rem(chip, 2)
        tall = lax.rem(chip + 2, 4)
        far = lax.rem(flat + 2, 4)
        around = [flat, tall]
    else:
        around = [lax.rem(chip + d, chips) for d in range(1, chips)]
    direct = [token(me_s, c * 2 + core, 0, length, i) for i, c in enumerate(around)]
    for copy in direct + to_sibling:
        copy.start()
    shared(me_z).start()

    pre[...] = jnp.zeros_like(pre)
    fetch[4].wait()
    strip = 512

    def turn_cot(j, carry):
        at = pl.ds(pl.multiple_of(j * strip, strip), strip)
        cott[at, :] = cotv[:, at].T
        return carry

    lax.fori_loop(0, full // strip, turn_cot, 0)

    def cot_of(s):
        return cott.at[pl.ds(pl.multiple_of(s * inner, inner), inner)]

    dys[me_s] = cot_of(me_s)[...]

    def step_hop(h):
        for p in (0, 1):
            for way in (0, 1):
                @pl.when(comes(way, h))
                def _():
                    flow(0, way, h, p, 1).wait_recv()
                if h < last_z:
                    @pl.when(sends(way, h))
                    def _():
                        flow(0, way, h, p, 0).start()
        if h < last_z:
            own_late(h)
        for way in (0, 1):
            @pl.when(comes(way, h))
            def _():
                shared(me_z - h if way == 0 else me_z + h).start()

    def late_hop(h, onward):
        for p in (0, 1):
            for way in (0, 1):
                goes = sends(way, h) if h < last_z else jnp.bool_(False)
                if onward:
                    if h < last_z:
                        @pl.when(goes)
                        def _():
                            flow(1, way, h, p, 1).wait_recv()
                            flow(1, way, h, p, 0).start()
                else:
                    @pl.when(jnp.logical_and(comes(way, h), jnp.logical_not(goes)))
                    def _():
                        flow(1, way, h, p, 1).wait_recv()

    if zeros > 2:
        step_hop(1)

    def chip_of(n):
        if square:
            return lax.rem(chip // 2 + n // 2, 2) * 2 + lax.rem(lax.rem(chip, 2) + n % 2, 2)
        return lax.rem(chip + n, chips)

    def turn(n, carry):
        for half_chip in (0, 1):
            k = chip_of(n) * 2 + half_chip
            tokt[:, pl.ds(pl.multiple_of(k * group, group), group)] = toks[k].T
        return carry

    early = 3 if square else 0
    if square:
        onward = [
            token(flat * 2 + core, tall * 2 + core, 0, cut, 2),
            token(tall * 2 + core, flat * 2 + core, cut, length - cut, 3),
        ]
        for i in (0, 1):
            direct[i].wait_recv()
            onward[i].start()
        direct += onward
        more = [passed(flat * 2 + core, 1), passed(tall * 2 + core, 2)]
        for copy in more:
            copy.start()
        to_sibling += more
        for copy in to_sibling:
            copy.wait_recv()
        lax.fori_loop(0, early, turn, 0)

    for h in range(2, last_z):
        step_hop(h)

    def flip(j):
        shared(j).wait_recv()
        wallt[j] = wall[pl.ds(pl.multiple_of(j * rows, rows), rows), :v2].T

    def project(j, first, final):
        def part_of(n, carry):
            at = pl.ds(pl.multiple_of(j * rows, rows), rows)
            cols = pl.ds(pl.multiple_of(chip_of(n) * pairs, pairs), pairs)
            pre[:v2, cols] += nn(wallt[j], tokt[at, cols])
            return carry

        lax.fori_loop(first, final, part_of, 0)

    def near(first, final, fresh):
        def one(j, carry):
            distance = jnp.abs(j - me_z)
            ready = distance < last_z if zeros > 1 else distance < 1

            @pl.when(ready)
            def _():
                if fresh:
                    flip(j)
                project(j, first, final)
            return carry

        lax.fori_loop(0, zeros, one, 0)

    if early:
        near(0, early, True)

    if square:
        token(far * 2 + core, tall * 2 + core, 0, cut, 2).wait_recv()
        token(far * 2 + core, flat * 2 + core, cut, length - cut, 3).wait_recv()
        rest = [passed(far * 2 + core, 3)]
    else:
        rest = []
        for d in range(1, chips):
            direct[d - 1].wait_recv()
            rest.append(passed(lax.rem(chip - d + chips, chips) * 2 + core, d))
    for copy in rest:
        copy.start()
    cots = []
    for d in range(1, seqs):
        peer = lax.rem(me_s + d, seqs)
        cots.append(remote(cot_of(peer), dys.at[me_s], csem.at[0], csem.at[1], (peer, me_z)))
    for copy in cots:
        copy.start()
    all_cots = remote(
        dys.at[pl.ds(0, seqs - 1)], dys.at[pl.ds(0, seqs - 1)], csem.at[0], csem.at[1], sibling
    )
    if not square:
        rest = to_sibling + rest
    for copy in rest:
        copy.wait_recv()
    to_sibling = to_sibling + rest if square else rest
    lax.fori_loop(early, chips, turn, 0)
    near(early, chips, not early)

    batch = 4 * group if chunks % 4 == 0 else pairs

    if zeros > 2:
        late_hop(1, True)
    if zeros > 1:
        step_hop(last_z)
        far_end = jnp.logical_or(me_z == 0, me_z == last_z)

        @pl.when(far_end)
        def _():
            flip(last_z - me_z)
            project(last_z - me_z, 0, chips)

    in_at = pl.multiple_of((1 - core) * STATE, 128)
    out_at = pl.multiple_of(core * STATE, 128)
    slot = lax.broadcasted_iota(jnp.int32, (slots, heads), 0)
    own_head = jnp.logical_and(
        lax.broadcasted_iota(jnp.int32, (slots, heads), 1) == me_s * hp + slot, slot < hp
    )

    def own(ref):
        return jnp.sum(jnp.where(own_head, ref[...], 0.0), axis=1, keepdims=True)

    bias, rate, gain = own(bias_in), -jnp.exp(own(log_in)), own(gain_in)
    row = lax.broadcasted_iota(jnp.int32, (group, group), 0)
    col = lax.broadcasted_iota(jnp.int32, (group, group), 1)
    causal = col >= row

    def spread(values, span):
        return jnp.concatenate(
            [jnp.broadcast_to(values[h : h + 1], (HEAD_DIM, values.shape[1])) for h in span], axis=0
        )

    def gather_rows(whole, span):
        parts = [
            jnp.sum(whole[i * HEAD_DIM : (i + 1) * HEAD_DIM], axis=0, keepdims=True)
            for i in range(len(span))
        ]
        return padded(parts, span)

    def padded(parts, span):
        lanes = parts[0].shape[1]
        if span[0] > 0:
            parts = [jnp.zeros((span[0], lanes), F32)] + parts
        if slots > span[-1] + 1:
            parts = parts + [jnp.zeros((slots - span[-1] - 1, lanes), F32)]
        return jnp.concatenate(parts, axis=0)

    raw = pre[top : top + slots, :] + bias
    soft = jax.nn.softplus(raw)
    curve = jax.nn.sigmoid(raw)
    stacked = jnp.concatenate([soft[:, k * group : (k + 1) * group] for k in range(chunks)], axis=0)
    steps[...] = stacked
    sigr[...] = jnp.concatenate([curve[:, k * group : (k + 1) * group] for k in range(chunks)], axis=0)
    logs = jnp.concatenate([rate] * chunks, axis=0) * stacked
    before = jnp.where(causal, 1.0, 0.0).astype(BF16)
    after = jnp.where(col <= row, 1.0, 0.0).astype(BF16)

    def summed(values, mask):
        a = values.astype(BF16)
        rest = values - a.astype(F32)
        b = rest.astype(BF16)
        c = (rest - b.astype(F32)).astype(BF16)
        return nn(a, mask) + (nn(b, mask) + nn(c, mask))

    cums[...] = summed(logs, before)

    def small(ref, k):
        return ref[pl.ds(pl.multiple_of(k * slots, slots), slots), :]

    def forward(g, k):
        span, mine_v, size = (range(n1), v1, in1) if g == 0 else (range(n1, hp), v2, in2)
        here = slice(span[0] * HEAD_DIM, span[0] * HEAD_DIM + size)
        at = pl.ds(pl.multiple_of(k * group, group), group)
        p = pre[mine_v : mine_v + size, at]
        sig = jax.nn.sigmoid(p)
        x = p * sig
        xs[k, here] = x
        pre[mine_v : mine_v + size, at] = sig * (1.0 + p * (1.0 - sig))
        step, cum = small(steps, k), small(cums, k)
        last = cum[:, group - 1 :]
        if g == 0:
            m_in, m_out = pre[pl.ds(in_at, STATE), at], pre[pl.ds(out_at, STATE), at]
            in16 = (m_in * jax.nn.sigmoid(m_in)).astype(BF16)
            out16 = (m_out * jax.nn.sigmoid(m_out)).astype(BF16)
            ins[k] = in16
            outs[k] = out16
            scores[k] = tn(in16, out16)
            cumt[k] = jnp.concatenate([cum, jnp.zeros((group - slots, group), F32)], axis=0).T
        else:
            in16 = ins[k]
        tail16 = (x * spread(step * jnp.exp(last - cum), span)).astype(BF16)
        tails[k, here] = tail16
        held = grad[here]
        states[k, here] = held.astype(BF16)
        leave = spread(jnp.exp(jnp.broadcast_to(last, (slots, STATE))), span)
        grad[here] = leave * held + nt(tail16, in16)

    def map_copy(k):
        return remote(maps.at[1 - core, k], got_map.at[k], msem.at[0, k], msem.at[1, k], sibling)

    def backward(g, k):
        span, mine_v, size = (range(n1), v1, in1) if g == 0 else (range(n1, hp), v2, in2)
        here = slice(span[0] * HEAD_DIM, span[0] * HEAD_DIM + size)
        at = pl.ds(pl.multiple_of(k * group, group), group)
        step, cum = small(steps, k), small(cums, k)
        last = cum[:, group - 1 :]
        x = xs[k, here]
        step_full = spread(step, span)
        u16 = (x * step_full).astype(BF16)
        tail16 = tails[k, here]
        in16, out16 = ins[k], outs[k]
        dy16 = dys[k, here]
        dy = dy16.astype(F32)
        tail = spread(jnp.exp(last - cum), span)
        lead = spread(jnp.exp(cum), span)
        leave = spread(jnp.exp(jnp.broadcast_to(last, (slots, STATE))), span)
        held16 = states[k, here]
        g_out = grad[here]
        g16 = g_out.astype(BF16)
        dy_lead = dy * lead
        lead16 = dy_lead.astype(BF16)

        score = scores[k]
        cum_col = cumt[k]
        d_score = jnp.zeros((group, group), F32)
        du_parts, r_parts = [], []
        for i, h in enumerate(span):
            at_h = slice(i * HEAD_DIM, (i + 1) * HEAD_DIM)
            diff = cum[h : h + 1] - cum_col[:, h : h + 1]
            within = jnp.exp(jnp.where(causal, diff, -1e30))
            mixing = (score * within).astype(BF16)
            d_mix = tn(u16[at_h], dy16[at_h])
            du_parts.append(nt(dy16[at_h], mixing))
            d_score = d_score + d_mix * within
            r_parts.append(jnp.sum(d_mix * mixing.astype(F32), axis=0, keepdims=True))
        du = jnp.concatenate(du_parts, axis=0) + nn(g16, in16) * tail
        from_x = gather_rows(du * x, span)
        from_u = gather_rows(du * u16.astype(F32), span)
        lead_rows = gather_rows(dy_lead * nn(held16, out16), span)
        cross = jnp.sum(gather_rows(g_out * states[k + 1, here].astype(F32), span), axis=1, keepdims=True)
        d_cum = padded(r_parts, span) + lead_rows - from_u
        d_log = summed(d_cum, after) + cross
        d_raw = (from_x + rate * d_log) * small(sigr, k)

        d_score16 = d_score.astype(BF16)
        d_out = nn(in16, d_score16) + tn(held16, lead16)
        d_in = nt(out16, d_score16) + tn(g16, tail16)
        grad[here] = leave * g_out + nt(lead16, out16)
        slope = pre[mine_v : mine_v + size, at]
        gain_full = spread(jnp.broadcast_to(gain, (slots, group)), span)
        grads[mine_v : mine_v + size, at] = ((du * step_full + dy * gain_full) * slope).astype(BF16)
        fill = jnp.zeros((16 - slots, group), F32)
        raw16 = jnp.concatenate([d_raw, fill], axis=0).astype(BF16)
        acc[0] += d_raw
        acc[1] += d_log * (rate * step)
        acc[2] += gather_rows(dy * x, span)
        if g == 0:
            grads[top : top + 16, at] = raw16
            maps[0, k] = d_in
            maps[1, k] = d_out
        else:
            grads[top : top + 16, at] += raw16
            m_in, m_out = pre[pl.ds(in_at, STATE), at], pre[pl.ds(out_at, STATE), at]
            s_in, s_out = jax.nn.sigmoid(m_in), jax.nn.sigmoid(m_out)
            d_in = (maps[0, k] + d_in) * (s_in * (1.0 + m_in * (1.0 - s_in)))
            d_out = (maps[1, k] + d_out) * (s_out * (1.0 + m_out * (1.0 - s_out)))
            maps[0, k] = d_in
            maps[1, k] = d_out
            grads[pl.ds(in_at, STATE), at] = d_in.astype(BF16)
            grads[pl.ds(out_at, STATE), at] = d_out.astype(BF16)
            map_copy(k).start()

            @pl.when(lax.rem(k, 2) != core)
            def _():
                swap(k // 2, k).start()

    def both_ways(g):
        def ahead(k, carry):
            forward(g, k)
            return carry

        def back(n, carry):
            backward(g, chunks - 1 - n)
            return carry

        here = slice(0, in1) if g == 0 else slice(in1, inner)
        lax.fori_loop(0, chunks, ahead, 0, unroll=2)
        states[chunks, here] = grad[here].astype(BF16)
        grad[here] = jnp.zeros_like(grad[here])
        if g == 0:
            for h in range(2, last_z):
                late_hop(h, True)
            all_cots.wait_recv()
        if g == 0:
            lax.fori_loop(0, chunks, back, 0, unroll=2)
        else:
            lax.fori_loop(0, chunks // 2, back, 0, unroll=2)
            serve(0, 1)
            lax.fori_loop(chunks // 2, chunks, back, 0, unroll=2)

    block = wbuf.shape[4]
    many = 4 if seqs % 4 == 0 else 2
    span_rows = many * zeros * block

    def weigh(g, first, size):
        def part_of(q, carry):
            at = pl.ds(pl.multiple_of(q * span_rows, span_rows), span_rows)
            product = nt(tokt[at, :], grads[first : first + size, :])
            for a in range(many):
                for t in range(zeros):
                    lo = (a * zeros + t) * block
                    wbuf[g, t, a % 2, q * (many // 2) + a // 2, :, 0:size] = product[
                        lo : lo + block
                    ].astype(BF16)
            return carry

        lax.fori_loop(0, seqs // many, part_of, 0)

    sizes = (w1, w2 + STATE)

    def back_flow(g, way, t, p):
        landed = rflow if way == 0 else lflow
        peer = up_peer if way == 0 else down_peer
        return remote(
            wbuf.at[g, t, p, :, :, pl.ds(0, sizes[g])], landed.at[g, t, p, :, :, pl.ds(0, sizes[g])],
            rsem.at[g, way, 0, t - 1 + way, p], rsem.at[g, way, 1, t - 1 + way, p], peer,
        )

    def from_ends(g):
        for z, way in ((0, 0), (last_z, 1)):
            if zeros > 1:
                @pl.when(me_z == z)
                def _():
                    for i in range(last_z):
                        for p in (0, 1):
                            back_flow(g, way, last_z - i if way == 0 else i, p).start()

    low = model // 2

    def turn_of(n):
        return lax.rem(chip + 1 + n, chips)

    def swap(i, k):
        return remote(
            grads.at[pl.ds(0, wide), pl.ds(pl.multiple_of(k * group, group), group)],
            sgrads.at[:, pl.ds(pl.multiple_of(i * group, group), group)],
            dsem.at[0, i], dsem.at[1, i], sibling,
        )

    def token_send(i):
        return remote(
            sent.at[i], tok_in.at[chip], ksem.at[0, i], ksem.at[1, chip], (i * 2 + core, me_z)
        )

    def events(z):
        found = []
        for g in (0, 1):
            for p in (0, 1):
                ends = 0.0
                for i in range(last_z):
                    for way in (0, 1):
                        t = last_z - i if way == 0 else i
                        hops = z if way == 0 else last_z - z
                        if hops == 0:
                            continue
                        when = (g * last_z + i) * 2 + p + 1 + 2.2 * hops
                        if t == z:
                            ends = max(ends, when)
                        elif (way == 0) == (z < t):
                            found.append((when, 1 + g, "pass", (way, t, p)))
                found.append((ends + 0.01, 1 + g, "end", p))
            if g == 0:
                found.append((ends + 0.02, 1, "heads", 0))
        return sorted(found, key=lambda e: e[:2])

    served = 4

    def serve(first, final):
        for z in range(zeros):
            listed = events(z)
            soon = [e for e in listed if e[1:3] == (1, "pass")][:served]
            todo = [e for e in listed if e not in soon] if final is None else soon[first:final]
            if todo:
                @pl.when(me_z == z)
                def _():
                    serve_at(z, todo)

    def serve_at(z, todo):
        for _, g, what, p in todo:
            g = g - 1
            if what == "pass":
                way, t, p = p
                landed = rflow if way == 0 else lflow
                back_flow(g, way, t, p).wait_recv()
                wbuf[g, t, p] = (
                    wbuf[g, t, p].astype(F32) + landed[g, t, p].astype(F32)
                ).astype(BF16)
                back_flow(g, way, t, p).start()
            elif what == "heads":
                close_heads()
                drain()
            else:
                finish_piece(z, g, p)

    def head_copy(d):
        return remote(
            hmine, hin.at[me_z], hsem.at[0], hsem.at[1], (me_s, lax.rem(me_z + d, zeros))
        )

    def head_along(d):
        return remote(
            hsum, hall.at[me_s], gsem.at[0], gsem.at[1], (lax.rem(me_s + d, seqs), me_z)
        )

    def all_heads():
        few = pl.ds(0, zeros - 1)
        return remote(hin.at[few], hin.at[few], hsem.at[0], hsem.at[1], sibling)

    def all_steps():
        few = pl.ds(0, zeros - 1)
        return remote(swbuf.at[few], swin.at[few], ysem.at[0], ysem.at[1], sibling)

    def close_heads():
        if zeros > 1:
            all_heads().wait_recv()
        sums = hin[0]
        for d in range(1, zeros):
            sums = sums + hin[d]
        hsum[...] = sums
        hall[me_s] = sums
        for d in range(1, seqs):
            head_along(d).start()

    def drain():
        for g in (0, 1):
            for p in (0, 1):
                for way in (0, 1):
                    for h in range(last_z):
                        @pl.when(sends(way, h))
                        def _():
                            flow(g, way, h, p, 0).wait_send()
        for j in range(zeros):
            shared(j).wait_send()
        for copy in direct + to_sibling + [all_cots]:
            copy.wait_send()

        def gone(k, carry):
            map_copy(k).wait_send()
            return carry

        lax.fori_loop(0, chunks, gone, 0)
        for i in range(chips):
            swap(i, 2 * i + 1 - core).wait_send()
        columns_copy.wait_send()

    def send_steps():
        steps_grad = nt(tokt[...], grads[top : top + 16, :])
        for t in range(zeros):
            lines = [
                steps_grad[(s * zeros + t) * block : (s * zeros + t + 1) * block] for s in range(seqs)
            ]
            swbuf[t] = jnp.concatenate(lines, axis=1).astype(BF16)
        swin[me_z] = swbuf[me_z]

        for d in range(1, zeros):
            steps_copy(d).start()

    def finish_piece(z, g, p):
        if z > 0:
            back_flow(g, 0, z, p).wait_recv()
        if z < last_z:
            back_flow(g, 1, z, p).wait_recv()
        if g == 1 and p == 0:
            if zeros > 1:
                all_steps().wait_recv()
            total = swin[0].astype(F32)
            for d in range(1, zeros):
                total = total + swin[d].astype(F32)
            total = total.astype(BF16)
            for s in range(seqs):
                stsend[s] = total[:, s * 16 : (s + 1) * 16]
            for s in range(seqs):
                @pl.when(me_s != s)
                def _():
                    steps_along(s).start()
        for j in range(seqs // 2):
            s = 2 * j + p
            value = wbuf[g, z, p, j, :, 0 : sizes[g]].astype(F32)
            if z > 0:
                value = value + rflow[g, z, p, j, :, 0 : sizes[g]].astype(F32)
            if z < last_z:
                value = value + lflow[g, z, p, j, :, 0 : sizes[g]].astype(F32)
            zsend[g, s, :, 0 : sizes[g]] = value.astype(BF16)
        for j in range(seqs // 2):
            @pl.when(me_s != 2 * j + p)
            def _():
                along(g, 2 * j + p).start()

    def along(g, s):
        lanes = pl.ds(0, sizes[g])
        return remote(
            zsend.at[g, s, :, lanes], rows_in.at[g, me_s, :, lanes],
            wsem.at[g, 0], wsem.at[g, 1], (s, me_z),
        )

    def steps_along(s):
        return remote(stsend.at[s], stin.at[me_s], xsem.at[0], xsem.at[1], (s, me_z))

    def steps_copy(d):
        target = lax.rem(me_z + d, zeros)
        return remote(
            swbuf.at[target], swin.at[me_z], ysem.at[0], ysem.at[1], (me_s, target)
        )

    grad[...] = jnp.zeros_like(grad)
    acc[...] = jnp.zeros_like(acc)
    grads[pl.ds(top, v2 - top), :] = jnp.zeros((v2 - top, chunks * group), BF16)
    if w2 > in2:
        grads[pl.ds(v2 + in2, w2 - in2), :] = jnp.zeros((w2 - in2, chunks * group), BF16)
    both_ways(0)
    weigh(0, v1, w1)
    from_ends(0)

    for h in range(1, zeros):
        late_hop(h, False)

    columns_copy = remote(
        wall.at[:, pl.ds(v1, wide - v1)], wall2.at[:, pl.ds(v1, wide - v1)], qsem.at[0], qsem.at[1], sibling
    )
    columns_copy.start()
    wall2[:, 0:STATE] = wall[:, STATE:v1]
    wall2[:, STATE:v1] = wall[:, 0:STATE]

    def project_late(i, carry):
        cols = pl.ds(pl.multiple_of(i * batch, batch), batch)
        pre[v2:wide, cols] = tn(wall[:, v2:wide], tokt[:, cols])
        return carry

    lax.fori_loop(0, chunks * group // batch, project_late, 0)
    both_ways(1)
    serve(1, 2)

    send_steps()
    for i in range(chips):
        at = pl.ds(pl.multiple_of((2 * i + core) * group, group), group)
        mgrads[:, i * group : (i + 1) * group] = grads[0:wide, at]
    columns_copy.wait_recv()
    for i in range(chips):
        swap(i, 2 * i + core).wait_recv()
    def back_project(j, carry):
        at = pl.ds(pl.multiple_of(j * low, low), low)
        product = nn(wall[at, :], mgrads[...]) + nn(wall2[at, :], sgrads[...])
        for i in range(chips):
            sent[i, at, :] = product[:, i * group : (i + 1) * group].astype(BF16)
        for turn_j in (0, 1):
            @pl.when(j == turn_j)
            def _():
                serve(2 + turn_j, 3 + turn_j)
        return carry

    lax.fori_loop(0, 2, back_project, 0)
    for n in range(chips):
        @pl.when(turn_of(n) != chip)
        def _():
            token_send(turn_of(n)).start()

    def merge(k, carry):
        map_copy(k).wait_recv()
        at = pl.ds(pl.multiple_of(k * group, group), group)
        grads[extra : extra + STATE, at] = (maps[core, k] + got_map[k]).astype(BF16)
        return carry

    lax.fori_loop(0, chunks, merge, 0)
    wide_head = hmine.shape[1]
    place_row = lax.broadcasted_iota(jnp.int32, (slots, wide_head), 0)
    place = jnp.logical_and(
        lax.broadcasted_iota(jnp.int32, (slots, wide_head), 1) == me_s * hp + place_row, place_row < hp
    )
    lines = [
        jnp.sum(
            jnp.where(place, jnp.sum(acc[i], axis=1, keepdims=True), 0.0), axis=0, keepdims=True
        )
        for i in range(3)
    ]
    hmine[...] = jnp.concatenate(lines + [jnp.zeros((5, wide_head), F32)], axis=0)
    hin[me_z] = hmine[...]

    for d in range(1, zeros):
        head_copy(d).start()

    weigh(1, v2, w2 + STATE)
    from_ends(1)

    serve(None, None)

    for g in (0, 1):
        rows_in[g, me_s] = zsend[g, me_s]
    for d in range(1, chips):
        at = lax.rem(chip + d, chips)
        remote(
            sent.at[at], tok_in.at[at], ksem.at[0, at], ksem.at[1, at], (at * 2 + core, me_z)
        ).wait_recv()
    tok_in[chip] = sent[chip]

    for j in (0, 1):
        at = slice(j * low, (j + 1) * low)
        value = tok_in[0, at, :].astype(F32)
        for source in range(1, chips):
            value = value + tok_in[source, at, :].astype(F32)
        hid[:, at] = value.T.astype(BF16)

    leaving = [pltpu.make_async_copy(hid, hid_hbm, loc.at[0])]
    leaving[0].start()

    def whole(src, dst, sems, count):
        few = pl.ds(0, count)
        return remote(src.at[few], dst.at[few], sems.at[0], sems.at[1], sibling)

    def along_whole(g):
        lanes = pl.ds(0, sizes[g])
        few = pl.ds(0, seqs - 1)
        return remote(
            zsend.at[g, few, :, lanes], rows_in.at[g, few, :, lanes], wsem.at[g, 0], wsem.at[g, 1], sibling
        )

    along_whole(0).wait_recv()
    for s in range(seqs):
        piece_in = rows_in[0, s].astype(F32)
        rows_out[:, s * inner : s * inner + in1] = piece_in[:, :in1]
    whole(hall, hall, gsem, seqs - 1).wait_recv()
    sums = hall[0]
    for s in range(1, seqs):
        sums = sums + hall[s]
    head_out[...] = sums[:3, :heads]
    leaving.append(pltpu.make_async_copy(head_out, head_hbm, loc.at[1]))
    leaving[1].start()
    map_sums = [jnp.zeros((block, STATE), F32), jnp.zeros((block, STATE), F32)]
    stin[me_s] = stsend[me_s]
    whole(stsend, stin, xsem, seqs - 1).wait_recv()
    along_whole(1).wait_recv()
    for s in range(seqs):
        piece_in = rows_in[1, s].astype(F32)
        rows_out[:, s * inner + in1 : (s + 1) * inner] = piece_in[:, :in2]
        base = full + 2 * STATE + s * hp
        rows_out[:, base : base + hp] = stin[s, :, :hp].astype(F32)
        map_sums[s % 2] = map_sums[s % 2] + piece_in[:, w2 : w2 + STATE]
    rows_out[:, full : full + 2 * STATE] = jnp.concatenate(map_sums, axis=1)
    leaving.append(pltpu.make_async_copy(rows_out, rows_hbm, loc.at[2]))
    leaving[2].start()

    for g in (0, 1):
        for p in (0, 1):
            for way in (0, 1):
                for t in range(zeros):
                    if t == (0 if way == 0 else last_z):
                        continue
                    ahead = me_z < t if way == 0 else me_z > t

                    @pl.when(ahead)
                    def _():
                        back_flow(g, way, t, p).wait_send()
    if zeros > 1:
        all_steps().wait_send()
        all_heads().wait_send()
    whole(hall, hall, gsem, seqs - 1).wait_send()
    along_whole(0).wait_send()
    along_whole(1).wait_send()
    whole(stsend, stin, xsem, seqs - 1).wait_send()
    for i in range(chips):
        @pl.when(i != chip)
        def _():
            token_send(i).wait_send()
    for copy in leaving:
        copy.wait()


def mixer_backward(hidden, cotangent, weight, bias, log, gain, seqs, zeros, hp):
    length, model = hidden.shape
    rows = weight.shape[0]
    heads = bias.shape[1]
    inner = hp * HEAD_DIM
    slots = up(hp, 8)
    (n1, w1), (n2, w2) = groups_of(hp)
    wide = 2 * STATE + w1 + w2
    ends = max(w1, w2 + STATE)
    block = rows // seqs
    chips = seqs // 2
    last = max(zeros - 1, 1)
    total = seqs * length
    full = seqs * inner
    span = up(inner + (HEAD_DIM if hp % 2 else 0), 128)
    lanes = up(heads, 128)
    dma = pltpu.SemaphoreType.DMA
    vmem = pl.BlockSpec(memory_space=pltpu.VMEM)
    anywhere = pl.BlockSpec(memory_space=pl.ANY)
    return pl.pallas_call(
        functools.partial(mixer_backward_kernel, seqs, zeros, hp),
        out_shape=(
            jax.ShapeDtypeStruct((length, model), BF16),
            jax.ShapeDtypeStruct((block, full + 2 * STATE + heads), F32),
            jax.ShapeDtypeStruct((3, heads), F32),
        ),
        in_specs=[anywhere] * 3 + [vmem] * 3,
        out_specs=(anywhere,) * 3,
        scratch_shapes=[
            pltpu.VMEM((length, model), BF16),
            pltpu.VMEM((block, full + 2 * STATE + heads), F32),
            pltpu.VMEM((3, heads), F32),
            pltpu.VMEM((rows, span), BF16),
            pltpu.VMEM((rows, heads), BF16),
            pltpu.VMEM((length, full), BF16),
            pltpu.VMEM((full, length), BF16),
            pltpu.VMEM((seqs, length, model), BF16),
            pltpu.VMEM((model, total), BF16),
            pltpu.VMEM((model, wide), BF16),
            pltpu.VMEM((zeros, 2 * STATE + w1, rows), BF16),
            pltpu.VMEM((wide, total), F32),
            pltpu.VMEM((seqs, inner, length), BF16),
            pltpu.VMEM((seqs, inner, length), F32),
            pltpu.VMEM((seqs, inner, length), BF16),
            pltpu.VMEM((seqs + 1, inner, STATE), BF16),
            pltpu.VMEM((wide + STATE, total), BF16),
            pltpu.VMEM((inner, STATE), F32),
            pltpu.VMEM((3, slots, length), F32),
            pltpu.VMEM((seqs * slots, length), F32),
            pltpu.VMEM((seqs * slots, length), F32),
            pltpu.VMEM((seqs, length, length), F32),
            pltpu.VMEM((seqs * slots, length), F32),
            pltpu.VMEM((2, seqs, STATE, length), F32),
            pltpu.VMEM((seqs, STATE, length), F32),
            pltpu.VMEM((model, wide), BF16),
            pltpu.VMEM((wide, chips * length), BF16),
            pltpu.VMEM((wide, chips * length), BF16),
            pltpu.VMEM((chips, model, length), BF16),
            pltpu.VMEM((chips, model, length), BF16),
            pltpu.VMEM((2, zeros, 2, seqs // 2, block, ends), BF16),
            pltpu.VMEM((2, zeros, 2, seqs // 2, block, ends), BF16),
            pltpu.VMEM((2, zeros, 2, seqs // 2, block, ends), BF16),
            pltpu.VMEM((2, seqs, block, ends), BF16),
            pltpu.VMEM((2, seqs, block, ends), BF16),
            pltpu.VMEM((zeros, 8, lanes), F32),
            pltpu.VMEM((8, lanes), F32),
            pltpu.VMEM((8, lanes), F32),
            pltpu.VMEM((seqs, 8, lanes), F32),
            pltpu.VMEM((seqs, STATE, length), BF16),
            pltpu.VMEM((seqs, STATE, length), BF16),
            pltpu.VMEM((seqs, length, length), F32),
            pltpu.VMEM((zeros, block, seqs * 16), BF16),
            pltpu.VMEM((zeros, block, seqs * 16), BF16),
            pltpu.VMEM((seqs, block, 16), BF16),
            pltpu.VMEM((seqs, block, 16), BF16),
            dma((2, 2, 2, last, 2)),
            dma((2, max(4, chips))),
            dma((2, chips)),
            dma((2,)),
            dma((2, zeros)),
            dma((2, seqs)),
            dma((2, chips)),
            dma((2, chips)),
            dma((2, 2, 2, last, 2)),
            dma((2,)),
            dma((2,)),
            dma((2, 2)),
            dma((5,)),
            dma((2,)),
            dma((2,)),
            dma((2,)),
        ],
        compiler_params=pltpu.CompilerParams(
            collective_id=0, has_side_effects=True, vmem_limit_bytes=63 * 1024 * 1024
        ),
        name="mixer_backward",
    )(hidden, cotangent, weight, bias, log, gain)


def store_kernel(*refs):
    count = len(refs) // 3
    sem = refs[-1]
    takes = [pltpu.make_async_copy(refs[i], refs[2 * count + i], sem.at[0, i]) for i in range(count)]
    puts = [
        pltpu.make_async_copy(refs[2 * count + i], refs[count + i], sem.at[1, i]) for i in range(count)
    ]
    for copy in takes:
        copy.start()
    for take, put in zip(takes, puts):
        take.wait()
        put.start()
    for copy in puts:
        copy.wait()


def store(*arrays):
    return pl.pallas_call(
        store_kernel,
        out_shape=tuple(jax.ShapeDtypeStruct(a.shape, a.dtype) for a in arrays),
        in_specs=[pl.BlockSpec(memory_space=pl.ANY)] * len(arrays),
        out_specs=(pl.BlockSpec(memory_space=pl.ANY),) * len(arrays),
        scratch_shapes=[pltpu.VMEM(a.shape, a.dtype) for a in arrays]
        + [pltpu.SemaphoreType.DMA((2, len(arrays)))],
        name="store",
    )(*arrays)


def body(seqs, zeros, hidden, output_grad, input_weight, step_bias, decay_log, skip_gain):
    heads = step_bias.shape[0]
    hp = up(heads, seqs) // seqs
    spare = seqs * hp - heads
    full, total = heads * HEAD_DIM, seqs * hp * HEAD_DIM
    tokens, cot, weight = hidden[0], output_grad[0], input_weight
    params = [step_bias, decay_log, skip_gain]
    if spare:
        cot = jnp.pad(cot, ((0, 0), (0, total - full)))
        gap = jnp.zeros((weight.shape[0], total - full), BF16)
        few = jnp.zeros((weight.shape[0], spare), BF16)
        weight = jnp.concatenate([weight[:, :full], gap, weight[:, full:], few], axis=1)
        params = [jnp.pad(v, (0, spare)) for v in params]
    token_grad, weight_grad, head_grads = mixer_backward(
        tokens, cot, weight, *[v[None] for v in params], seqs, zeros, hp
    )
    token_grad, weight_grad, head_grads = store(token_grad, weight_grad, head_grads)
    if spare:
        weight_grad = jnp.concatenate(
            [weight_grad[:, :full], weight_grad[:, total : total + 2 * STATE + heads]], axis=1
        )
        head_grads = head_grads[:, :heads]
    return (token_grad[None], weight_grad, head_grads)


def solution(mesh):
    placed = (P("zero", "seq", None), P("zero", "seq", None), P("zero", None), P(), P(), P())
    return jax.shard_map(
        functools.partial(body, mesh.shape["seq"], mesh.shape["zero"]),
        mesh=mesh,
        in_specs=placed,
        out_specs=(P("zero", "seq", None), P(("seq", "zero"), None), P()),
        check_vma=False,
    )
```

```python
import functools

import jax
import jax.numpy as jnp
from jax import lax
from jax.experimental import pallas as pl
from jax.experimental.pallas import tpu as pltpu
from jax.sharding import PartitionSpec as P

HEAD_DIM = 64
STATE = 128
MESH = pl.DeviceIdType.MESH
F32 = jnp.float32
BF16 = jnp.bfloat16


def up(size, unit):
    return -(-size // unit) * unit


def nn(a, b):
    return lax.dot_general(a, b, (((1,), (0,)), ((), ())), preferred_element_type=F32)


def nt(a, b):
    return lax.dot_general(a, b, (((1,), (1,)), ((), ())), preferred_element_type=F32)


def tn(a, b):
    return lax.dot_general(a, b, (((0,), (0,)), ((), ())), preferred_element_type=F32)


def halves(a):
    high = a.astype(BF16)
    return high, (a - high.astype(F32)).astype(BF16)


def remote(src, dst, send, recv, peer):
    return pltpu.make_async_remote_copy(src, dst, send, recv, peer, MESH)


def groups_of(hp):
    first = hp - hp // 2
    second = hp - first
    return (first, up(first * HEAD_DIM + 16, 128)), (second, up(second * HEAD_DIM, 128))


def mixer_backward_kernel(
    seqs, zeros, hp,
    hidden, cotangent, weight, bias_in, log_in, gain_in,
    hid_hbm, rows_hbm, head_hbm,
    hid, rows_out, head_out, window, tiny, cotv, cott,
    toks, tokt, wall, wallt, pre, dys, xs, tails, states, grads, grad, acc, steps, cums, cumt, sigr,
    maps, got_map, wall2, mgrads, sgrads, relay, sent, tok_in, wbuf, rflow, lflow, zsend, rows_in, hin, hsum, hmine, hall,
    ins, outs, scores, swbuf, swin, stsend, stin,
    asem, tsem, psem, csem, ssem, msem, dsem, ksem, rsem, gsem, hsem, wsem, loc, ysem, xsem, qsem,
):
    me_s, me_z = lax.axis_index("seq"), lax.axis_index("zero")
    chips = seqs // 2
    chip, core = me_s // 2, lax.rem(me_s, 2)
    sib = me_s // 2 * 2 + 1 - core
    sibling = (sib, me_z)
    length, model = hidden.shape
    rows = weight.shape[0]
    wide = wall.shape[1]
    inner = dys.shape[1]
    (n1, w1), (n2, w2) = groups_of(hp)
    in1, in2 = n1 * HEAD_DIM, n2 * HEAD_DIM
    slots = acc.shape[1]
    full = cotangent.shape[1]
    chunks, group = seqs, length
    v1 = 2 * STATE
    top, v2 = v1 + in1, v1 + w1
    extra = wide
    up_peer, down_peer = (me_s, me_z + 1), (me_s, me_z - 1)
    half = rows // 2
    last_z = zeros - 1
    pairs = 2 * group

    peers = [(lax.rem(me_s + d, seqs), me_z) for d in range(1, seqs)]
    peers += [(me_s, lax.rem(me_z + d, zeros)) for d in range(1, zeros)]
    barrier = pltpu.get_barrier_semaphore()
    for peer in peers:
        pl.semaphore_signal(barrier, inc=1, device_id=peer, device_id_type=MESH)

    start = pl.multiple_of(me_s * inner // 128 * 128, 128)
    mine = pl.ds(pl.multiple_of(me_z * rows, rows), rows)
    fetch = [
        pltpu.make_async_copy(weight.at[:, pl.ds(start, window.shape[1])], window, loc.at[0]),
        pltpu.make_async_copy(
            weight.at[:, pl.ds(pl.multiple_of(full + core * STATE, 128), STATE)],
            wall.at[mine, pl.ds(STATE, STATE)], loc.at[1],
        ),
        pltpu.make_async_copy(weight.at[:, pl.ds(full + 2 * STATE, tiny.shape[1])], tiny, loc.at[2]),
        pltpu.make_async_copy(hidden, toks.at[me_s], loc.at[3]),
        pltpu.make_async_copy(cotangent, cotv, loc.at[4]),
    ]
    for copy in fetch:
        copy.start()
    heads = tiny.shape[1]
    head_row = lax.broadcasted_iota(jnp.int32, (heads, v2 - top), 0)
    head_col = lax.broadcasted_iota(jnp.int32, (heads, v2 - top), 1)
    chosen = jnp.logical_and(head_row == me_s * hp + head_col, head_col < hp)
    chosen = jnp.where(chosen, 1.0, 0.0).astype(BF16)
    fetch[2].wait()
    wall[mine, top:v2] = nn(tiny[...], chosen).astype(BF16)
    fetch[0].wait()
    def place_values(shift):
        wall[mine, v1:top] = window[:, shift : shift + in1]
        wall[mine, v2 : v2 + in2] = window[:, shift + in1 : shift + inner]
        if w2 > in2:
            wall[mine, v2 + in2 : v2 + w2] = jnp.zeros((rows, w2 - in2), BF16)

    if hp % 2:
        shifted = lax.rem(me_s, 2)
        for shift in (0, 1):
            @pl.when(shifted == shift)
            def _():
                place_values(shift * HEAD_DIM)
    else:
        place_values(0)
    fetch[1].wait()
    fetch[3].wait()

    pl.semaphore_wait(barrier, len(peers))

    spans = ((STATE, STATE + w1), (v2, w2))

    def piece(g, at, p):
        first = pl.multiple_of(at * rows + p * half, half)
        return wall.at[pl.ds(first, half), pl.ds(*spans[g])]

    def flow(g, way, h, p, recv):
        at = me_z - h if way == 0 else me_z + h
        return remote(
            piece(g, at, p), piece(g, at, p),
            asem.at[g, way, 0, min(h, last_z - 1), p], asem.at[g, way, 1, h - recv, p],
            up_peer if way == 0 else down_peer,
        )

    def sends(way, h):
        if way == 0:
            return jnp.logical_and(me_z < last_z, me_z >= h)
        return jnp.logical_and(me_z > 0, me_z + h <= last_z)

    def comes(way, h):
        return me_z >= h if way == 0 else me_z + h <= last_z

    def shared(at):
        first = pl.multiple_of(at * rows, rows)
        return remote(
            wall.at[pl.ds(first, rows), pl.ds(STATE, STATE)],
            wall.at[pl.ds(first, rows), pl.ds(0, STATE)],
            ssem.at[0, at], ssem.at[1, at], sibling,
        )

    for p in (0, 1):
        for way in (0, 1):
            @pl.when(sends(way, 0))
            def _():
                flow(0, way, 0, p, 0).start()

    def own_late(h):
        for way in (0, 1):
            distance = me_z if way == 0 else last_z - me_z

            @pl.when(jnp.logical_and(distance == h, sends(way, 0)))
            def _():
                for p in (0, 1):
                    flow(1, way, 0, p, 0).start()

    own_late(0)

    def token(src_s, dst, lo, size, slot):
        block = toks.at[src_s, pl.ds(lo, size)]
        return remote(block, block, tsem.at[0, slot], tsem.at[1, slot], (dst, me_z))

    def passed(src_s, slot):
        return remote(toks.at[src_s], toks.at[src_s], psem.at[0, slot], psem.at[1, slot], sibling)

    square = chips == 4
    cut = length // 2
    to_sibling = [passed(me_s, 0)]
    if square:
        flat = chip + 1 - 2 * lax.rem(chip, 2)
        tall = lax.rem(chip + 2, 4)
        far = lax.rem(flat + 2, 4)
        around = [flat, tall]
    else:
        around = [lax.rem(chip + d, chips) for d in range(1, chips)]
    if square:
        direct = [
            token(me_s, flat * 2 + core, 0, cut, 0),
            token(me_s, tall * 2 + core, cut, length - cut, 1),
            token(me_s, flat * 2 + core, cut, length - cut, 4),
            token(me_s, tall * 2 + core, 0, cut, 5),
        ]
        onward = [
            token(flat * 2 + core, tall * 2 + core, 0, cut, 2),
            token(tall * 2 + core, flat * 2 + core, cut, length - cut, 3),
        ]
    else:
        direct = [token(me_s, c * 2 + core, 0, length, i) for i, c in enumerate(around)]
    for copy in direct + to_sibling:
        copy.start()
    shared(me_z).start()

    pre[...] = jnp.zeros_like(pre)
    fetch[4].wait()
    strip = 512

    def turn_cot(j, carry):
        at = pl.ds(pl.multiple_of(j * strip, strip), strip)
        cott[at, :] = cotv[:, at].T
        return carry

    lax.fori_loop(0, full // strip, turn_cot, 0)

    def cot_of(s):
        return cott.at[pl.ds(pl.multiple_of(s * inner, inner), inner)]

    dys[me_s] = cot_of(me_s)[...]

    def send_on():
        if square:
            for i in (0, 1):
                direct[i].wait_recv()
                onward[i].start()

    def step_hop(h):
        for p in (0, 1):
            if h == 1 and p == 1 and zeros > 2:
                send_on()
            for way in (0, 1):
                @pl.when(comes(way, h))
                def _():
                    flow(0, way, h, p, 1).wait_recv()
                if h < last_z:
                    @pl.when(sends(way, h))
                    def _():
                        flow(0, way, h, p, 0).start()
        if h < last_z:
            own_late(h)
        for way in (0, 1):
            @pl.when(comes(way, h))
            def _():
                shared(me_z - h if way == 0 else me_z + h).start()

    def late_hop(h, onward):
        for p in (0, 1):
            for way in (0, 1):
                goes = sends(way, h) if h < last_z else jnp.bool_(False)
                if onward:
                    if h < last_z:
                        @pl.when(goes)
                        def _():
                            flow(1, way, h, p, 1).wait_recv()
                            flow(1, way, h, p, 0).start()
                else:
                    @pl.when(jnp.logical_and(comes(way, h), jnp.logical_not(goes)))
                    def _():
                        flow(1, way, h, p, 1).wait_recv()

    if zeros > 2:
        step_hop(1)
    else:
        send_on()

    def chip_of(n):
        if square:
            return lax.rem(chip // 2 + n // 2, 2) * 2 + lax.rem(lax.rem(chip, 2) + n % 2, 2)
        return lax.rem(chip + n, chips)

    def turn(n, carry):
        for half_chip in (0, 1):
            k = chip_of(n) * 2 + half_chip
            tokt[:, pl.ds(pl.multiple_of(k * group, group), group)] = toks[k].T
        return carry

    early = 3 if square else 0
    if square:
        for i in (2, 3):
            direct[i].wait_recv()
        direct += onward
        more = [passed(flat * 2 + core, 1), passed(tall * 2 + core, 2)]
        for copy in more:
            copy.start()
        to_sibling += more
        for copy in to_sibling:
            copy.wait_recv()
        lax.fori_loop(0, early, turn, 0)

    cots = []
    for d in range(1, seqs):
        peer = lax.rem(me_s + d, seqs)
        cots.append(remote(cot_of(peer), dys.at[me_s], csem.at[0], csem.at[1], (peer, me_z)))
    for copy in cots:
        copy.start()
    all_cots = remote(
        dys.at[pl.ds(0, seqs - 1)], dys.at[pl.ds(0, seqs - 1)], csem.at[0], csem.at[1], sibling
    )
    for h in range(2, last_z):
        step_hop(h)

    def flip(j):
        shared(j).wait_recv()
        wallt[j] = wall[pl.ds(pl.multiple_of(j * rows, rows), rows), :v2].T

    def project(j, first, final):
        def part_of(n, carry):
            at = pl.ds(pl.multiple_of(j * rows, rows), rows)
            cols = pl.ds(pl.multiple_of(chip_of(n) * pairs, pairs), pairs)
            pre[:v2, cols] += nn(wallt[j], tokt[at, cols])
            return carry

        lax.fori_loop(first, final, part_of, 0)

    def project_all(j):
        def part_of(n, carry):
            at = pl.ds(pl.multiple_of(j * rows, rows), rows)
            cols = pl.ds(pl.multiple_of(n * 2 * pairs, 2 * pairs), 2 * pairs)
            pre[:v2, cols] += nn(wallt[j], tokt[at, cols])
            return carry

        lax.fori_loop(0, chips // 2, part_of, 0)

    def near(first, final, fresh):
        def one(j, carry):
            distance = jnp.abs(j - me_z)
            ready = distance < last_z if zeros > 1 else distance < 1

            @pl.when(ready)
            def _():
                if fresh:
                    flip(j)
                project(j, first, final)
            return carry

        lax.fori_loop(0, zeros, one, 0)

    if square:
        token(far * 2 + core, tall * 2 + core, 0, cut, 2).wait_recv()
        token(far * 2 + core, flat * 2 + core, cut, length - cut, 3).wait_recv()
        rest = [passed(far * 2 + core, 3)]
    else:
        rest = []
        for d in range(1, chips):
            direct[d - 1].wait_recv()
            rest.append(passed(lax.rem(chip - d + chips, chips) * 2 + core, d))
    for copy in rest:
        copy.start()
    if early:
        near(0, early, True)
    if not square:
        rest = to_sibling + rest
    for copy in rest:
        copy.wait_recv()
    to_sibling = to_sibling + rest if square else rest
    lax.fori_loop(early, chips, turn, 0)
    near(early, chips, not early)

    batch = 4 * group if chunks % 4 == 0 else pairs

    if zeros > 2:
        late_hop(1, True)
    if zeros > 1:
        step_hop(last_z)
        far_end = jnp.logical_or(me_z == 0, me_z == last_z)

        @pl.when(far_end)
        def _():
            flip(last_z - me_z)
            project_all(last_z - me_z)

    in_at = pl.multiple_of((1 - core) * STATE, 128)
    out_at = pl.multiple_of(core * STATE, 128)
    slot = lax.broadcasted_iota(jnp.int32, (slots, heads), 0)
    own_head = jnp.logical_and(
        lax.broadcasted_iota(jnp.int32, (slots, heads), 1) == me_s * hp + slot, slot < hp
    )

    def own(ref):
        return jnp.sum(jnp.where(own_head, ref[...], 0.0), axis=1, keepdims=True)

    bias, rate, gain = own(bias_in), -jnp.exp(own(log_in)), own(gain_in)
    row = lax.broadcasted_iota(jnp.int32, (group, group), 0)
    col = lax.broadcasted_iota(jnp.int32, (group, group), 1)
    causal = col >= row

    def spread(values, span):
        return jnp.concatenate(
            [jnp.broadcast_to(values[h : h + 1], (HEAD_DIM, values.shape[1])) for h in span], axis=0
        )

    def gather_rows(whole, span):
        parts = [
            jnp.sum(whole[i * HEAD_DIM : (i + 1) * HEAD_DIM], axis=0, keepdims=True)
            for i in range(len(span))
        ]
        return padded(parts, span)

    def padded(parts, span):
        lanes = parts[0].shape[1]
        if span[0] > 0:
            parts = [jnp.zeros((span[0], lanes), F32)] + parts
        if slots > span[-1] + 1:
            parts = parts + [jnp.zeros((slots - span[-1] - 1, lanes), F32)]
        return jnp.concatenate(parts, axis=0)

    raw = pre[top : top + slots, :] + bias
    soft = jax.nn.softplus(raw)
    curve = jax.nn.sigmoid(raw)
    stacked = jnp.concatenate([soft[:, k * group : (k + 1) * group] for k in range(chunks)], axis=0)
    steps[...] = stacked
    sigr[...] = jnp.concatenate([curve[:, k * group : (k + 1) * group] for k in range(chunks)], axis=0)
    logs = jnp.concatenate([rate] * chunks, axis=0) * stacked
    before = jnp.where(causal, 1.0, 0.0).astype(BF16)
    after = jnp.where(col <= row, 1.0, 0.0).astype(BF16)

    def summed(values, mask):
        a = values.astype(BF16)
        rest = values - a.astype(F32)
        b = rest.astype(BF16)
        c = (rest - b.astype(F32)).astype(BF16)
        return nn(a, mask) + (nn(b, mask) + nn(c, mask))

    cums[...] = summed(logs, before)

    def small(ref, k):
        return ref[pl.ds(pl.multiple_of(k * slots, slots), slots), :]

    def forward(g, k):
        span, mine_v, size = (range(n1), v1, in1) if g == 0 else (range(n1, hp), v2, in2)
        here = slice(span[0] * HEAD_DIM, span[0] * HEAD_DIM + size)
        at = pl.ds(pl.multiple_of(k * group, group), group)
        p = pre[mine_v : mine_v + size, at]
        sig = jax.nn.sigmoid(p)
        x = p * sig
        xs[k, here] = x
        pre[mine_v : mine_v + size, at] = sig * (1.0 + p * (1.0 - sig))
        step, cum = small(steps, k), small(cums, k)
        last = cum[:, group - 1 :]
        if g == 0:
            m_in, m_out = pre[pl.ds(in_at, STATE), at], pre[pl.ds(out_at, STATE), at]
            in16 = (m_in * jax.nn.sigmoid(m_in)).astype(BF16)
            out16 = (m_out * jax.nn.sigmoid(m_out)).astype(BF16)
            ins[k] = in16
            outs[k] = out16
            scores[k] = tn(in16, out16)
            cumt[k] = jnp.concatenate([cum, jnp.zeros((group - slots, group), F32)], axis=0).T
        else:
            in16 = ins[k]
        tail16 = (x * spread(step * jnp.exp(last - cum), span)).astype(BF16)
        tails[k, here] = tail16
        held = grad[here]
        states[k, here] = held.astype(BF16)
        leave = spread(jnp.exp(jnp.broadcast_to(last, (slots, STATE))), span)
        grad[here] = leave * held + nt(tail16, in16)

    def map_copy(k):
        return remote(maps.at[1 - core, k], got_map.at[k], msem.at[0, k], msem.at[1, k], sibling)

    def backward(g, k):
        span, mine_v, size = (range(n1), v1, in1) if g == 0 else (range(n1, hp), v2, in2)
        here = slice(span[0] * HEAD_DIM, span[0] * HEAD_DIM + size)
        at = pl.ds(pl.multiple_of(k * group, group), group)
        step, cum = small(steps, k), small(cums, k)
        last = cum[:, group - 1 :]
        x = xs[k, here]
        step_full = spread(step, span)
        u16 = (x * step_full).astype(BF16)
        tail16 = tails[k, here]
        in16, out16 = ins[k], outs[k]
        dy16 = dys[k, here]
        dy = dy16.astype(F32)
        tail = spread(jnp.exp(last - cum), span)
        lead = spread(jnp.exp(cum), span)
        leave = spread(jnp.exp(jnp.broadcast_to(last, (slots, STATE))), span)
        held16 = states[k, here]
        g_out = grad[here]
        g16 = g_out.astype(BF16)
        dy_lead = dy * lead
        lead16 = dy_lead.astype(BF16)

        score = scores[k]
        cum_col = cumt[k]
        d_score = jnp.zeros((group, group), F32)
        du_parts, r_parts = [], []
        for i, h in enumerate(span):
            at_h = slice(i * HEAD_DIM, (i + 1) * HEAD_DIM)
            diff = cum[h : h + 1] - cum_col[:, h : h + 1]
            within = jnp.exp(jnp.where(causal, diff, -1e30))
            mixing = (score * within).astype(BF16)
            d_mix = tn(u16[at_h], dy16[at_h])
            du_parts.append(nt(dy16[at_h], mixing))
            d_score = d_score + d_mix * within
            r_parts.append(jnp.sum(d_mix * mixing.astype(F32), axis=0, keepdims=True))
        du = jnp.concatenate(du_parts, axis=0) + nn(g16, in16) * tail
        from_x = gather_rows(du * x, span)
        from_u = gather_rows(du * u16.astype(F32), span)
        lead_rows = gather_rows(dy_lead * nn(held16, out16), span)
        cross = jnp.sum(gather_rows(g_out * states[k + 1, here].astype(F32), span), axis=1, keepdims=True)
        d_cum = padded(r_parts, span) + lead_rows - from_u
        d_log = summed(d_cum, after) + cross
        d_raw = (from_x + rate * d_log) * small(sigr, k)

        d_score16 = d_score.astype(BF16)
        d_out = nn(in16, d_score16) + tn(held16, lead16)
        d_in = nt(out16, d_score16) + tn(g16, tail16)
        grad[here] = leave * g_out + nt(lead16, out16)
        slope = pre[mine_v : mine_v + size, at]
        gain_full = spread(jnp.broadcast_to(gain, (slots, group)), span)
        grads[mine_v : mine_v + size, at] = ((du * step_full + dy * gain_full) * slope).astype(BF16)
        fill = jnp.zeros((16 - slots, group), F32)
        raw16 = jnp.concatenate([d_raw, fill], axis=0).astype(BF16)
        acc[0] += d_raw
        acc[1] += d_log * (rate * step)
        acc[2] += gather_rows(dy * x, span)
        if g == 0:
            grads[top : top + 16, at] = raw16
            maps[0, k] = d_in
            maps[1, k] = d_out
        else:
            grads[top : top + 16, at] += raw16
            m_in, m_out = pre[pl.ds(in_at, STATE), at], pre[pl.ds(out_at, STATE), at]
            s_in, s_out = jax.nn.sigmoid(m_in), jax.nn.sigmoid(m_out)
            d_in = (maps[0, k] + d_in) * (s_in * (1.0 + m_in * (1.0 - s_in)))
            d_out = (maps[1, k] + d_out) * (s_out * (1.0 + m_out * (1.0 - s_out)))
            maps[0, k] = d_in
            maps[1, k] = d_out
            grads[pl.ds(in_at, STATE), at] = d_in.astype(BF16)
            grads[pl.ds(out_at, STATE), at] = d_out.astype(BF16)
            map_copy(k).start()

            @pl.when(lax.rem(k, 2) != core)
            def _():
                swap(k // 2, k).start()

    def both_ways(g):
        def ahead(k, carry):
            forward(g, k)
            return carry

        def back(n, carry):
            backward(g, chunks - 1 - n)
            return carry

        here = slice(0, in1) if g == 0 else slice(in1, inner)
        lax.fori_loop(0, chunks, ahead, 0, unroll=2)
        states[chunks, here] = grad[here].astype(BF16)
        grad[here] = jnp.zeros_like(grad[here])
        if g == 0:
            for h in range(2, last_z):
                late_hop(h, True)
            all_cots.wait_recv()
        if g == 0:
            lax.fori_loop(0, chunks, back, 0, unroll=2)
        else:
            lax.fori_loop(0, chunks // 2, back, 0, unroll=2)
            serve(0, 1)
            lax.fori_loop(chunks // 2, chunks, back, 0, unroll=2)

    block = wbuf.shape[4]
    many = 4 if seqs % 4 == 0 else 2
    span_rows = many * zeros * block

    def weigh(g, first, size):
        def part_of(q, carry):
            at = pl.ds(pl.multiple_of(q * span_rows, span_rows), span_rows)
            product = nt(tokt[at, :], grads[first : first + size, :])
            for a in range(many):
                for t in range(zeros):
                    lo = (a * zeros + t) * block
                    wbuf[g, t, a % 2, q * (many // 2) + a // 2, :, 0:size] = product[
                        lo : lo + block
                    ].astype(BF16)
            return carry

        lax.fori_loop(0, seqs // many, part_of, 0)

    sizes = (w1, w2 + STATE)

    def back_flow(g, way, t, p):
        landed = rflow if way == 0 else lflow
        peer = up_peer if way == 0 else down_peer
        return remote(
            wbuf.at[g, t, p, :, :, pl.ds(0, sizes[g])], landed.at[g, t, p, :, :, pl.ds(0, sizes[g])],
            rsem.at[g, way, 0, t - 1 + way, p], rsem.at[g, way, 1, t - 1 + way, p], peer,
        )

    def from_ends(g):
        for z, way in ((0, 0), (last_z, 1)):
            if zeros > 1:
                @pl.when(me_z == z)
                def _():
                    for i in range(last_z):
                        for p in (0, 1):
                            back_flow(g, way, last_z - i if way == 0 else i, p).start()

    low = model // 2

    def turn_of(n):
        return lax.rem(chip + 1 + n, chips)

    def swap(i, k):
        return remote(
            grads.at[pl.ds(0, wide), pl.ds(pl.multiple_of(k * group, group), group)],
            sgrads.at[:, pl.ds(pl.multiple_of(i * group, group), group)],
            dsem.at[0, i], dsem.at[1, i], sibling,
        )

    def token_send(i):
        return remote(
            sent.at[i], tok_in.at[chip], ksem.at[0, i], ksem.at[1, chip], (i * 2 + core, me_z)
        )

    def plane_copy(part_no):
        to_flat = part_no % 2 == 0
        peer = (flat if to_flat else tall) * 2 + core
        first_half = part_no in (0, 2, 5)
        at = pl.ds(0 if first_half else low, low)
        if part_no < 2:
            src, dst = sent.at[far, at], relay.at[part_no]
        else:
            src, dst = sent.at[flat if to_flat else tall, at], tok_in.at[chip, at]
        return remote(src, dst, ksem.at[0, part_no], ksem.at[1, part_no], (peer, me_z))

    def relay_on():
        if square:
            for part_no, target, lo in ((1, flat, low), (0, tall, 0)):
                plane_copy(part_no).wait_recv()
                at = slice(lo, lo + low)
                sent[target, at, :] = (
                    sent[target, at, :].astype(F32) + relay[part_no].astype(F32)
                ).astype(BF16)
                plane_copy(4 + (1 - part_no)).start()

    def events(z):
        found = [(9.7, 2, "relay", 0)]
        for g in (0, 1):
            for p in (0, 1):
                ends = 0.0
                for i in range(last_z):
                    for way in (0, 1):
                        t = last_z - i if way == 0 else i
                        hops = z if way == 0 else last_z - z
                        if hops == 0:
                            continue
                        when = (g * last_z + i) * 2 + p + 1 + 2.2 * hops
                        if t == z:
                            ends = max(ends, when)
                        elif (way == 0) == (z < t):
                            found.append((when, 1 + g, "pass", (way, t, p)))
                found.append((ends + 0.01, 1 + g, "end", p))
            if g == 0:
                found.append((ends + 0.02, 1, "heads", 0))
        return sorted(found, key=lambda e: e[:2])

    served = 4

    def serve(first, final):
        for z in range(zeros):
            listed = events(z)
            soon = [e for e in listed if e[1:3] == (1, "pass")][:served]
            todo = [e for e in listed if e not in soon] if final is None else soon[first:final]
            if todo:
                @pl.when(me_z == z)
                def _():
                    serve_at(z, todo)

    def serve_at(z, todo):
        for _, g, what, p in todo:
            g = g - 1
            if what == "pass":
                way, t, p = p
                landed = rflow if way == 0 else lflow
                back_flow(g, way, t, p).wait_recv()
                wbuf[g, t, p] = (
                    wbuf[g, t, p].astype(F32) + landed[g, t, p].astype(F32)
                ).astype(BF16)
                back_flow(g, way, t, p).start()
            elif what == "relay":
                relay_on()
            elif what == "heads":
                close_heads()
                drain()
            else:
                finish_piece(z, g, p)

    def head_copy(d):
        return remote(
            hmine, hin.at[me_z], hsem.at[0], hsem.at[1], (me_s, lax.rem(me_z + d, zeros))
        )

    def head_along(d):
        return remote(
            hsum, hall.at[me_s], gsem.at[0], gsem.at[1], (lax.rem(me_s + d, seqs), me_z)
        )

    def all_heads():
        few = pl.ds(0, zeros - 1)
        return remote(hin.at[few], hin.at[few], hsem.at[0], hsem.at[1], sibling)

    def all_steps():
        few = pl.ds(0, zeros - 1)
        return remote(swbuf.at[few], swin.at[few], ysem.at[0], ysem.at[1], sibling)

    def close_heads():
        if zeros > 1:
            all_heads().wait_recv()
        sums = hin[0]
        for d in range(1, zeros):
            sums = sums + hin[d]
        hsum[...] = sums
        hall[me_s] = sums
        for d in range(1, seqs):
            head_along(d).start()

    def drain():
        for g in (0, 1):
            for p in (0, 1):
                for way in (0, 1):
                    for h in range(last_z):
                        @pl.when(sends(way, h))
                        def _():
                            flow(g, way, h, p, 0).wait_send()
        for j in range(zeros):
            shared(j).wait_send()
        for copy in direct + to_sibling + [all_cots]:
            copy.wait_send()

        def gone(k, carry):
            map_copy(k).wait_send()
            return carry

        lax.fori_loop(0, chunks, gone, 0)
        for i in range(chips):
            swap(i, 2 * i + 1 - core).wait_send()
        columns_copy.wait_send()

    def send_steps():
        steps_grad = nt(tokt[...], grads[top : top + 16, :])
        for t in range(zeros):
            lines = [
                steps_grad[(s * zeros + t) * block : (s * zeros + t + 1) * block] for s in range(seqs)
            ]
            swbuf[t] = jnp.concatenate(lines, axis=1).astype(BF16)
        swin[me_z] = swbuf[me_z]

        for d in range(1, zeros):
            steps_copy(d).start()

    def finish_piece(z, g, p):
        if z > 0:
            back_flow(g, 0, z, p).wait_recv()
        if z < last_z:
            back_flow(g, 1, z, p).wait_recv()
        if g == 1 and p == 0:
            if zeros > 1:
                all_steps().wait_recv()
            total = swin[0].astype(F32)
            for d in range(1, zeros):
                total = total + swin[d].astype(F32)
            total = total.astype(BF16)
            for s in range(seqs):
                stsend[s] = total[:, s * 16 : (s + 1) * 16]
            for s in range(seqs):
                @pl.when(me_s != s)
                def _():
                    steps_along(s).start()
        for j in range(seqs // 2):
            s = 2 * j + p
            value = wbuf[g, z, p, j, :, 0 : sizes[g]].astype(F32)
            if z > 0:
                value = value + rflow[g, z, p, j, :, 0 : sizes[g]].astype(F32)
            if z < last_z:
                value = value + lflow[g, z, p, j, :, 0 : sizes[g]].astype(F32)
            zsend[g, s, :, 0 : sizes[g]] = value.astype(BF16)
        for j in range(seqs // 2):
            @pl.when(me_s != 2 * j + p)
            def _():
                along(g, 2 * j + p).start()

    def along(g, s):
        lanes = pl.ds(0, sizes[g])
        return remote(
            zsend.at[g, s, :, lanes], rows_in.at[g, me_s, :, lanes],
            wsem.at[g, 0], wsem.at[g, 1], (s, me_z),
        )

    def steps_along(s):
        return remote(stsend.at[s], stin.at[me_s], xsem.at[0], xsem.at[1], (s, me_z))

    def steps_copy(d):
        target = lax.rem(me_z + d, zeros)
        return remote(
            swbuf.at[target], swin.at[me_z], ysem.at[0], ysem.at[1], (me_s, target)
        )

    grad[...] = jnp.zeros_like(grad)
    acc[...] = jnp.zeros_like(acc)
    grads[pl.ds(top, v2 - top), :] = jnp.zeros((v2 - top, chunks * group), BF16)
    if w2 > in2:
        grads[pl.ds(v2 + in2, w2 - in2), :] = jnp.zeros((w2 - in2, chunks * group), BF16)
    both_ways(0)
    weigh(0, v1, w1)
    from_ends(0)

    for h in range(1, zeros):
        late_hop(h, False)

    columns_copy = remote(
        wall.at[:, pl.ds(v1, wide - v1)], wall2.at[:, pl.ds(v1, wide - v1)], qsem.at[0], qsem.at[1], sibling
    )
    columns_copy.start()
    wall2[:, 0:STATE] = wall[:, STATE:v1]
    wall2[:, STATE:v1] = wall[:, 0:STATE]

    def project_late(i, carry):
        cols = pl.ds(pl.multiple_of(i * batch, batch), batch)
        pre[v2:wide, cols] = tn(wall[:, v2:wide], tokt[:, cols])
        return carry

    lax.fori_loop(0, chunks * group // batch, project_late, 0)
    both_ways(1)
    serve(1, 2)

    send_steps()
    for i in range(chips):
        at = pl.ds(pl.multiple_of((2 * i + core) * group, group), group)
        mgrads[:, i * group : (i + 1) * group] = grads[0:wide, at]
    columns_copy.wait_recv()
    for i in range(chips):
        swap(i, 2 * i + core).wait_recv()
    def back_project(j, carry):
        at = pl.ds(pl.multiple_of(j * low, low), low)
        product = nn(wall[at, :], mgrads[...]) + nn(wall2[at, :], sgrads[...])
        for i in range(chips):
            sent[i, at, :] = product[:, i * group : (i + 1) * group].astype(BF16)
        for turn_j in (0, 1):
            @pl.when(j == turn_j)
            def _():
                serve(2 + turn_j, 3 + turn_j)
        return carry

    lax.fori_loop(0, 2, back_project, 0)
    if square:
        for part_no in (0, 1, 2, 3):
            plane_copy(part_no).start()
    else:
        for n in range(chips):
            @pl.when(turn_of(n) != chip)
            def _():
                token_send(turn_of(n)).start()

    def merge(k, carry):
        map_copy(k).wait_recv()
        at = pl.ds(pl.multiple_of(k * group, group), group)
        grads[extra : extra + STATE, at] = (maps[core, k] + got_map[k]).astype(BF16)
        return carry

    lax.fori_loop(0, chunks, merge, 0)
    wide_head = hmine.shape[1]
    place_row = lax.broadcasted_iota(jnp.int32, (slots, wide_head), 0)
    place = jnp.logical_and(
        lax.broadcasted_iota(jnp.int32, (slots, wide_head), 1) == me_s * hp + place_row, place_row < hp
    )
    lines = [
        jnp.sum(
            jnp.where(place, jnp.sum(acc[i], axis=1, keepdims=True), 0.0), axis=0, keepdims=True
        )
        for i in range(3)
    ]
    hmine[...] = jnp.concatenate(lines + [jnp.zeros((5, wide_head), F32)], axis=0)
    hin[me_z] = hmine[...]

    for d in range(1, zeros):
        head_copy(d).start()

    weigh(1, v2, w2 + STATE)
    from_ends(1)

    serve(None, None)

    for g in (0, 1):
        rows_in[g, me_s] = zsend[g, me_s]
    if square:
        for part_no in (2, 3, 4, 5):
            plane_copy(part_no).wait_recv()
        sources = [flat, tall]
    else:
        for d in range(1, chips):
            at = lax.rem(chip + d, chips)
            remote(
                sent.at[at], tok_in.at[at], ksem.at[0, at], ksem.at[1, at], (at * 2 + core, me_z)
            ).wait_recv()
        sources = [lax.rem(chip + d, chips) for d in range(1, chips)]

    for j in (0, 1):
        at = slice(j * low, (j + 1) * low)
        value = sent[chip, at, :].astype(F32)
        for source in sources:
            value = value + tok_in[source, at, :].astype(F32)
        hid[:, at] = value.T.astype(BF16)

    leaving = [pltpu.make_async_copy(hid, hid_hbm, loc.at[0])]
    leaving[0].start()

    def whole(src, dst, sems, count):
        few = pl.ds(0, count)
        return remote(src.at[few], dst.at[few], sems.at[0], sems.at[1], sibling)

    def along_whole(g):
        lanes = pl.ds(0, sizes[g])
        few = pl.ds(0, seqs - 1)
        return remote(
            zsend.at[g, few, :, lanes], rows_in.at[g, few, :, lanes], wsem.at[g, 0], wsem.at[g, 1], sibling
        )

    along_whole(0).wait_recv()
    for s in range(seqs):
        piece_in = rows_in[0, s].astype(F32)
        rows_out[:, s * inner : s * inner + in1] = piece_in[:, :in1]
    whole(hall, hall, gsem, seqs - 1).wait_recv()
    sums = hall[0]
    for s in range(1, seqs):
        sums = sums + hall[s]
    head_out[...] = sums[:3, :heads]
    leaving.append(pltpu.make_async_copy(head_out, head_hbm, loc.at[1]))
    leaving[1].start()
    map_sums = [jnp.zeros((block, STATE), F32), jnp.zeros((block, STATE), F32)]
    stin[me_s] = stsend[me_s]
    whole(stsend, stin, xsem, seqs - 1).wait_recv()
    along_whole(1).wait_recv()
    for s in range(seqs):
        piece_in = rows_in[1, s].astype(F32)
        rows_out[:, s * inner + in1 : (s + 1) * inner] = piece_in[:, :in2]
        base = full + 2 * STATE + s * hp
        rows_out[:, base : base + hp] = stin[s, :, :hp].astype(F32)
        map_sums[s % 2] = map_sums[s % 2] + piece_in[:, w2 : w2 + STATE]
    rows_out[:, full : full + 2 * STATE] = jnp.concatenate(map_sums, axis=1)
    leaving.append(pltpu.make_async_copy(rows_out, rows_hbm, loc.at[2]))
    leaving[2].start()

    for g in (0, 1):
        for p in (0, 1):
            for way in (0, 1):
                for t in range(zeros):
                    if t == (0 if way == 0 else last_z):
                        continue
                    ahead = me_z < t if way == 0 else me_z > t

                    @pl.when(ahead)
                    def _():
                        back_flow(g, way, t, p).wait_send()
    if zeros > 1:
        all_steps().wait_send()
        all_heads().wait_send()
    whole(hall, hall, gsem, seqs - 1).wait_send()
    along_whole(0).wait_send()
    along_whole(1).wait_send()
    whole(stsend, stin, xsem, seqs - 1).wait_send()
    if square:
        for part_no in range(6):
            plane_copy(part_no).wait_send()
    else:
        for i in range(chips):
            @pl.when(i != chip)
            def _():
                token_send(i).wait_send()
    for copy in leaving:
        copy.wait()


def mixer_backward(hidden, cotangent, weight, bias, log, gain, seqs, zeros, hp):
    length, model = hidden.shape
    rows = weight.shape[0]
    heads = bias.shape[1]
    inner = hp * HEAD_DIM
    slots = up(hp, 8)
    (n1, w1), (n2, w2) = groups_of(hp)
    wide = 2 * STATE + w1 + w2
    ends = max(w1, w2 + STATE)
    block = rows // seqs
    chips = seqs // 2
    last = max(zeros - 1, 1)
    total = seqs * length
    full = seqs * inner
    span = up(inner + (HEAD_DIM if hp % 2 else 0), 128)
    lanes = up(heads, 128)
    dma = pltpu.SemaphoreType.DMA
    vmem = pl.BlockSpec(memory_space=pltpu.VMEM)
    anywhere = pl.BlockSpec(memory_space=pl.ANY)
    return pl.pallas_call(
        functools.partial(mixer_backward_kernel, seqs, zeros, hp),
        out_shape=(
            jax.ShapeDtypeStruct((length, model), BF16),
            jax.ShapeDtypeStruct((block, full + 2 * STATE + heads), F32),
            jax.ShapeDtypeStruct((3, heads), F32),
        ),
        in_specs=[anywhere] * 3 + [vmem] * 3,
        out_specs=(anywhere,) * 3,
        scratch_shapes=[
            pltpu.VMEM((length, model), BF16),
            pltpu.VMEM((block, full + 2 * STATE + heads), F32),
            pltpu.VMEM((3, heads), F32),
            pltpu.VMEM((rows, span), BF16),
            pltpu.VMEM((rows, heads), BF16),
            pltpu.VMEM((length, full), BF16),
            pltpu.VMEM((full, length), BF16),
            pltpu.VMEM((seqs, length, model), BF16),
            pltpu.VMEM((model, total), BF16),
            pltpu.VMEM((model, wide), BF16),
            pltpu.VMEM((zeros, 2 * STATE + w1, rows), BF16),
            pltpu.VMEM((wide, total), F32),
            pltpu.VMEM((seqs, inner, length), BF16),
            pltpu.VMEM((seqs, inner, length), F32),
            pltpu.VMEM((seqs, inner, length), BF16),
            pltpu.VMEM((seqs + 1, inner, STATE), BF16),
            pltpu.VMEM((wide + STATE, total), BF16),
            pltpu.VMEM((inner, STATE), F32),
            pltpu.VMEM((3, slots, length), F32),
            pltpu.VMEM((seqs * slots, length), F32),
            pltpu.VMEM((seqs * slots, length), F32),
            pltpu.VMEM((seqs, length, length), F32),
            pltpu.VMEM((seqs * slots, length), F32),
            pltpu.VMEM((2, seqs, STATE, length), F32),
            pltpu.VMEM((seqs, STATE, length), F32),
            pltpu.VMEM((model, wide), BF16),
            pltpu.VMEM((wide, chips * length), BF16),
            pltpu.VMEM((wide, chips * length), BF16),
            pltpu.VMEM((2, model // 2, length), BF16),
            pltpu.VMEM((chips, model, length), BF16),
            pltpu.VMEM((chips, model, length), BF16),
            pltpu.VMEM((2, zeros, 2, seqs // 2, block, ends), BF16),
            pltpu.VMEM((2, zeros, 2, seqs // 2, block, ends), BF16),
            pltpu.VMEM((2, zeros, 2, seqs // 2, block, ends), BF16),
            pltpu.VMEM((2, seqs, block, ends), BF16),
            pltpu.VMEM((2, seqs, block, ends), BF16),
            pltpu.VMEM((zeros, 8, lanes), F32),
            pltpu.VMEM((8, lanes), F32),
            pltpu.VMEM((8, lanes), F32),
            pltpu.VMEM((seqs, 8, lanes), F32),
            pltpu.VMEM((seqs, STATE, length), BF16),
            pltpu.VMEM((seqs, STATE, length), BF16),
            pltpu.VMEM((seqs, length, length), F32),
            pltpu.VMEM((zeros, block, seqs * 16), BF16),
            pltpu.VMEM((zeros, block, seqs * 16), BF16),
            pltpu.VMEM((seqs, block, 16), BF16),
            pltpu.VMEM((seqs, block, 16), BF16),
            dma((2, 2, 2, last, 2)),
            dma((2, max(6, chips))),
            dma((2, chips)),
            dma((2,)),
            dma((2, zeros)),
            dma((2, seqs)),
            dma((2, chips)),
            dma((2, max(6, chips))),
            dma((2, 2, 2, last, 2)),
            dma((2,)),
            dma((2,)),
            dma((2, 2)),
            dma((5,)),
            dma((2,)),
            dma((2,)),
            dma((2,)),
        ],
        compiler_params=pltpu.CompilerParams(
            collective_id=0, has_side_effects=True, vmem_limit_bytes=63 * 1024 * 1024
        ),
        name="mixer_backward",
    )(hidden, cotangent, weight, bias, log, gain)


def store_kernel(*refs):
    count = len(refs) // 3
    sem = refs[-1]
    takes = [pltpu.make_async_copy(refs[i], refs[2 * count + i], sem.at[0, i]) for i in range(count)]
    puts = [
        pltpu.make_async_copy(refs[2 * count + i], refs[count + i], sem.at[1, i]) for i in range(count)
    ]
    for copy in takes:
        copy.start()
    for take, put in zip(takes, puts):
        take.wait()
        put.start()
    for copy in puts:
        copy.wait()


def store(*arrays):
    return pl.pallas_call(
        store_kernel,
        out_shape=tuple(jax.ShapeDtypeStruct(a.shape, a.dtype) for a in arrays),
        in_specs=[pl.BlockSpec(memory_space=pl.ANY)] * len(arrays),
        out_specs=(pl.BlockSpec(memory_space=pl.ANY),) * len(arrays),
        scratch_shapes=[pltpu.VMEM(a.shape, a.dtype) for a in arrays]
        + [pltpu.SemaphoreType.DMA((2, len(arrays)))],
        name="store",
    )(*arrays)


def body(seqs, zeros, hidden, output_grad, input_weight, step_bias, decay_log, skip_gain):
    heads = step_bias.shape[0]
    hp = up(heads, seqs) // seqs
    spare = seqs * hp - heads
    full, total = heads * HEAD_DIM, seqs * hp * HEAD_DIM
    tokens, cot, weight = hidden[0], output_grad[0], input_weight
    params = [step_bias, decay_log, skip_gain]
    if spare:
        cot = jnp.pad(cot, ((0, 0), (0, total - full)))
        gap = jnp.zeros((weight.shape[0], total - full), BF16)
        few = jnp.zeros((weight.shape[0], spare), BF16)
        weight = jnp.concatenate([weight[:, :full], gap, weight[:, full:], few], axis=1)
        params = [jnp.pad(v, (0, spare)) for v in params]
    token_grad, weight_grad, head_grads = mixer_backward(
        tokens, cot, weight, *[v[None] for v in params], seqs, zeros, hp
    )
    token_grad, weight_grad, head_grads = store(token_grad, weight_grad, head_grads)
    if spare:
        weight_grad = jnp.concatenate(
            [weight_grad[:, :full], weight_grad[:, total : total + 2 * STATE + heads]], axis=1
        )
        head_grads = head_grads[:, :heads]
    return (token_grad[None], weight_grad, head_grads)


def solution(mesh):
    placed = (P("zero", "seq", None), P("zero", "seq", None), P("zero", None), P(), P(), P())
    return jax.shard_map(
        functools.partial(body, mesh.shape["seq"], mesh.shape["zero"]),
        mesh=mesh,
        in_specs=placed,
        out_specs=(P("zero", "seq", None), P(("seq", "zero"), None), P()),
        check_vma=False,
    )
```

```python
import functools

import jax
import jax.numpy as jnp
from jax import lax
from jax.experimental import pallas as pl
from jax.experimental.pallas import tpu as pltpu
from jax.sharding import PartitionSpec as P

HEAD_DIM = 64
STATE = 128
MESH = pl.DeviceIdType.MESH
F32 = jnp.float32
BF16 = jnp.bfloat16


def up(size, unit):
    return -(-size // unit) * unit


def nn(a, b):
    return lax.dot_general(a, b, (((1,), (0,)), ((), ())), preferred_element_type=F32)


def nt(a, b):
    return lax.dot_general(a, b, (((1,), (1,)), ((), ())), preferred_element_type=F32)


def tn(a, b):
    return lax.dot_general(a, b, (((0,), (0,)), ((), ())), preferred_element_type=F32)


def halves(a):
    high = a.astype(BF16)
    return high, (a - high.astype(F32)).astype(BF16)


def remote(src, dst, send, recv, peer):
    return pltpu.make_async_remote_copy(src, dst, send, recv, peer, MESH)


def groups_of(hp):
    first = hp - hp // 2
    second = hp - first
    return (first, up(first * HEAD_DIM + 16, 128)), (second, up(second * HEAD_DIM, 128))


def mixer_backward_kernel(
    seqs, zeros, hp,
    hidden, cotangent, weight, bias_in, log_in, gain_in,
    hid_hbm, rows_hbm, head_hbm,
    hid, rows_out, head_out, window, tiny, cotv, cott,
    toks, tokt, wall, wallt, pre, dys, xs, tails, states, grads, grad, acc, steps, cums, cumt, sigr,
    maps, got_map, wall2, mgrads, sgrads, relay, sent, tok_in, wbuf, rflow, lflow, zsend, rows_in, hin, hsum, hmine, hall,
    ins, outs, scores, swbuf, swin, stsend, stin,
    asem, tsem, psem, csem, ssem, msem, dsem, ksem, rsem, gsem, hsem, wsem, loc, ysem, xsem, qsem,
):
    me_s, me_z = lax.axis_index("seq"), lax.axis_index("zero")
    chips = seqs // 2
    chip, core = me_s // 2, lax.rem(me_s, 2)
    sib = me_s // 2 * 2 + 1 - core
    sibling = (sib, me_z)
    length, model = hidden.shape
    rows = weight.shape[0]
    wide = wall.shape[1]
    inner = dys.shape[1]
    (n1, w1), (n2, w2) = groups_of(hp)
    in1, in2 = n1 * HEAD_DIM, n2 * HEAD_DIM
    slots = acc.shape[1]
    full = cotangent.shape[1]
    chunks, group = seqs, length
    v1 = 2 * STATE
    top, v2 = v1 + in1, v1 + w1
    extra = wide
    up_peer, down_peer = (me_s, me_z + 1), (me_s, me_z - 1)
    half = rows // 2
    last_z = zeros - 1
    pairs = 2 * group

    peers = [(lax.rem(me_s + d, seqs), me_z) for d in range(1, seqs)]
    peers += [(me_s, lax.rem(me_z + d, zeros)) for d in range(1, zeros)]
    barrier = pltpu.get_barrier_semaphore()
    for peer in peers:
        pl.semaphore_signal(barrier, inc=1, device_id=peer, device_id_type=MESH)

    start = pl.multiple_of(me_s * inner // 128 * 128, 128)
    mine = pl.ds(pl.multiple_of(me_z * rows, rows), rows)
    fetch = [
        pltpu.make_async_copy(weight.at[:, pl.ds(start, window.shape[1])], window, loc.at[0]),
        pltpu.make_async_copy(
            weight.at[:, pl.ds(pl.multiple_of(full + core * STATE, 128), STATE)],
            wall.at[mine, pl.ds(STATE, STATE)], loc.at[1],
        ),
        pltpu.make_async_copy(weight.at[:, pl.ds(full + 2 * STATE, tiny.shape[1])], tiny, loc.at[2]),
        pltpu.make_async_copy(hidden, toks.at[me_s], loc.at[3]),
        pltpu.make_async_copy(cotangent, cotv, loc.at[4]),
    ]
    for copy in fetch:
        copy.start()
    heads = tiny.shape[1]
    head_row = lax.broadcasted_iota(jnp.int32, (heads, v2 - top), 0)
    head_col = lax.broadcasted_iota(jnp.int32, (heads, v2 - top), 1)
    chosen = jnp.logical_and(head_row == me_s * hp + head_col, head_col < hp)
    chosen = jnp.where(chosen, 1.0, 0.0).astype(BF16)
    fetch[2].wait()
    wall[mine, top:v2] = nn(tiny[...], chosen).astype(BF16)
    fetch[0].wait()
    def place_values(shift):
        wall[mine, v1:top] = window[:, shift : shift + in1]
        wall[mine, v2 : v2 + in2] = window[:, shift + in1 : shift + inner]
        if w2 > in2:
            wall[mine, v2 + in2 : v2 + w2] = jnp.zeros((rows, w2 - in2), BF16)

    if hp % 2:
        shifted = lax.rem(me_s, 2)
        for shift in (0, 1):
            @pl.when(shifted == shift)
            def _():
                place_values(shift * HEAD_DIM)
    else:
        place_values(0)
    fetch[1].wait()
    fetch[3].wait()

    pl.semaphore_wait(barrier, len(peers))

    spans = ((STATE, STATE + w1), (v2, w2))

    def piece(g, at, p):
        first = pl.multiple_of(at * rows + p * half, half)
        return wall.at[pl.ds(first, half), pl.ds(*spans[g])]

    def flow(g, way, h, p, recv):
        at = me_z - h if way == 0 else me_z + h
        return remote(
            piece(g, at, p), piece(g, at, p),
            asem.at[g, way, 0, min(h, last_z - 1), p], asem.at[g, way, 1, h - recv, p],
            up_peer if way == 0 else down_peer,
        )

    def sends(way, h):
        if way == 0:
            return jnp.logical_and(me_z < last_z, me_z >= h)
        return jnp.logical_and(me_z > 0, me_z + h <= last_z)

    def comes(way, h):
        return me_z >= h if way == 0 else me_z + h <= last_z

    def shared(at):
        first = pl.multiple_of(at * rows, rows)
        return remote(
            wall.at[pl.ds(first, rows), pl.ds(STATE, STATE)],
            wall.at[pl.ds(first, rows), pl.ds(0, STATE)],
            ssem.at[0, at], ssem.at[1, at], sibling,
        )

    for p in (0, 1):
        for way in (0, 1):
            @pl.when(sends(way, 0))
            def _():
                flow(0, way, 0, p, 0).start()

    def own_late(h):
        for way in (0, 1):
            distance = me_z if way == 0 else last_z - me_z

            @pl.when(jnp.logical_and(distance == h, sends(way, 0)))
            def _():
                for p in (0, 1):
                    flow(1, way, 0, p, 0).start()

    own_late(0)

    def token(src_s, dst, lo, size, slot):
        block = toks.at[src_s, pl.ds(lo, size)]
        return remote(block, block, tsem.at[0, slot], tsem.at[1, slot], (dst, me_z))

    def passed(src_s, slot):
        return remote(toks.at[src_s], toks.at[src_s], psem.at[0, slot], psem.at[1, slot], sibling)

    square = chips == 4
    cut = length // 2
    to_sibling = [passed(me_s, 0)]
    if square:
        flat = chip + 1 - 2 * lax.rem(chip, 2)
        tall = lax.rem(chip + 2, 4)
        far = lax.rem(flat + 2, 4)
        around = [flat, tall]
    else:
        around = [lax.rem(chip + d, chips) for d in range(1, chips)]
    if square:
        direct = [
            token(me_s, flat * 2 + core, 0, cut, 0),
            token(me_s, tall * 2 + core, cut, length - cut, 1),
            token(me_s, flat * 2 + core, cut, length - cut, 4),
            token(me_s, tall * 2 + core, 0, cut, 5),
        ]
        onward = [
            token(flat * 2 + core, tall * 2 + core, 0, cut, 2),
            token(tall * 2 + core, flat * 2 + core, cut, length - cut, 3),
        ]
    else:
        direct = [token(me_s, c * 2 + core, 0, length, i) for i, c in enumerate(around)]
    for copy in direct + to_sibling:
        copy.start()
    shared(me_z).start()

    pre[...] = jnp.zeros_like(pre)
    fetch[4].wait()
    strip = 512

    def turn_cot(j, carry):
        at = pl.ds(pl.multiple_of(j * strip, strip), strip)
        cott[at, :] = cotv[:, at].T
        return carry

    lax.fori_loop(0, full // strip, turn_cot, 0)

    def cot_of(s):
        return cott.at[pl.ds(pl.multiple_of(s * inner, inner), inner)]

    dys[me_s] = cot_of(me_s)[...]

    def send_on():
        if square:
            for i in (0, 1):
                direct[i].wait_recv()
                onward[i].start()

    def step_hop(h):
        for p in (0, 1):
            if h == 1 and p == 1 and zeros > 2:
                send_on()
            for way in (0, 1):
                @pl.when(comes(way, h))
                def _():
                    flow(0, way, h, p, 1).wait_recv()
                if h < last_z:
                    @pl.when(sends(way, h))
                    def _():
                        flow(0, way, h, p, 0).start()
        if h < last_z:
            own_late(h)
        for way in (0, 1):
            @pl.when(comes(way, h))
            def _():
                shared(me_z - h if way == 0 else me_z + h).start()

    def late_hop(h, onward):
        for p in (0, 1):
            for way in (0, 1):
                goes = sends(way, h) if h < last_z else jnp.bool_(False)
                if onward:
                    if h < last_z:
                        @pl.when(goes)
                        def _():
                            flow(1, way, h, p, 1).wait_recv()
                            flow(1, way, h, p, 0).start()
                else:
                    @pl.when(jnp.logical_and(comes(way, h), jnp.logical_not(goes)))
                    def _():
                        flow(1, way, h, p, 1).wait_recv()

    if zeros > 2:
        step_hop(1)
    else:
        send_on()

    def chip_of(n):
        if square:
            return lax.rem(chip // 2 + n // 2, 2) * 2 + lax.rem(lax.rem(chip, 2) + n % 2, 2)
        return lax.rem(chip + n, chips)

    def turn(n, carry):
        for half_chip in (0, 1):
            k = chip_of(n) * 2 + half_chip
            tokt[:, pl.ds(pl.multiple_of(k * group, group), group)] = toks[k].T
        return carry

    early = 3 if square else 0
    if square:
        for i in (2, 3):
            direct[i].wait_recv()
        direct += onward
        more = [passed(flat * 2 + core, 1), passed(tall * 2 + core, 2)]
        for copy in more:
            copy.start()
        to_sibling += more
        for copy in to_sibling:
            copy.wait_recv()
        lax.fori_loop(0, early, turn, 0)

    cots = []
    for d in range(1, seqs):
        peer = lax.rem(me_s + d, seqs)
        cots.append(remote(cot_of(peer), dys.at[me_s], csem.at[0], csem.at[1], (peer, me_z)))
    for copy in cots:
        copy.start()
    all_cots = remote(
        dys.at[pl.ds(0, seqs - 1)], dys.at[pl.ds(0, seqs - 1)], csem.at[0], csem.at[1], sibling
    )
    for h in range(2, last_z):
        step_hop(h)

    def flip(j):
        shared(j).wait_recv()
        wallt[j] = wall[pl.ds(pl.multiple_of(j * rows, rows), rows), :v2].T

    def project(j, first, final):
        def part_of(n, carry):
            at = pl.ds(pl.multiple_of(j * rows, rows), rows)
            cols = pl.ds(pl.multiple_of(chip_of(n) * pairs, pairs), pairs)
            pre[:v2, cols] += nn(wallt[j], tokt[at, cols])
            return carry

        lax.fori_loop(first, final, part_of, 0)

    def project_all(j):
        def part_of(n, carry):
            at = pl.ds(pl.multiple_of(j * rows, rows), rows)
            cols = pl.ds(pl.multiple_of(n * 2 * pairs, 2 * pairs), 2 * pairs)
            pre[:v2, cols] += nn(wallt[j], tokt[at, cols])
            return carry

        lax.fori_loop(0, chips // 2, part_of, 0)

    def near(first, final, fresh):
        def one(j, carry):
            distance = jnp.abs(j - me_z)
            ready = distance < last_z if zeros > 1 else distance < 1

            @pl.when(ready)
            def _():
                if fresh:
                    flip(j)
                project(j, first, final)
            return carry

        lax.fori_loop(0, zeros, one, 0)

    if square:
        token(far * 2 + core, tall * 2 + core, 0, cut, 2).wait_recv()
        token(far * 2 + core, flat * 2 + core, cut, length - cut, 3).wait_recv()
        rest = [passed(far * 2 + core, 3)]
    else:
        rest = []
        for d in range(1, chips):
            direct[d - 1].wait_recv()
            rest.append(passed(lax.rem(chip - d + chips, chips) * 2 + core, d))
    for copy in rest:
        copy.start()
    if early:
        near(0, early, True)
    if not square:
        rest = to_sibling + rest
    for copy in rest:
        copy.wait_recv()
    to_sibling = to_sibling + rest if square else rest
    lax.fori_loop(early, chips, turn, 0)
    near(early, chips, not early)

    batch = 4 * group if chunks % 4 == 0 else pairs

    if zeros > 2:
        late_hop(1, True)
    if zeros > 1:
        step_hop(last_z)
        far_end = jnp.logical_or(me_z == 0, me_z == last_z)

        @pl.when(far_end)
        def _():
            flip(last_z - me_z)
            project_all(last_z - me_z)

    in_at = pl.multiple_of((1 - core) * STATE, 128)
    out_at = pl.multiple_of(core * STATE, 128)
    slot = lax.broadcasted_iota(jnp.int32, (slots, heads), 0)
    own_head = jnp.logical_and(
        lax.broadcasted_iota(jnp.int32, (slots, heads), 1) == me_s * hp + slot, slot < hp
    )

    def own(ref):
        return jnp.sum(jnp.where(own_head, ref[...], 0.0), axis=1, keepdims=True)

    bias, rate, gain = own(bias_in), -jnp.exp(own(log_in)), own(gain_in)
    row = lax.broadcasted_iota(jnp.int32, (group, group), 0)
    col = lax.broadcasted_iota(jnp.int32, (group, group), 1)
    causal = col >= row

    def spread(values, span):
        return jnp.concatenate(
            [jnp.broadcast_to(values[h : h + 1], (HEAD_DIM, values.shape[1])) for h in span], axis=0
        )

    def gather_rows(whole, span):
        parts = [
            jnp.sum(whole[i * HEAD_DIM : (i + 1) * HEAD_DIM], axis=0, keepdims=True)
            for i in range(len(span))
        ]
        return padded(parts, span)

    def padded(parts, span):
        lanes = parts[0].shape[1]
        if span[0] > 0:
            parts = [jnp.zeros((span[0], lanes), F32)] + parts
        if slots > span[-1] + 1:
            parts = parts + [jnp.zeros((slots - span[-1] - 1, lanes), F32)]
        return jnp.concatenate(parts, axis=0)

    raw = pre[top : top + slots, :] + bias
    soft = jax.nn.softplus(raw)
    curve = jax.nn.sigmoid(raw)
    stacked = jnp.concatenate([soft[:, k * group : (k + 1) * group] for k in range(chunks)], axis=0)
    steps[...] = stacked
    sigr[...] = jnp.concatenate([curve[:, k * group : (k + 1) * group] for k in range(chunks)], axis=0)
    logs = jnp.concatenate([rate] * chunks, axis=0) * stacked
    before = jnp.where(causal, 1.0, 0.0).astype(BF16)
    after = jnp.where(col <= row, 1.0, 0.0).astype(BF16)

    def summed(values, mask):
        a = values.astype(BF16)
        rest = values - a.astype(F32)
        b = rest.astype(BF16)
        c = (rest - b.astype(F32)).astype(BF16)
        return nn(a, mask) + (nn(b, mask) + nn(c, mask))

    cums[...] = summed(logs, before)

    def small(ref, k):
        return ref[pl.ds(pl.multiple_of(k * slots, slots), slots), :]

    def forward(g, k):
        span, mine_v, size = (range(n1), v1, in1) if g == 0 else (range(n1, hp), v2, in2)
        here = slice(span[0] * HEAD_DIM, span[0] * HEAD_DIM + size)
        at = pl.ds(pl.multiple_of(k * group, group), group)
        p = pre[mine_v : mine_v + size, at]
        sig = jax.nn.sigmoid(p)
        x = p * sig
        xs[k, here] = x
        pre[mine_v : mine_v + size, at] = sig * (1.0 + p * (1.0 - sig))
        step, cum = small(steps, k), small(cums, k)
        last = cum[:, group - 1 :]
        if g == 0:
            m_in, m_out = pre[pl.ds(in_at, STATE), at], pre[pl.ds(out_at, STATE), at]
            in16 = (m_in * jax.nn.sigmoid(m_in)).astype(BF16)
            out16 = (m_out * jax.nn.sigmoid(m_out)).astype(BF16)
            ins[k] = in16
            outs[k] = out16
            scores[k] = tn(in16, out16)
            cumt[k] = jnp.concatenate([cum, jnp.zeros((group - slots, group), F32)], axis=0).T
        else:
            in16 = ins[k]
        tail16 = (x * spread(step * jnp.exp(last - cum), span)).astype(BF16)
        tails[k, here] = tail16
        held = grad[here]
        states[k, here] = held.astype(BF16)
        leave = spread(jnp.exp(jnp.broadcast_to(last, (slots, STATE))), span)
        grad[here] = leave * held + nt(tail16, in16)

    def map_copy(k):
        return remote(maps.at[1 - core, k], got_map.at[k], msem.at[0, k], msem.at[1, k], sibling)

    def backward(g, k):
        span, mine_v, size = (range(n1), v1, in1) if g == 0 else (range(n1, hp), v2, in2)
        here = slice(span[0] * HEAD_DIM, span[0] * HEAD_DIM + size)
        at = pl.ds(pl.multiple_of(k * group, group), group)
        step, cum = small(steps, k), small(cums, k)
        last = cum[:, group - 1 :]
        x = xs[k, here]
        step_full = spread(step, span)
        u16 = (x * step_full).astype(BF16)
        tail16 = tails[k, here]
        in16, out16 = ins[k], outs[k]
        dy16 = dys[k, here]
        dy = dy16.astype(F32)
        tail = spread(jnp.exp(last - cum), span)
        lead = spread(jnp.exp(cum), span)
        leave = spread(jnp.exp(jnp.broadcast_to(last, (slots, STATE))), span)
        held16 = states[k, here]
        g_out = grad[here]
        g16 = g_out.astype(BF16)
        dy_lead = dy * lead
        lead16 = dy_lead.astype(BF16)

        score = scores[k]
        cum_col = cumt[k]
        d_score = jnp.zeros((group, group), F32)
        du_parts, r_parts = [], []
        for i, h in enumerate(span):
            at_h = slice(i * HEAD_DIM, (i + 1) * HEAD_DIM)
            diff = cum[h : h + 1] - cum_col[:, h : h + 1]
            within = jnp.exp(jnp.where(causal, diff, -1e30))
            mixing = (score * within).astype(BF16)
            d_mix = tn(u16[at_h], dy16[at_h])
            du_parts.append(nt(dy16[at_h], mixing))
            d_score = d_score + d_mix * within
            r_parts.append(jnp.sum(d_mix * mixing.astype(F32), axis=0, keepdims=True))
        du = jnp.concatenate(du_parts, axis=0) + nn(g16, in16) * tail
        from_x = gather_rows(du * x, span)
        from_u = gather_rows(du * u16.astype(F32), span)
        lead_rows = gather_rows(dy_lead * nn(held16, out16), span)
        cross = jnp.sum(gather_rows(g_out * states[k + 1, here].astype(F32), span), axis=1, keepdims=True)
        d_cum = padded(r_parts, span) + lead_rows - from_u
        d_log = summed(d_cum, after) + cross
        d_raw = (from_x + rate * d_log) * small(sigr, k)

        d_score16 = d_score.astype(BF16)
        d_out = nn(in16, d_score16) + tn(held16, lead16)
        d_in = nt(out16, d_score16) + tn(g16, tail16)
        grad[here] = leave * g_out + nt(lead16, out16)
        slope = pre[mine_v : mine_v + size, at]
        gain_full = spread(jnp.broadcast_to(gain, (slots, group)), span)
        grads[mine_v : mine_v + size, at] = ((du * step_full + dy * gain_full) * slope).astype(BF16)
        fill = jnp.zeros((16 - slots, group), F32)
        raw16 = jnp.concatenate([d_raw, fill], axis=0).astype(BF16)
        acc[0] += d_raw
        acc[1] += d_log * (rate * step)
        acc[2] += gather_rows(dy * x, span)
        if g == 0:
            grads[top : top + 16, at] = raw16
            maps[0, k] = d_in
            maps[1, k] = d_out
        else:
            grads[top : top + 16, at] += raw16
            m_in, m_out = pre[pl.ds(in_at, STATE), at], pre[pl.ds(out_at, STATE), at]
            s_in, s_out = jax.nn.sigmoid(m_in), jax.nn.sigmoid(m_out)
            d_in = (maps[0, k] + d_in) * (s_in * (1.0 + m_in * (1.0 - s_in)))
            d_out = (maps[1, k] + d_out) * (s_out * (1.0 + m_out * (1.0 - s_out)))
            maps[0, k] = d_in
            maps[1, k] = d_out
            grads[pl.ds(in_at, STATE), at] = d_in.astype(BF16)
            grads[pl.ds(out_at, STATE), at] = d_out.astype(BF16)
            map_copy(k).start()

            @pl.when(lax.rem(k, 2) != core)
            def _():
                swap(k // 2, k).start()

    def both_ways(g):
        def ahead(k, carry):
            forward(g, k)
            return carry

        def back(n, carry):
            backward(g, chunks - 1 - n)
            return carry

        here = slice(0, in1) if g == 0 else slice(in1, inner)
        lax.fori_loop(0, chunks, ahead, 0, unroll=4)
        states[chunks, here] = grad[here].astype(BF16)
        grad[here] = jnp.zeros_like(grad[here])
        if g == 0:
            for h in range(2, last_z):
                late_hop(h, True)
            all_cots.wait_recv()
        if g == 0:
            lax.fori_loop(0, chunks, back, 0, unroll=2)
        else:
            lax.fori_loop(0, chunks // 2, back, 0, unroll=2)
            serve(0, 1)
            lax.fori_loop(chunks // 2, chunks, back, 0, unroll=2)

    block = wbuf.shape[4]
    many = 4 if seqs % 4 == 0 else 2
    span_rows = many * zeros * block

    def weigh(g, first, size):
        def part_of(q, carry):
            at = pl.ds(pl.multiple_of(q * span_rows, span_rows), span_rows)
            product = nt(tokt[at, :], grads[first : first + size, :])
            for a in range(many):
                for t in range(zeros):
                    lo = (a * zeros + t) * block
                    wbuf[g, t, a % 2, q * (many // 2) + a // 2, :, 0:size] = product[
                        lo : lo + block
                    ].astype(BF16)
            return carry

        lax.fori_loop(0, seqs // many, part_of, 0)

    sizes = (w1, w2 + STATE)

    def back_flow(g, way, t, p):
        landed = rflow if way == 0 else lflow
        peer = up_peer if way == 0 else down_peer
        return remote(
            wbuf.at[g, t, p, :, :, pl.ds(0, sizes[g])], landed.at[g, t, p, :, :, pl.ds(0, sizes[g])],
            rsem.at[g, way, 0, t - 1 + way, p], rsem.at[g, way, 1, t - 1 + way, p], peer,
        )

    def from_ends(g):
        for z, way in ((0, 0), (last_z, 1)):
            if zeros > 1:
                @pl.when(me_z == z)
                def _():
                    for i in range(last_z):
                        for p in (0, 1):
                            back_flow(g, way, last_z - i if way == 0 else i, p).start()

    low = model // 2

    def turn_of(n):
        return lax.rem(chip + 1 + n, chips)

    def swap(i, k):
        return remote(
            grads.at[pl.ds(0, wide), pl.ds(pl.multiple_of(k * group, group), group)],
            sgrads.at[:, pl.ds(pl.multiple_of(i * group, group), group)],
            dsem.at[0, i], dsem.at[1, i], sibling,
        )

    def token_send(i):
        return remote(
            sent.at[i], tok_in.at[chip], ksem.at[0, i], ksem.at[1, chip], (i * 2 + core, me_z)
        )

    def plane_copy(part_no):
        to_flat = part_no % 2 == 0
        peer = (flat if to_flat else tall) * 2 + core
        first_half = part_no in (0, 2, 5)
        at = pl.ds(0 if first_half else low, low)
        if part_no < 2:
            src, dst = sent.at[far, at], relay.at[part_no]
        else:
            src, dst = sent.at[flat if to_flat else tall, at], tok_in.at[chip, at]
        return remote(src, dst, ksem.at[0, part_no], ksem.at[1, part_no], (peer, me_z))

    def relay_on():
        if square:
            for part_no, target, lo in ((1, flat, low), (0, tall, 0)):
                plane_copy(part_no).wait_recv()
                at = slice(lo, lo + low)
                sent[target, at, :] = (
                    sent[target, at, :].astype(F32) + relay[part_no].astype(F32)
                ).astype(BF16)
                plane_copy(4 + (1 - part_no)).start()

    def events(z):
        found = [(9.7, 2, "relay", 0)]
        for g in (0, 1):
            for p in (0, 1):
                ends = 0.0
                for i in range(last_z):
                    for way in (0, 1):
                        t = last_z - i if way == 0 else i
                        hops = z if way == 0 else last_z - z
                        if hops == 0:
                            continue
                        when = (g * last_z + i) * 2 + p + 1 + 2.2 * hops
                        if t == z:
                            ends = max(ends, when)
                        elif (way == 0) == (z < t):
                            found.append((when, 1 + g, "pass", (way, t, p)))
                found.append((ends + 0.01, 1 + g, "end", p))
            if g == 0:
                found.append((ends + 0.02, 1, "heads", 0))
        return sorted(found, key=lambda e: e[:2])

    served = 4

    def serve(first, final):
        for z in range(zeros):
            listed = events(z)
            soon = [e for e in listed if e[1:3] == (1, "pass")][:served]
            todo = [e for e in listed if e not in soon] if final is None else soon[first:final]
            if todo:
                @pl.when(me_z == z)
                def _():
                    serve_at(z, todo)

    def serve_at(z, todo):
        for _, g, what, p in todo:
            g = g - 1
            if what == "pass":
                way, t, p = p
                landed = rflow if way == 0 else lflow
                back_flow(g, way, t, p).wait_recv()
                wbuf[g, t, p] = (
                    wbuf[g, t, p].astype(F32) + landed[g, t, p].astype(F32)
                ).astype(BF16)
                back_flow(g, way, t, p).start()
            elif what == "relay":
                relay_on()
            elif what == "heads":
                close_heads()
                drain()
            else:
                finish_piece(z, g, p)

    def head_copy(d):
        return remote(
            hmine, hin.at[me_z], hsem.at[0], hsem.at[1], (me_s, lax.rem(me_z + d, zeros))
        )

    def head_along(d):
        return remote(
            hsum, hall.at[me_s], gsem.at[0], gsem.at[1], (lax.rem(me_s + d, seqs), me_z)
        )

    def all_heads():
        few = pl.ds(0, zeros - 1)
        return remote(hin.at[few], hin.at[few], hsem.at[0], hsem.at[1], sibling)

    def all_steps():
        few = pl.ds(0, zeros - 1)
        return remote(swbuf.at[few], swin.at[few], ysem.at[0], ysem.at[1], sibling)

    def close_heads():
        if zeros > 1:
            all_heads().wait_recv()
        sums = hin[0]
        for d in range(1, zeros):
            sums = sums + hin[d]
        hsum[...] = sums
        hall[me_s] = sums
        for d in range(1, seqs):
            head_along(d).start()

    def drain():
        for g in (0, 1):
            for p in (0, 1):
                for way in (0, 1):
                    for h in range(last_z):
                        @pl.when(sends(way, h))
                        def _():
                            flow(g, way, h, p, 0).wait_send()
        for j in range(zeros):
            shared(j).wait_send()
        for copy in direct + to_sibling + [all_cots]:
            copy.wait_send()

        def gone(k, carry):
            map_copy(k).wait_send()
            return carry

        lax.fori_loop(0, chunks, gone, 0)
        for i in range(chips):
            swap(i, 2 * i + 1 - core).wait_send()
        columns_copy.wait_send()

    def send_steps():
        steps_grad = nt(tokt[...], grads[top : top + 16, :])
        for t in range(zeros):
            lines = [
                steps_grad[(s * zeros + t) * block : (s * zeros + t + 1) * block] for s in range(seqs)
            ]
            swbuf[t] = jnp.concatenate(lines, axis=1).astype(BF16)
        swin[me_z] = swbuf[me_z]

        for d in range(1, zeros):
            steps_copy(d).start()

    def finish_piece(z, g, p):
        if z > 0:
            back_flow(g, 0, z, p).wait_recv()
        if z < last_z:
            back_flow(g, 1, z, p).wait_recv()
        if g == 1 and p == 0:
            if zeros > 1:
                all_steps().wait_recv()
            total = swin[0].astype(F32)
            for d in range(1, zeros):
                total = total + swin[d].astype(F32)
            total = total.astype(BF16)
            for s in range(seqs):
                stsend[s] = total[:, s * 16 : (s + 1) * 16]
            for s in range(seqs):
                @pl.when(me_s != s)
                def _():
                    steps_along(s).start()
        for j in range(seqs // 2):
            s = 2 * j + p
            value = wbuf[g, z, p, j, :, 0 : sizes[g]].astype(F32)
            if z > 0:
                value = value + rflow[g, z, p, j, :, 0 : sizes[g]].astype(F32)
            if z < last_z:
                value = value + lflow[g, z, p, j, :, 0 : sizes[g]].astype(F32)
            zsend[g, s, :, 0 : sizes[g]] = value.astype(BF16)
        for j in range(seqs // 2):
            @pl.when(me_s != 2 * j + p)
            def _():
                along(g, 2 * j + p).start()

    def along(g, s):
        lanes = pl.ds(0, sizes[g])
        return remote(
            zsend.at[g, s, :, lanes], rows_in.at[g, me_s, :, lanes],
            wsem.at[g, 0], wsem.at[g, 1], (s, me_z),
        )

    def steps_along(s):
        return remote(stsend.at[s], stin.at[me_s], xsem.at[0], xsem.at[1], (s, me_z))

    def steps_copy(d):
        target = lax.rem(me_z + d, zeros)
        return remote(
            swbuf.at[target], swin.at[me_z], ysem.at[0], ysem.at[1], (me_s, target)
        )

    grad[...] = jnp.zeros_like(grad)
    acc[...] = jnp.zeros_like(acc)
    grads[pl.ds(top, v2 - top), :] = jnp.zeros((v2 - top, chunks * group), BF16)
    if w2 > in2:
        grads[pl.ds(v2 + in2, w2 - in2), :] = jnp.zeros((w2 - in2, chunks * group), BF16)
    both_ways(0)
    weigh(0, v1, w1)
    from_ends(0)

    for h in range(1, zeros):
        late_hop(h, False)

    columns_copy = remote(
        wall.at[:, pl.ds(v1, wide - v1)], wall2.at[:, pl.ds(v1, wide - v1)], qsem.at[0], qsem.at[1], sibling
    )
    columns_copy.start()
    wall2[:, 0:STATE] = wall[:, STATE:v1]
    wall2[:, STATE:v1] = wall[:, 0:STATE]

    def project_late(i, carry):
        cols = pl.ds(pl.multiple_of(i * batch, batch), batch)
        pre[v2:wide, cols] = tn(wall[:, v2:wide], tokt[:, cols])
        return carry

    lax.fori_loop(0, chunks * group // batch, project_late, 0)
    both_ways(1)
    serve(1, 2)

    send_steps()
    for i in range(chips):
        at = pl.ds(pl.multiple_of((2 * i + core) * group, group), group)
        mgrads[:, i * group : (i + 1) * group] = grads[0:wide, at]
    columns_copy.wait_recv()
    for i in range(chips):
        swap(i, 2 * i + core).wait_recv()
    def back_project(j, carry):
        at = pl.ds(pl.multiple_of(j * low, low), low)
        product = nn(wall[at, :], mgrads[...]) + nn(wall2[at, :], sgrads[...])
        for i in range(chips):
            sent[i, at, :] = product[:, i * group : (i + 1) * group].astype(BF16)
        for turn_j in (0, 1):
            @pl.when(j == turn_j)
            def _():
                serve(2 + turn_j, 3 + turn_j)
        return carry

    lax.fori_loop(0, 2, back_project, 0)
    if square:
        for part_no in (0, 1, 2, 3):
            plane_copy(part_no).start()
    else:
        for n in range(chips):
            @pl.when(turn_of(n) != chip)
            def _():
                token_send(turn_of(n)).start()

    def merge(k, carry):
        map_copy(k).wait_recv()
        at = pl.ds(pl.multiple_of(k * group, group), group)
        grads[extra : extra + STATE, at] = (maps[core, k] + got_map[k]).astype(BF16)
        return carry

    lax.fori_loop(0, chunks, merge, 0)
    wide_head = hmine.shape[1]
    place_row = lax.broadcasted_iota(jnp.int32, (slots, wide_head), 0)
    place = jnp.logical_and(
        lax.broadcasted_iota(jnp.int32, (slots, wide_head), 1) == me_s * hp + place_row, place_row < hp
    )
    lines = [
        jnp.sum(
            jnp.where(place, jnp.sum(acc[i], axis=1, keepdims=True), 0.0), axis=0, keepdims=True
        )
        for i in range(3)
    ]
    hmine[...] = jnp.concatenate(lines + [jnp.zeros((5, wide_head), F32)], axis=0)
    hin[me_z] = hmine[...]

    for d in range(1, zeros):
        head_copy(d).start()

    weigh(1, v2, w2 + STATE)
    from_ends(1)

    serve(None, None)

    for g in (0, 1):
        rows_in[g, me_s] = zsend[g, me_s]
    if square:
        for part_no in (2, 3, 4, 5):
            plane_copy(part_no).wait_recv()
        sources = [flat, tall]
    else:
        for d in range(1, chips):
            at = lax.rem(chip + d, chips)
            remote(
                sent.at[at], tok_in.at[at], ksem.at[0, at], ksem.at[1, at], (at * 2 + core, me_z)
            ).wait_recv()
        sources = [lax.rem(chip + d, chips) for d in range(1, chips)]

    for j in (0, 1):
        at = slice(j * low, (j + 1) * low)
        value = sent[chip, at, :].astype(F32)
        for source in sources:
            value = value + tok_in[source, at, :].astype(F32)
        hid[:, at] = value.T.astype(BF16)

    leaving = [pltpu.make_async_copy(hid, hid_hbm, loc.at[0])]
    leaving[0].start()

    def whole(src, dst, sems, count):
        few = pl.ds(0, count)
        return remote(src.at[few], dst.at[few], sems.at[0], sems.at[1], sibling)

    def along_whole(g):
        lanes = pl.ds(0, sizes[g])
        few = pl.ds(0, seqs - 1)
        return remote(
            zsend.at[g, few, :, lanes], rows_in.at[g, few, :, lanes], wsem.at[g, 0], wsem.at[g, 1], sibling
        )

    along_whole(0).wait_recv()
    for s in range(seqs):
        piece_in = rows_in[0, s].astype(F32)
        rows_out[:, s * inner : s * inner + in1] = piece_in[:, :in1]
    whole(hall, hall, gsem, seqs - 1).wait_recv()
    sums = hall[0]
    for s in range(1, seqs):
        sums = sums + hall[s]
    head_out[...] = sums[:3, :heads]
    leaving.append(pltpu.make_async_copy(head_out, head_hbm, loc.at[1]))
    leaving[1].start()
    map_sums = [jnp.zeros((block, STATE), F32), jnp.zeros((block, STATE), F32)]
    stin[me_s] = stsend[me_s]
    whole(stsend, stin, xsem, seqs - 1).wait_recv()
    along_whole(1).wait_recv()
    for s in range(seqs):
        piece_in = rows_in[1, s].astype(F32)
        rows_out[:, s * inner + in1 : (s + 1) * inner] = piece_in[:, :in2]
        base = full + 2 * STATE + s * hp
        rows_out[:, base : base + hp] = stin[s, :, :hp].astype(F32)
        map_sums[s % 2] = map_sums[s % 2] + piece_in[:, w2 : w2 + STATE]
    rows_out[:, full : full + 2 * STATE] = jnp.concatenate(map_sums, axis=1)
    leaving.append(pltpu.make_async_copy(rows_out, rows_hbm, loc.at[2]))
    leaving[2].start()

    for g in (0, 1):
        for p in (0, 1):
            for way in (0, 1):
                for t in range(zeros):
                    if t == (0 if way == 0 else last_z):
                        continue
                    ahead = me_z < t if way == 0 else me_z > t

                    @pl.when(ahead)
                    def _():
                        back_flow(g, way, t, p).wait_send()
    if zeros > 1:
        all_steps().wait_send()
        all_heads().wait_send()
    whole(hall, hall, gsem, seqs - 1).wait_send()
    along_whole(0).wait_send()
    along_whole(1).wait_send()
    whole(stsend, stin, xsem, seqs - 1).wait_send()
    if square:
        for part_no in range(6):
            plane_copy(part_no).wait_send()
    else:
        for i in range(chips):
            @pl.when(i != chip)
            def _():
                token_send(i).wait_send()
    for copy in leaving:
        copy.wait()


def mixer_backward(hidden, cotangent, weight, bias, log, gain, seqs, zeros, hp):
    length, model = hidden.shape
    rows = weight.shape[0]
    heads = bias.shape[1]
    inner = hp * HEAD_DIM
    slots = up(hp, 8)
    (n1, w1), (n2, w2) = groups_of(hp)
    wide = 2 * STATE + w1 + w2
    ends = max(w1, w2 + STATE)
    block = rows // seqs
    chips = seqs // 2
    last = max(zeros - 1, 1)
    total = seqs * length
    full = seqs * inner
    span = up(inner + (HEAD_DIM if hp % 2 else 0), 128)
    lanes = up(heads, 128)
    dma = pltpu.SemaphoreType.DMA
    vmem = pl.BlockSpec(memory_space=pltpu.VMEM)
    anywhere = pl.BlockSpec(memory_space=pl.ANY)
    return pl.pallas_call(
        functools.partial(mixer_backward_kernel, seqs, zeros, hp),
        out_shape=(
            jax.ShapeDtypeStruct((length, model), BF16),
            jax.ShapeDtypeStruct((block, full + 2 * STATE + heads), F32),
            jax.ShapeDtypeStruct((3, heads), F32),
        ),
        in_specs=[anywhere] * 3 + [vmem] * 3,
        out_specs=(anywhere,) * 3,
        scratch_shapes=[
            pltpu.VMEM((length, model), BF16),
            pltpu.VMEM((block, full + 2 * STATE + heads), F32),
            pltpu.VMEM((3, heads), F32),
            pltpu.VMEM((rows, span), BF16),
            pltpu.VMEM((rows, heads), BF16),
            pltpu.VMEM((length, full), BF16),
            pltpu.VMEM((full, length), BF16),
            pltpu.VMEM((seqs, length, model), BF16),
            pltpu.VMEM((model, total), BF16),
            pltpu.VMEM((model, wide), BF16),
            pltpu.VMEM((zeros, 2 * STATE + w1, rows), BF16),
            pltpu.VMEM((wide, total), F32),
            pltpu.VMEM((seqs, inner, length), BF16),
            pltpu.VMEM((seqs, inner, length), F32),
            pltpu.VMEM((seqs, inner, length), BF16),
            pltpu.VMEM((seqs + 1, inner, STATE), BF16),
            pltpu.VMEM((wide + STATE, total), BF16),
            pltpu.VMEM((inner, STATE), F32),
            pltpu.VMEM((3, slots, length), F32),
            pltpu.VMEM((seqs * slots, length), F32),
            pltpu.VMEM((seqs * slots, length), F32),
            pltpu.VMEM((seqs, length, length), F32),
            pltpu.VMEM((seqs * slots, length), F32),
            pltpu.VMEM((2, seqs, STATE, length), F32),
            pltpu.VMEM((seqs, STATE, length), F32),
            pltpu.VMEM((model, wide), BF16),
            pltpu.VMEM((wide, chips * length), BF16),
            pltpu.VMEM((wide, chips * length), BF16),
            pltpu.VMEM((2, model // 2, length), BF16),
            pltpu.VMEM((chips, model, length), BF16),
            pltpu.VMEM((chips, model, length), BF16),
            pltpu.VMEM((2, zeros, 2, seqs // 2, block, ends), BF16),
            pltpu.VMEM((2, zeros, 2, seqs // 2, block, ends), BF16),
            pltpu.VMEM((2, zeros, 2, seqs // 2, block, ends), BF16),
            pltpu.VMEM((2, seqs, block, ends), BF16),
            pltpu.VMEM((2, seqs, block, ends), BF16),
            pltpu.VMEM((zeros, 8, lanes), F32),
            pltpu.VMEM((8, lanes), F32),
            pltpu.VMEM((8, lanes), F32),
            pltpu.VMEM((seqs, 8, lanes), F32),
            pltpu.VMEM((seqs, STATE, length), BF16),
            pltpu.VMEM((seqs, STATE, length), BF16),
            pltpu.VMEM((seqs, length, length), F32),
            pltpu.VMEM((zeros, block, seqs * 16), BF16),
            pltpu.VMEM((zeros, block, seqs * 16), BF16),
            pltpu.VMEM((seqs, block, 16), BF16),
            pltpu.VMEM((seqs, block, 16), BF16),
            dma((2, 2, 2, last, 2)),
            dma((2, max(6, chips))),
            dma((2, chips)),
            dma((2,)),
            dma((2, zeros)),
            dma((2, seqs)),
            dma((2, chips)),
            dma((2, max(6, chips))),
            dma((2, 2, 2, last, 2)),
            dma((2,)),
            dma((2,)),
            dma((2, 2)),
            dma((5,)),
            dma((2,)),
            dma((2,)),
            dma((2,)),
        ],
        compiler_params=pltpu.CompilerParams(
            collective_id=0, has_side_effects=True, vmem_limit_bytes=63 * 1024 * 1024
        ),
        name="mixer_backward",
    )(hidden, cotangent, weight, bias, log, gain)


def store_kernel(*refs):
    count = len(refs) // 3
    sem = refs[-1]
    takes = [pltpu.make_async_copy(refs[i], refs[2 * count + i], sem.at[0, i]) for i in range(count)]
    puts = [
        pltpu.make_async_copy(refs[2 * count + i], refs[count + i], sem.at[1, i]) for i in range(count)
    ]
    for copy in takes:
        copy.start()
    for take, put in zip(takes, puts):
        take.wait()
        put.start()
    for copy in puts:
        copy.wait()


def store(*arrays):
    return pl.pallas_call(
        store_kernel,
        out_shape=tuple(jax.ShapeDtypeStruct(a.shape, a.dtype) for a in arrays),
        in_specs=[pl.BlockSpec(memory_space=pl.ANY)] * len(arrays),
        out_specs=(pl.BlockSpec(memory_space=pl.ANY),) * len(arrays),
        scratch_shapes=[pltpu.VMEM(a.shape, a.dtype) for a in arrays]
        + [pltpu.SemaphoreType.DMA((2, len(arrays)))],
        name="store",
    )(*arrays)


def body(seqs, zeros, hidden, output_grad, input_weight, step_bias, decay_log, skip_gain):
    heads = step_bias.shape[0]
    hp = up(heads, seqs) // seqs
    spare = seqs * hp - heads
    full, total = heads * HEAD_DIM, seqs * hp * HEAD_DIM
    tokens, cot, weight = hidden[0], output_grad[0], input_weight
    params = [step_bias, decay_log, skip_gain]
    if spare:
        cot = jnp.pad(cot, ((0, 0), (0, total - full)))
        gap = jnp.zeros((weight.shape[0], total - full), BF16)
        few = jnp.zeros((weight.shape[0], spare), BF16)
        weight = jnp.concatenate([weight[:, :full], gap, weight[:, full:], few], axis=1)
        params = [jnp.pad(v, (0, spare)) for v in params]
    token_grad, weight_grad, head_grads = mixer_backward(
        tokens, cot, weight, *[v[None] for v in params], seqs, zeros, hp
    )
    token_grad, weight_grad, head_grads = store(token_grad, weight_grad, head_grads)
    if spare:
        weight_grad = jnp.concatenate(
            [weight_grad[:, :full], weight_grad[:, total : total + 2 * STATE + heads]], axis=1
        )
        head_grads = head_grads[:, :heads]
    return (token_grad[None], weight_grad, head_grads)


def solution(mesh):
    placed = (P("zero", "seq", None), P("zero", "seq", None), P("zero", None), P(), P(), P())
    return jax.shard_map(
        functools.partial(body, mesh.shape["seq"], mesh.shape["zero"]),
        mesh=mesh,
        in_specs=placed,
        out_specs=(P("zero", "seq", None), P(("seq", "zero"), None), P()),
        check_vma=False,
    )
```
